8 devices in a mesh: sweep: 2 (over z, y), ent: 4 (over x, core).
Axes of the slice: x: 2, y: 2, z: 1, core: 2. Of those that a mesh axis runs over, the one named last changes fastest.
Arguments:
- ent_emb: float32 [65536, 400], P(('sweep', 'ent')), parts along dimension 0
- ent_ada: float32 [65536], P(('sweep', 'ent')), parts along dimension 0
- rel_emb: float32 [2690, 400], P('sweep'), parts along dimension 0
- rel_ada: float32 [2690], P('sweep'), parts along dimension 0
- head_idx: int32 [8, 3, 2048], P(('sweep', 'ent')), parts along dimension 0
- tail_idx: int32 [8, 3, 2048], P(('sweep', 'ent')), parts along dimension 0
- rel_idx: int32 [8, 3, 2048], P(('sweep', 'ent')), parts along dimension 0
- edge_mask: int32 [8, 3, 2048], P(('sweep', 'ent')), parts along dimension 0
- neg_idx: int32 [6, 1000], P('sweep'), parts along dimension 0
Outputs:
- output 1: float32 [65536, 400], P(('sweep', 'ent')), parts along dimension 0
- output 2: float32 [65536], P(('sweep', 'ent')), parts along dimension 0
- output 3: float32 [2690, 400], P('sweep'), parts along dimension 0
- output 4: float32 [2690], P('sweep'), parts along dimension 0
- output 5: float32 [8, 3], P(('sweep', 'ent')), parts along dimension 0
There are 2 independent parts. The reference program is written for one: setup_inputs(seed, part) draws one part's arguments, and reference() takes and returns one part's arrays. A program takes and returns all parts, laid end to end along the dimension named above; each array names one.
All inputs are finite; a program needn't handle non-finite values.
Results may differ from the reference program's by a relative error of at most 0.001.
Values are sent between devices in bfloat16 or wider.
A program may use at most 1 GiB of HBM per device.

```python
import jax
import jax.numpy as jnp
from jax import lax

ENT_DEVS = 4
PART_ROWS = 8192
EMB_DIM = 400
NUM_REL = 1345
NEG_COUNT = 1000
EDGE_COUNT = 2048
ROUNDS = 3
TABLE_ROWS = ENT_DEVS * PART_ROWS
LEARN_RATE = 0.05
ADA_EPS = 1e-10


def draw_index(rng_key, upper, out_shape):
    key_a, key_b, key_c = jax.random.split(rng_key, 3)
    plain_ids = jax.random.randint(key_a, out_shape, 0, upper)
    hot_ids = jax.random.randint(key_b, out_shape, 0, max(upper // 16, 1))
    hot_pick = jax.random.randint(key_c, out_shape, 0, 4)
    return jnp.where(hot_pick == 0, hot_ids, plain_ids).astype(jnp.int32)


def setup_inputs(seed: int = 0, part: int = 0) -> dict:
    part_key = jax.random.fold_in(jax.random.key(seed), part)
    keys = jax.random.split(part_key, 10)
    rel_hits = EDGE_COUNT * ENT_DEVS / NUM_REL
    bucket = (ENT_DEVS, ROUNDS, EDGE_COUNT)
    fill_count = jax.random.randint(keys[7], (ENT_DEVS, ROUNDS, 1), EDGE_COUNT // 8, EDGE_COUNT + 1)
    return {
        'ent_emb': jax.random.normal(keys[0], (TABLE_ROWS, EMB_DIM), jnp.float32) * EMB_DIM ** -0.25,
        'ent_ada': jax.random.uniform(keys[1], (TABLE_ROWS,), jnp.float32, 0.5, 1.5) * EMB_DIM ** -0.5,
        'rel_emb': jax.random.normal(keys[2], (NUM_REL, EMB_DIM), jnp.float32) * 0.5 ** 0.5,
        'rel_ada': jax.random.uniform(keys[3], (NUM_REL,), jnp.float32, 0.5, 1.5) * (0.5 * rel_hits / EMB_DIM),
        'head_idx': draw_index(keys[4], PART_ROWS, bucket),
        'tail_idx': draw_index(keys[5], PART_ROWS, bucket),
        'rel_idx': jax.random.randint(keys[6], bucket, 0, NUM_REL).astype(jnp.int32),
        'edge_mask': (jax.random.randint(keys[8], bucket, 0, EDGE_COUNT) < fill_count).astype(jnp.int32),
        'neg_idx': jax.random.randint(keys[9], (ROUNDS, NEG_COUNT), 0, TABLE_ROWS).astype(jnp.int32),
    }


def bucket_grads(head_rows, tail_rows, neg_rows, rel_rows, edge_w):
    half = head_rows.shape[-1] // 2
    head_f = head_rows.astype(jnp.float32)
    h_re = head_f[:, :half]
    h_im = head_f[:, half:]
    r_re = rel_rows[:, :half]
    r_im = rel_rows[:, half:]
    query = jnp.concatenate([h_re * r_re - h_im * r_im, h_re * r_im + h_im * r_re], axis=1)
    query_bf = query.astype(jnp.bfloat16)
    tail_f = tail_rows.astype(jnp.float32)
    pos_score = jnp.sum(query * tail_f, axis=1)
    neg_score = jnp.dot(query_bf, neg_rows.T, preferred_element_type=jnp.float32)
    top_score = jnp.maximum(pos_score, jnp.max(neg_score, axis=1))
    pos_exp = jnp.exp(pos_score - top_score)
    neg_exp = jnp.exp(neg_score - top_score[:, None])
    norm_sum = pos_exp + jnp.sum(neg_exp, axis=1)
    log_norm = top_score + jnp.log(norm_sum)
    loss = jnp.sum(edge_w * (log_norm - pos_score)) / EDGE_COUNT
    pos_grad = edge_w * (pos_exp / norm_sum - 1.0)
    neg_grad = (edge_w[:, None] * neg_exp / norm_sum[:, None]).astype(jnp.bfloat16)
    query_grad = pos_grad[:, None] * tail_f + jnp.dot(neg_grad, neg_rows, preferred_element_type=jnp.float32)
    tail_grad = pos_grad[:, None] * query
    negrow_grad = jnp.dot(neg_grad.T, query_bf, preferred_element_type=jnp.float32)
    g_re = query_grad[:, :half]
    g_im = query_grad[:, half:]
    head_grad = jnp.concatenate([g_re * r_re + g_im * r_im, g_im * r_re - g_re * r_im], axis=1)
    relrow_grad = jnp.concatenate([g_re * h_re + g_im * h_im, g_im * h_re - g_re * h_im], axis=1)
    return loss, head_grad, tail_grad, negrow_grad, relrow_grad


def adagrad_rows(table, state, grad):
    new_state = state + jnp.mean(grad * grad, axis=1)
    return table - LEARN_RATE * grad / jnp.sqrt(new_state + ADA_EPS)[:, None], new_state


def reference(ent_emb, ent_ada, rel_emb, rel_ada, head_idx, tail_idx, rel_idx, edge_mask, neg_idx):
    def train_step(carry, round_no):
        table, state, rel_tab, rel_state = carry
        table_bf = table.astype(jnp.bfloat16)
        neg_ids = neg_idx[round_no]
        neg_rows = table_bf[neg_ids]

        def one_bucket(acc_pair, dev_no):
            grad_ent, grad_rel = acc_pair
            head_ids = dev_no * PART_ROWS + head_idx[dev_no, round_no]
            tail_ids = ((dev_no + round_no) % ENT_DEVS) * PART_ROWS + tail_idx[dev_no, round_no]
            rel_ids = rel_idx[dev_no, round_no]
            edge_w = edge_mask[dev_no, round_no].astype(jnp.float32)
            loss, head_grad, tail_grad, negrow_grad, relrow_grad = bucket_grads(
                table_bf[head_ids], table_bf[tail_ids], neg_rows, rel_tab[rel_ids], edge_w)
            grad_ent = grad_ent.at[head_ids].add(head_grad).at[tail_ids].add(tail_grad).at[neg_ids].add(negrow_grad)
            grad_rel = grad_rel.at[rel_ids].add(relrow_grad)
            return (grad_ent, grad_rel), loss

        zero_acc = (jnp.zeros_like(table), jnp.zeros_like(rel_tab))
        (grad_ent, grad_rel), losses = lax.scan(one_bucket, zero_acc, jnp.arange(ENT_DEVS))
        table, state = adagrad_rows(table, state, grad_ent)
        rel_tab, rel_state = adagrad_rows(rel_tab, rel_state, grad_rel)
        return (table, state, rel_tab, rel_state), losses

    init_carry = (ent_emb, ent_ada, rel_emb, rel_ada)
    (table, state, rel_tab, rel_state), losses = lax.scan(train_step, init_carry, jnp.arange(ROUNDS))
    return table, state, rel_tab, rel_state, losses.T
```

```python
import functools

import jax
import jax.numpy as jnp
from jax import lax
from jax.experimental import pallas as pl
from jax.experimental.pallas import tpu as pltpu
from jax.sharding import PartitionSpec as P

LEARN_RATE = 0.05
ADA_EPS = 1e-10
LANES = 128
SLICES = 4
CHUNK = 256
BATCH = 4
F32 = jnp.float32
BF16 = jnp.bfloat16


def ceil_to(value, unit):
    return -(-value // unit) * unit


def vmem():
    return pl.BlockSpec(memory_space=pltpu.VMEM)


def smem():
    return pl.BlockSpec(memory_space=pltpu.SMEM)


def hbm():
    return pl.BlockSpec(memory_space=pltpu.MemorySpace.HBM)


def four(index):
    return pl.multiple_of(index, SLICES)


def gather_rows(src, ids, base, stage, count):
    for k in range(count):
        stage[pl.ds(SLICES * k, SLICES), :] = src[pl.ds(four(ids[base + k]), SLICES), :]


def stage_cols(stage, slice_no):
    return stage[pl.ds(slice_no, LANES, stride=SLICES), :].T


def add_rows(acc, ids, base, rows, row_base, count):
    for first in range(0, count, BATCH):
        index = [ids[base + first + k] for k in range(BATCH)]
        grads = [rows[pl.ds(four(row_base + SLICES * (first + k)), SLICES), :] for k in range(BATCH)]
        total = [acc[pl.ds(four(index[k]), SLICES), :] + grads[k] for k in range(BATCH)]
        for k in range(1, BATCH):
            for earlier in range(k):
                total[k] = total[k] + jnp.where(index[earlier] == index[k], grads[earlier], 0.0)
        for k in range(BATCH):
            acc[pl.ds(four(index[k]), SLICES), :] = total[k]


def zero_rows(ref, step=1024):
    rows = ref.shape[0]
    whole = rows // step

    def body(i, _):
        ref[pl.ds(pl.multiple_of(i * step, 8), step), :] = jnp.zeros((step, LANES), ref.dtype)
        return 0

    lax.fori_loop(0, whole, body, 0)
    if rows % step:
        ref[pl.ds(whole * step, rows % step), :] = jnp.zeros((rows % step, LANES), ref.dtype)


def gather_out(dim, table, ids, out, stage, count):
    def body(b, _):
        gather_rows(table, ids, b * LANES, stage, LANES)
        cols = pl.ds(pl.multiple_of(b * LANES, LANES), LANES)
        for j in range(SLICES):
            size = min(LANES, dim - j * LANES)
            out[pl.ds(j * LANES, size), cols] = stage_cols(stage, j)[:size].astype(BF16)
        return 0

    lax.fori_loop(0, count // LANES, body, 0)


def gather_all(dim, core, table, heads, tails, negs, hb, tb, nk, ns, nbuf, stage):
    half = nbuf.shape[1] // 2
    gather_out(dim, table, negs, nbuf, stage, nbuf.shape[1])
    nk[...] = nbuf[:, pl.ds(pl.multiple_of(core * half, LANES), half)]
    ns[...] = nbuf[:, pl.ds(pl.multiple_of((1 - core) * half, LANES), half)]
    gather_out(dim, table, tails, tb, stage, tb.shape[1])
    gather_out(dim, table, heads, hb, stage, hb.shape[1])


def entry_kernel(dim, rows, core_ref, heads, tails, negs, et, g, t4_out, v_out, hb, tb, nk, ns,
                 t4, v, inbuf, stage, nbuf, in_sem, out_sem):
    cols = inbuf.shape[2]
    steps = rows // cols
    per = cols // LANES

    def fetch(step, slot):
        return pltpu.make_async_copy(et.at[:, pl.ds(pl.multiple_of(step * cols, LANES), cols)],
                                     inbuf.at[slot, pl.ds(0, dim)], in_sem.at[slot])

    fetch(0, 0).start()
    for slot in range(2):
        inbuf[slot, pl.ds(dim, SLICES * LANES - dim), :] = jnp.zeros((SLICES * LANES - dim, cols), F32)
    t4[pl.ds(rows * SLICES, 32), :] = jnp.zeros((32, LANES), F32)

    def body(step, _):
        slot = lax.rem(step, 2)

        @pl.when(step + 1 < steps)
        def _():
            fetch(step + 1, 1 - slot).start()

        fetch(step, slot).wait()
        for b in range(per):
            row0 = (step * per + b) * LANES
            for j in range(SLICES):
                t4[pl.ds(SLICES * row0 + j, LANES, stride=SLICES), :] = inbuf[slot, pl.ds(j * LANES, LANES), pl.ds(b * LANES, LANES)].T
            v[pl.ds(pl.multiple_of(row0, 8), LANES), :] = jnp.broadcast_to(g[pl.ds(step * per + b, 1), :], (LANES, LANES)).T
        return 0

    lax.fori_loop(0, steps, body, 0)
    save_t = pltpu.make_async_copy(t4.at[pl.ds(0, rows * SLICES)], t4_out, out_sem.at[0])
    save_v = pltpu.make_async_copy(v, v_out, out_sem.at[1])
    save_v.start()
    gather_all(dim, core_ref[0], t4, heads, tails, negs, hb, tb, nk, ns, nbuf, stage)
    save_t.start()
    save_t.wait()
    save_v.wait()


def bucket_kernel(dim, neg_count, num_rel, edges, first, *refs):
    if first:
        (core_ref, rel, w, hb, tb, nfull, nother, rfm, vr,
         loss, dp_out, hg, nk, ns, rk, rs, r4,
         nb, nbt, ds, sc, rt, ng, racc, stage, qs, fm) = refs
    else:
        (core_ref, rel, w, hb, tb, nfull, nother, rfm_in, vr_in, rmine, rother,
         loss, dp_out, hg, nk, ns, rk, rs, r4, rfm, vr,
         nb, nbt, ds, sc, rt, ng, racc, stage, qs, fm) = refs
    core = core_ref[0]
    half = dim // 2
    relp = rfm.shape[1]
    negp = nb.shape[1]
    tops = SLICES * LANES
    my_half = pl.ds(pl.multiple_of(core * half, 8), half)
    other_half = pl.ds(pl.multiple_of((1 - core) * half, 8), half)

    if not first:
        fm[my_half, pl.ds(0, relp)] = rmine[...]
        fm[other_half, pl.ds(0, relp)] = rother[...]
        grad = fm[pl.ds(0, dim), pl.ds(0, relp)]
        vr[...] = vr_in[...] + jnp.sum(grad * grad, axis=0, keepdims=True) / dim
        rate = LEARN_RATE / jnp.sqrt(vr[...] + ADA_EPS)
        rfm[...] = rfm_in[...] - fm[pl.ds(0, dim), pl.ds(0, relp)] * rate

    fm[pl.ds(dim, tops - dim), :] = jnp.zeros((tops - dim, fm.shape[1]), F32)
    rt[pl.ds(dim, tops - dim), :] = jnp.zeros((tops - dim, CHUNK), F32)
    qs[pl.ds(dim, tops - dim), :] = jnp.zeros((tops - dim, CHUNK), F32)
    for b in range(relp // LANES):
        for j in range(SLICES):
            if (j + 1) * LANES <= dim:
                block = rfm[pl.ds(j * LANES, LANES), pl.ds(b * LANES, LANES)]
            else:
                fm[pl.ds(j * LANES, dim - j * LANES), pl.ds(0, LANES)] = rfm[pl.ds(j * LANES, dim - j * LANES), pl.ds(b * LANES, LANES)]
                block = fm[pl.ds(j * LANES, LANES), pl.ds(0, LANES)]
            r4[pl.ds(SLICES * b * LANES + j, LANES, stride=SLICES), :] = block.T

    nhalf = negp // 2
    nb[:, pl.ds(pl.multiple_of(core * nhalf, LANES), nhalf)] = nfull[...]
    nb[:, pl.ds(pl.multiple_of((1 - core) * nhalf, LANES), nhalf)] = nother[...]
    for b in range(negp // LANES):
        nbt[pl.ds(b * LANES, LANES), :] = nb[:, pl.ds(b * LANES, LANES)].astype(F32).T.astype(BF16)
    zero_rows(racc)
    ng[...] = jnp.zeros(ng.shape, F32)
    ds[pl.ds(neg_count, negp - neg_count), :] = jnp.zeros((negp - neg_count, CHUNK), BF16)

    def step(c, loss_row):
        cols = pl.ds(pl.multiple_of(c * CHUNK, LANES), CHUNK)
        for b in range(CHUNK // LANES):
            gather_rows(r4, rel, c * CHUNK + b * LANES, stage, LANES)
            for j in range(SLICES):
                rt[pl.ds(j * LANES, LANES), pl.ds(b * LANES, LANES)] = stage_cols(stage, j)
        h = hb[:, cols].astype(F32)
        q_re = h[:half] * rt[pl.ds(0, half), :] - h[half:] * rt[pl.ds(half, half), :]
        q_im = h[:half] * rt[pl.ds(half, half), :] + h[half:] * rt[pl.ds(0, half), :]
        q = jnp.concatenate([q_re, q_im], axis=0)
        qb = q.astype(BF16)
        t = tb[:, cols].astype(F32)
        pos = jnp.sum(q * t, axis=0, keepdims=True)
        sc[...] = lax.dot_general(nbt[...], qb, (((1,), (0,)), ((), ())), preferred_element_type=F32)
        top = jnp.maximum(pos, jnp.max(sc[pl.ds(0, neg_count), :], axis=0, keepdims=True))
        pos_exp = jnp.exp(pos - top)
        norm = pos_exp
        part = 200
        for i in range(0, neg_count, part):
            size = min(part, neg_count - i)
            e = jnp.exp(sc[pl.ds(i, size), :] - top)
            sc[pl.ds(i, size), :] = e
            norm = norm + jnp.sum(e, axis=0, keepdims=True)
        wt = w[:, cols]
        loss_row = loss_row + wt * (top + jnp.log(norm) - pos)
        dp = wt * (pos_exp / norm - 1.0)
        dp_out[:, cols] = dp
        scale = wt / norm
        ds[pl.ds(0, neg_count), :] = (sc[pl.ds(0, neg_count), :] * scale).astype(BF16)
        ng[...] += lax.dot_general(ds[...], qb, (((1,), (1,)), ((), ())), preferred_element_type=F32)
        gq = lax.dot_general(nb[...], ds[...], (((1,), (0,)), ((), ())), preferred_element_type=F32) + dp * tb[:, cols].astype(F32)
        g_re, g_im = gq[:half], gq[half:]
        h = hb[:, cols].astype(F32)
        r_re, r_im = rt[pl.ds(0, half), :], rt[pl.ds(half, half), :]
        qs[pl.ds(0, half), :] = g_re * r_re + g_im * r_im
        qs[pl.ds(half, half), :] = g_im * r_re - g_re * r_im
        for b in range(CHUNK // LANES):
            for j in range(SLICES):
                hg[pl.ds(SLICES * (c * CHUNK + b * LANES) + j, LANES, stride=SLICES), :] = qs[pl.ds(j * LANES, LANES), pl.ds(b * LANES, LANES)].T
        h_re, h_im = h[:half], h[half:]
        qs[pl.ds(0, half), :] = g_re * h_re + g_im * h_im
        qs[pl.ds(half, half), :] = g_im * h_re - g_re * h_im
        for b in range(CHUNK // LANES):
            for j in range(SLICES):
                stage[pl.ds(j, LANES, stride=SLICES), :] = qs[pl.ds(j * LANES, LANES), pl.ds(b * LANES, LANES)].T
            add_rows(racc, rel, c * CHUNK + b * LANES, stage, 0, LANES)
        return loss_row

    loss_row = lax.fori_loop(0, edges // CHUNK, step, jnp.zeros((1, CHUNK), F32))
    loss[...] = jnp.broadcast_to(jnp.sum(loss_row, axis=1, keepdims=True) / edges, loss.shape)

    for b in range(negp // LANES):
        for j in range(SLICES):
            size = min(LANES, dim - j * LANES)
            fm[pl.ds(j * LANES, size), pl.ds(b * LANES, LANES)] = ng[pl.ds(b * LANES, LANES), pl.ds(j * LANES, size)].T
    nk[...] = fm[my_half, pl.ds(0, negp)]
    ns[...] = fm[other_half, pl.ds(0, negp)]
    for b in range(relp // LANES):
        for j in range(SLICES):
            size = min(LANES, dim - j * LANES)
            fm[pl.ds(j * LANES, size), pl.ds(b * LANES, LANES)] = racc[pl.ds(SLICES * b * LANES + j, LANES, stride=SLICES), :].T[:size]
    rk[...] = fm[my_half, pl.ds(0, relp)]
    rs[...] = fm[other_half, pl.ds(0, relp)]


def update_kernel(dim, rows, edges, last, *refs):
    if last:
        (core_ref, heads, tails, rel, negs, t4_in, v_in, hg, hb_in, dp, r4, nmine, nother,
         et_out, g_out, t4, v, acc, stage, rt, outbuf, in_sem, out_sem) = refs
    else:
        (core_ref, heads, tails, rel, negs, heads_n, tails_n, negs_n, t4_in, v_in, hg, hb_in, dp, r4, nmine, nother,
         t4_out, v_out, hb, tb, nk, ns, t4, v, acc, stage, rt, nbuf, in_sem, out_sem) = refs
    core = core_ref[0]
    half = dim // 2
    tops = SLICES * LANES
    load_t = pltpu.make_async_copy(t4_in, t4.at[pl.ds(0, rows * SLICES)], in_sem.at[0])
    load_v = pltpu.make_async_copy(v_in, v, in_sem.at[1])
    load_t.start()
    load_v.start()
    zero_rows(acc)
    t4[pl.ds(rows * SLICES, 32), :] = jnp.zeros((32, LANES), F32)
    rt[pl.ds(dim, tops - dim), :] = jnp.zeros((tops - dim, LANES), F32)

    def head_step(b, _):
        add_rows(acc, heads, b * 32, hg, b * 32 * SLICES, 32)
        return 0

    lax.fori_loop(0, edges // 32, head_step, 0)

    def unstage():
        for j in range(SLICES):
            stage[pl.ds(j, LANES, stride=SLICES), :] = rt[pl.ds(j * LANES, LANES), :].T

    def tail_step(b, _):
        cols = pl.ds(pl.multiple_of(b * LANES, LANES), LANES)
        gather_rows(r4, rel, b * LANES, stage, LANES)
        for j in range(SLICES):
            rt[pl.ds(j * LANES, LANES), :] = stage_cols(stage, j)
        h = hb_in[:, cols].astype(F32)
        r_re, r_im = rt[pl.ds(0, half), :], rt[pl.ds(half, half), :]
        scale = dp[:, cols]
        q_re = scale * (h[:half] * r_re - h[half:] * r_im)
        q_im = scale * (h[:half] * r_im + h[half:] * r_re)
        rt[pl.ds(0, half), :] = q_re
        rt[pl.ds(half, half), :] = q_im
        unstage()
        add_rows(acc, tails, b * LANES, stage, 0, LANES)
        return 0

    lax.fori_loop(0, edges // LANES, tail_step, 0)

    def neg_step(b, _):
        cols = pl.ds(pl.multiple_of(b * LANES, LANES), LANES)
        rt[pl.ds(pl.multiple_of(core * half, 8), half), :] = nmine[:, cols]
        rt[pl.ds(pl.multiple_of((1 - core) * half, 8), half), :] = nother[:, cols]
        unstage()
        add_rows(acc, negs, b * LANES, stage, 0, LANES)
        return 0

    lax.fori_loop(0, nmine.shape[1] // LANES, neg_step, 0)
    load_t.wait()
    load_v.wait()

    block = LANES

    def ada_step(b, _):
        row0 = b * block
        parts = [acc[pl.ds(SLICES * row0 + j, block, stride=SLICES), :] for j in range(SLICES)]
        square = parts[0] * parts[0]
        for j in range(1, SLICES):
            square = square + parts[j] * parts[j]
        vrows = pl.ds(pl.multiple_of(row0, 8), block)
        new_v = v[vrows, :] + jnp.sum(square, axis=1, keepdims=True) / dim
        v[vrows, :] = new_v
        rate = LEARN_RATE / jnp.sqrt(new_v + ADA_EPS)
        for j in range(SLICES):
            where = pl.ds(SLICES * row0 + j, block, stride=SLICES)
            t4[where, :] = t4[where, :] - acc[where, :] * rate
        return 0

    lax.fori_loop(0, rows // block, ada_step, 0)

    if not last:
        save_v = pltpu.make_async_copy(v, v_out, out_sem.at[1])
        save_v.start()
        gather_all(dim, core, t4, heads_n, tails_n, negs_n, hb, tb, nk, ns, nbuf, stage)
        save_t = pltpu.make_async_copy(t4.at[pl.ds(0, rows * SLICES)], t4_out, out_sem.at[0])
        save_t.start()
        save_t.wait()
        save_v.wait()
        return

    width = outbuf.shape[2]
    per = width // LANES
    steps = rows // width

    def save(step, slot):
        return pltpu.make_async_copy(outbuf.at[slot], et_out.at[:, pl.ds(pl.multiple_of(step * width, LANES), width)], out_sem.at[slot])

    def exit_step(step, _):
        slot = lax.rem(step, 2)

        @pl.when(step >= 2)
        def _():
            save(step - 2, slot).wait()

        for b in range(per):
            row0 = (step * per + b) * LANES
            for j in range(SLICES):
                size = min(LANES, dim - j * LANES)
                outbuf[slot, pl.ds(j * LANES, size), pl.ds(b * LANES, LANES)] = t4[pl.ds(SLICES * row0 + j, LANES, stride=SLICES), :].T[:size]
            g_out[pl.ds(step * per + b, 1), :] = v[pl.ds(pl.multiple_of(row0, 8), LANES), :].T[:1]
        save(step, slot).start()
        return 0

    lax.fori_loop(0, steps, exit_step, 0)
    save(steps - 2, (steps - 2) % 2).wait()
    save(steps - 1, (steps - 1) % 2).wait()


def params():
    return pltpu.CompilerParams(vmem_limit_bytes=63 * 1024 * 1024)


def cost(micros):
    return pl.CostEstimate(flops=int(micros * 5e6), bytes_accessed=0, transcendentals=0)


def shape(dims, dtype=F32):
    return jax.ShapeDtypeStruct(dims, dtype)


def solution(mesh):
    ent_size = mesh.shape['ent']
    row_spec = P(('sweep', 'ent'), None)
    flat_spec = P(('sweep', 'ent'))
    rel_spec = P('sweep', None)
    state_spec = P('sweep')
    edge_spec = P(('sweep', 'ent'), None, None)
    swap = [(i, i ^ 1) for i in range(ent_size)]
    cross = [(i, i ^ 2) for i in range(ent_size)]

    def shift(amount):
        return [(i, (i + amount) % ent_size) for i in range(ent_size)]

    def group_sum(keep, send):
        part = keep + lax.ppermute(send, 'ent', swap)
        mine = part + lax.ppermute(part, 'ent', cross)
        return mine, lax.ppermute(mine, 'ent', swap)

    def device_fn(ent_emb, ent_ada, rel_emb, rel_ada, head_idx, tail_idx, rel_idx, edge_mask, neg_idx):
        rows, dim = ent_emb.shape
        num_rel = rel_emb.shape[0]
        _, rounds, edges = head_idx.shape
        neg_count = neg_idx.shape[1]
        negp = ceil_to(neg_count, 2 * LANES)
        relp = ceil_to(num_rel, LANES)
        half = dim // 2
        my_dev = lax.axis_index('ent')
        core = (my_dev % 2).reshape(1)

        heads = [head_idx[0, s] * SLICES for s in range(rounds)]
        own_tails = [tail_idx[0, s] * SLICES for s in range(rounds)]
        own_rels = [rel_idx[0, s] * SLICES for s in range(rounds)]
        tails, rels = [own_tails[0]], [own_rels[0]]
        for s in range(1, rounds):
            got = lax.ppermute(jnp.stack([own_tails[s], own_rels[s]]), 'ent', shift(s))
            tails.append(got[0])
            rels.append(got[1])
        owned = (neg_idx // rows) == my_dev
        neg_local = jnp.where(owned, neg_idx % rows, rows) * SLICES
        neg_local = jnp.pad(neg_local, ((0, 0), (0, negp - neg_count)), constant_values=rows * SLICES)
        negs = [neg_local[s] for s in range(rounds)]
        weights = edge_mask[0].astype(F32)

        wide_rows = (rows + 8) * SLICES
        bucket_out = [shape((dim, edges), BF16), shape((dim, edges), BF16), shape((dim, negp // 2), BF16), shape((dim, negp // 2), BF16)]
        stage_shape = pltpu.VMEM((SLICES * LANES, LANES), F32)
        t4, v, hb, tb, nk, ns = pl.pallas_call(
            functools.partial(entry_kernel, dim, rows),
            out_shape=[shape((rows * SLICES, LANES)), shape((rows, LANES))] + bucket_out,
            in_specs=[smem()] * 4 + [hbm(), vmem()],
            out_specs=[hbm(), hbm()] + [vmem()] * 4,
            scratch_shapes=[pltpu.VMEM((wide_rows, LANES), F32), pltpu.VMEM((rows, LANES), F32),
                            pltpu.VMEM((2, SLICES * LANES, 4 * LANES), F32), stage_shape, pltpu.VMEM((dim, negp), BF16),
                            pltpu.SemaphoreType.DMA((2,)), pltpu.SemaphoreType.DMA((2,))],
            compiler_params=params(), cost_estimate=cost(40), name='entry',
        )(core, heads[0], tails[0], negs[0], ent_emb.T, ent_ada.reshape(rows // LANES, LANES))

        rfm = jnp.pad(rel_emb.T, ((0, 0), (0, relp - num_rel)))
        vr = jnp.pad(rel_ada, (0, relp - num_rel), constant_values=1.0).reshape(1, relp)
        losses = []
        rel_grads = None
        for s in range(rounds):
            nmine, nother = group_sum(nk, ns)
            if s == 0:
                tail_cols, head_cols = tb, hb
            else:
                tail_cols = lax.ppermute(tb, 'ent', shift(-s))
                head_cols = lax.ppermute(hb, 'ent', shift(s))
            first = s == 0
            outs = [shape((1, LANES)), shape((1, edges)), shape((edges * SLICES, LANES)),
                    shape((half, negp)), shape((half, negp)), shape((half, relp)), shape((half, relp)), shape((relp * SLICES, LANES))]
            args = [core, own_rels[s], weights[s].reshape(1, edges), hb, tail_cols, nmine, nother, rfm, vr]
            if not first:
                outs += [shape((dim, relp)), shape((1, relp))]
                args += list(rel_grads)
            res = pl.pallas_call(
                functools.partial(bucket_kernel, dim, neg_count, num_rel, edges, first),
                out_shape=outs,
                in_specs=[smem()] * 2 + [vmem()] * (len(args) - 2),
                out_specs=[vmem()] * len(outs),
                scratch_shapes=[pltpu.VMEM((dim, negp), BF16), pltpu.VMEM((negp, dim), BF16), pltpu.VMEM((negp, CHUNK), BF16),
                                pltpu.VMEM((negp, CHUNK), F32), pltpu.VMEM((SLICES * LANES, CHUNK), F32), pltpu.VMEM((negp, dim), F32),
                                pltpu.VMEM((relp * SLICES, LANES), F32), stage_shape, pltpu.VMEM((SLICES * LANES, CHUNK), F32),
                                pltpu.VMEM((SLICES * LANES, max(relp, negp)), F32)],
                compiler_params=params(), cost_estimate=cost(40), name='bucket',
            )(*args)
            loss, dp, hg, gk, gs, rk, rs, r4 = res[:8]
            if not first:
                rfm, vr = res[8:]
            losses.append(loss[0, 0])
            gmine, gother = group_sum(gk, gs)
            rel_grads = group_sum(rk, rs)
            if s > 0:
                dp = lax.ppermute(dp, 'ent', shift(s))
            last = s == rounds - 1
            args = [core, heads[s], tails[s], rels[s], negs[s]]
            if not last:
                args += [heads[s + 1], tails[s + 1], negs[s + 1]]
            scalars = len(args)
            args += [t4, v, hg, head_cols, dp, r4, gmine, gother]
            scratch = [pltpu.VMEM((wide_rows, LANES), F32), pltpu.VMEM((rows, LANES), F32), pltpu.VMEM((wide_rows, LANES), F32),
                       stage_shape, pltpu.VMEM((SLICES * LANES, LANES), F32)]
            if last:
                outs = [shape((dim, rows)), shape((rows // LANES, LANES))]
                specs = [hbm(), vmem()]
                scratch += [pltpu.VMEM((2, dim, 4 * LANES), F32)]
            else:
                outs = [shape((rows * SLICES, LANES)), shape((rows, LANES))] + bucket_out
                specs = [hbm(), hbm()] + [vmem()] * 4
                scratch += [pltpu.VMEM((dim, negp), BF16)]
            res = pl.pallas_call(
                functools.partial(update_kernel, dim, rows, edges, last),
                out_shape=outs,
                in_specs=[smem()] * scalars + [hbm()] * 2 + [vmem()] * 6,
                out_specs=specs,
                scratch_shapes=scratch + [pltpu.SemaphoreType.DMA((2,)), pltpu.SemaphoreType.DMA((2,))],
                compiler_params=params(), cost_estimate=cost(60), name='update',
            )(*args)
            if last:
                et, g = res
            else:
                t4, v, hb, tb, nk, ns = res

        even = core[0] == 0
        rg = jnp.where(even, jnp.concatenate(rel_grads, axis=0), jnp.concatenate(rel_grads[::-1], axis=0))
        new_vr = vr + jnp.mean(rg * rg, axis=0, keepdims=True)
        new_r = rfm - LEARN_RATE * rg / jnp.sqrt(new_vr + ADA_EPS)
        return et.T, g.reshape(rows), new_r[:, :num_rel].T, new_vr[0, :num_rel], jnp.stack(losses)[None, :]

    return jax.shard_map(device_fn, mesh=mesh,
                         in_specs=(row_spec, flat_spec, rel_spec, state_spec, edge_spec, edge_spec, edge_spec, edge_spec, rel_spec),
                         out_specs=(row_spec, flat_spec, rel_spec, state_spec, row_spec), check_vma=False)
```

```python
import functools

import jax
import jax.numpy as jnp
from jax import lax
from jax.experimental import pallas as pl
from jax.experimental.pallas import tpu as pltpu
from jax.sharding import PartitionSpec as P


LEARN_RATE = 0.05
ADA_EPS = 1e-10
LANES = 128
SLICES = 4
CHUNK = 256
BATCH = 4
F32 = jnp.float32
BF16 = jnp.bfloat16


def ceil_to(value, unit):
    return -(-value // unit) * unit


def vmem():
    return pl.BlockSpec(memory_space=pltpu.VMEM)


def smem():
    return pl.BlockSpec(memory_space=pltpu.SMEM)


def hbm():
    return pl.BlockSpec(memory_space=pltpu.MemorySpace.HBM)


def four(index):
    return pl.multiple_of(index, SLICES)


def gather_rows(src, ids, base, stage, count):
    for k in range(count):
        stage[pl.ds(SLICES * k, SLICES), :] = src[pl.ds(four(ids[base + k]), SLICES), :]


def stage_cols(stage, slice_no):
    return stage[pl.ds(slice_no, LANES, stride=SLICES), :].T


def add_rows(acc, ids, base, rows, row_base, count):
    for first in range(0, count, BATCH):
        index = [ids[base + first + k] for k in range(BATCH)]
        grads = [rows[pl.ds(four(row_base + SLICES * (first + k)), SLICES), :] for k in range(BATCH)]
        total = [acc[pl.ds(four(index[k]), SLICES), :] + grads[k] for k in range(BATCH)]
        for k in range(1, BATCH):
            for earlier in range(k):
                total[k] = total[k] + jnp.where(index[earlier] == index[k], grads[earlier], 0.0)
        for k in range(BATCH):
            acc[pl.ds(four(index[k]), SLICES), :] = total[k]


def zero_rows(ref, step=1024):
    rows = ref.shape[0]
    whole = rows // step

    def body(i, _):
        ref[pl.ds(pl.multiple_of(i * step, 8), step), :] = jnp.zeros((step, LANES), ref.dtype)
        return 0

    lax.fori_loop(0, whole, body, 0)
    if rows % step:
        ref[pl.ds(whole * step, rows % step), :] = jnp.zeros((rows % step, LANES), ref.dtype)


def gather_out(dim, table, ids, out, stage, count):
    def body(b, _):
        gather_rows(table, ids, b * LANES, stage, LANES)
        cols = pl.ds(pl.multiple_of(b * LANES, LANES), LANES)
        for j in range(SLICES):
            size = min(LANES, dim - j * LANES)
            out[pl.ds(j * LANES, size), cols] = stage_cols(stage, j)[:size].astype(BF16)
        return 0

    lax.fori_loop(0, count // LANES, body, 0)


def gather_negs(dim, core, table, negs, nk, ns, nbuf, stage):
    half = nbuf.shape[1] // 2
    gather_out(dim, table, negs, nbuf, stage, nbuf.shape[1])
    nk[...] = nbuf[:, pl.ds(pl.multiple_of(core * half, LANES), half)]
    ns[...] = nbuf[:, pl.ds(pl.multiple_of((1 - core) * half, LANES), half)]


def entry_kernel(dim, rows, core_ref, negs, et, g, t4_out, v_out, nk, ns,
                 t4, v, inbuf, stage, nbuf, in_sem, out_sem):
    cols = inbuf.shape[2]
    steps = rows // cols
    per = cols // LANES

    def fetch(step, slot):
        return pltpu.make_async_copy(et.at[:, pl.ds(pl.multiple_of(step * cols, LANES), cols)],
                                     inbuf.at[slot, pl.ds(0, dim)], in_sem.at[slot])

    fetch(0, 0).start()
    for slot in range(2):
        inbuf[slot, pl.ds(dim, SLICES * LANES - dim), :] = jnp.zeros((SLICES * LANES - dim, cols), F32)
    t4[pl.ds(rows * SLICES, 32), :] = jnp.zeros((32, LANES), F32)

    def body(step, _):
        slot = lax.rem(step, 2)

        @pl.when(step + 1 < steps)
        def _():
            fetch(step + 1, 1 - slot).start()

        fetch(step, slot).wait()
        for b in range(per):
            row0 = (step * per + b) * LANES
            for j in range(SLICES):
                t4[pl.ds(SLICES * row0 + j, LANES, stride=SLICES), :] = inbuf[slot, pl.ds(j * LANES, LANES), pl.ds(b * LANES, LANES)].T
            v[pl.ds(pl.multiple_of(row0, 8), LANES), :] = jnp.broadcast_to(g[pl.ds(step * per + b, 1), :], (LANES, LANES)).T
        return 0

    lax.fori_loop(0, steps, body, 0)
    save_t = pltpu.make_async_copy(t4.at[pl.ds(0, rows * SLICES)], t4_out, out_sem.at[0])
    save_v = pltpu.make_async_copy(v, v_out, out_sem.at[1])
    save_t.start()
    save_v.start()
    gather_negs(dim, core_ref[0], t4, negs, nk, ns, nbuf, stage)
    save_t.wait()
    save_v.wait()


def gather_kernel(dim, lists, *refs):
    ids, t4_in, outs = refs[:lists], refs[lists], refs[lists + 1:2 * lists + 1]
    t4, stage, sem = refs[2 * lists + 1:]
    load = pltpu.make_async_copy(t4_in, t4, sem)
    load.start()
    load.wait()
    for i in range(lists):
        gather_out(dim, t4, ids[i], outs[i], stage, outs[i].shape[1])


def query_kernel(dim, edges, first, *refs):
    if first:
        core_ref, rel, hb, rfm, q_out, r_out, r4, stage, fm = refs
    else:
        core_ref, rel, hb, rfm_in, vr_in, rmine, rother, q_out, r_out, r4, rfm, vr, stage, fm = refs
        core = core_ref[0]
    half = dim // 2
    relp = rfm.shape[1]
    tops = SLICES * LANES
    if not first:
        fm[pl.ds(pl.multiple_of(core * half, 8), half), :] = rmine[...]
        fm[pl.ds(pl.multiple_of((1 - core) * half, 8), half), :] = rother[...]
        grad = fm[pl.ds(0, dim), :]
        vr[...] = vr_in[...] + jnp.sum(grad * grad, axis=0, keepdims=True) / dim
        rate = LEARN_RATE / jnp.sqrt(vr[...] + ADA_EPS)
        rfm[...] = rfm_in[...] - fm[pl.ds(0, dim), :] * rate
    fm[pl.ds(dim, tops - dim), pl.ds(0, LANES)] = jnp.zeros((tops - dim, LANES), F32)
    for b in range(relp // LANES):
        for j in range(SLICES):
            if (j + 1) * LANES <= dim:
                block = rfm[pl.ds(j * LANES, LANES), pl.ds(b * LANES, LANES)]
            else:
                fm[pl.ds(j * LANES, dim - j * LANES), pl.ds(0, LANES)] = rfm[pl.ds(j * LANES, dim - j * LANES), pl.ds(b * LANES, LANES)]
                block = fm[pl.ds(j * LANES, LANES), pl.ds(0, LANES)]
            r4[pl.ds(SLICES * b * LANES + j, LANES, stride=SLICES), :] = block.T

    def step(b, _):
        cols = pl.ds(pl.multiple_of(b * LANES, LANES), LANES)
        gather_rows(r4, rel, b * LANES, stage, LANES)
        for j in range(SLICES):
            size = min(LANES, dim - j * LANES)
            r_out[pl.ds(j * LANES, size), cols] = stage_cols(stage, j)[:size]
        h = hb[:, cols].astype(F32)
        r_re, r_im = r_out[pl.ds(0, half), cols], r_out[pl.ds(half, half), cols]
        q_out[pl.ds(0, half), cols] = h[:half] * r_re - h[half:] * r_im
        q_out[pl.ds(half, half), cols] = h[:half] * r_im + h[half:] * r_re
        return 0

    lax.fori_loop(0, edges // LANES, step, 0)


def place_negs(core, nb, nfull, nother):
    nhalf = nfull.shape[1]
    nb[:, pl.ds(pl.multiple_of(core * nhalf, LANES), nhalf)] = nfull[...]
    nb[:, pl.ds(pl.multiple_of((1 - core) * nhalf, LANES), nhalf)] = nother[...]


def score_kernel(dim, neg_count, edges, core_ref, w, q, tb, nfull, nother,
                 loss, dp_out, ds, nk, ns, nb, nbt, sc, ng, fm):
    core = core_ref[0]
    half = dim // 2
    negp = nb.shape[1]
    place_negs(core, nb, nfull, nother)
    for b in range(negp // LANES):
        nbt[pl.ds(b * LANES, LANES), :] = nb[:, pl.ds(b * LANES, LANES)].astype(F32).T.astype(BF16)
    ng[...] = jnp.zeros(ng.shape, F32)
    ds[pl.ds(neg_count, negp - neg_count), :] = jnp.zeros((negp - neg_count, edges), BF16)

    def step(c, loss_row):
        cols = pl.ds(pl.multiple_of(c * CHUNK, LANES), CHUNK)
        qb = q[:, cols].astype(BF16)
        pos = jnp.sum(q[:, cols] * tb[:, cols].astype(F32), axis=0, keepdims=True)
        sc[...] = lax.dot_general(nbt[...], qb, (((1,), (0,)), ((), ())), preferred_element_type=F32)
        top = jnp.maximum(pos, jnp.max(sc[pl.ds(0, neg_count), :], axis=0, keepdims=True))
        pos_exp = jnp.exp(pos - top)
        norm = pos_exp
        part = 200
        for i in range(0, neg_count, part):
            size = min(part, neg_count - i)
            e = jnp.exp(sc[pl.ds(i, size), :] - top)
            sc[pl.ds(i, size), :] = e
            norm = norm + jnp.sum(e, axis=0, keepdims=True)
        wt = w[:, cols]
        loss_row = loss_row + wt * (top + jnp.log(norm) - pos)
        dp_out[:, cols] = wt * (pos_exp / norm - 1.0)
        scale = wt / norm
        ds[pl.ds(0, neg_count), cols] = (sc[pl.ds(0, neg_count), :] * scale).astype(BF16)
        ng[...] += lax.dot_general(ds[:, cols], qb, (((1,), (1,)), ((), ())), preferred_element_type=F32)
        return loss_row

    loss_row = lax.fori_loop(0, edges // CHUNK, step, jnp.zeros((1, CHUNK), F32))
    loss[...] = jnp.broadcast_to(jnp.sum(loss_row, axis=1, keepdims=True) / edges, loss.shape)
    for b in range(negp // LANES):
        for j in range(SLICES):
            size = min(LANES, dim - j * LANES)
            fm[pl.ds(j * LANES, size), pl.ds(b * LANES, LANES)] = ng[pl.ds(b * LANES, LANES), pl.ds(j * LANES, size)].T
    nk[...] = fm[pl.ds(pl.multiple_of(core * half, 8), half), :]
    ns[...] = fm[pl.ds(pl.multiple_of((1 - core) * half, 8), half), :]


def grad_kernel(dim, edges, core_ref, rel, ds, dp, tb, hb, r, nfull, nother,
                hg, rk, rs, nb, racc, stage, qs, fm):
    core = core_ref[0]
    half = dim // 2
    relp = rk.shape[1]
    tops = SLICES * LANES
    place_negs(core, nb, nfull, nother)
    zero_rows(racc)
    qs[pl.ds(dim, tops - dim), :] = jnp.zeros((tops - dim, CHUNK), F32)

    def step(c, _):
        cols = pl.ds(pl.multiple_of(c * CHUNK, LANES), CHUNK)
        gq = lax.dot_general(nb[...], ds[:, cols], (((1,), (0,)), ((), ())), preferred_element_type=F32) + dp[:, cols] * tb[:, cols].astype(F32)
        g_re, g_im = gq[:half], gq[half:]
        h = hb[:, cols].astype(F32)
        h_re, h_im = h[:half], h[half:]
        qs[pl.ds(0, half), :] = g_re * h_re + g_im * h_im
        qs[pl.ds(half, half), :] = g_im * h_re - g_re * h_im
        for b in range(CHUNK // LANES):
            for j in range(SLICES):
                stage[pl.ds(SLICES * b * LANES + j, LANES, stride=SLICES), :] = qs[pl.ds(j * LANES, LANES), pl.ds(b * LANES, LANES)].T
        r_re, r_im = r[pl.ds(0, half), cols], r[pl.ds(half, half), cols]
        qs[pl.ds(0, half), :] = g_re * r_re + g_im * r_im
        qs[pl.ds(half, half), :] = g_im * r_re - g_re * r_im
        for b in range(CHUNK // LANES):
            for j in range(SLICES):
                hg[pl.ds(SLICES * (c * CHUNK + b * LANES) + j, LANES, stride=SLICES), :] = qs[pl.ds(j * LANES, LANES), pl.ds(b * LANES, LANES)].T
        add_rows(racc, rel, c * CHUNK, stage, 0, CHUNK)
        return 0

    lax.fori_loop(0, edges // CHUNK, step, 0)
    for b in range(relp // LANES):
        for j in range(SLICES):
            size = min(LANES, dim - j * LANES)
            fm[pl.ds(j * LANES, size), pl.ds(b * LANES, LANES)] = racc[pl.ds(SLICES * b * LANES + j, LANES, stride=SLICES), :].T[:size]
    rk[...] = fm[pl.ds(pl.multiple_of(core * half, 8), half), :]
    rs[...] = fm[pl.ds(pl.multiple_of((1 - core) * half, 8), half), :]


def unstage(rt, stage):
    for j in range(SLICES):
        stage[pl.ds(j, LANES, stride=SLICES), :] = rt[pl.ds(j * LANES, LANES), :].T


def scatter_kernel(dim, rows, edges, own, *refs):
    if own:
        heads, tails, hg, dp, q, acc_out, acc, stage, rt, sem = refs
    else:
        heads, tails, rel, hg, dp, hb_in, r4, acc_out, acc, stage, rt, sem = refs
    half = dim // 2
    tops = SLICES * LANES
    zero_rows(acc)
    rt[pl.ds(dim, tops - dim), :] = jnp.zeros((tops - dim, LANES), F32)

    def head_step(b, _):
        add_rows(acc, heads, b * 32, hg, b * 32 * SLICES, 32)
        return 0

    lax.fori_loop(0, edges // 32, head_step, 0)

    def tail_step(b, _):
        cols = pl.ds(pl.multiple_of(b * LANES, LANES), LANES)
        scale = dp[:, cols]
        if own:
            rt[pl.ds(0, dim), :] = q[:, cols] * scale
        else:
            gather_rows(r4, rel, b * LANES, stage, LANES)
            for j in range(SLICES):
                rt[pl.ds(j * LANES, LANES), :] = stage_cols(stage, j)
            h = hb_in[:, cols].astype(F32)
            r_re, r_im = rt[pl.ds(0, half), :], rt[pl.ds(half, half), :]
            q_re = scale * (h[:half] * r_re - h[half:] * r_im)
            q_im = scale * (h[:half] * r_im + h[half:] * r_re)
            rt[pl.ds(0, half), :] = q_re
            rt[pl.ds(half, half), :] = q_im
        unstage(rt, stage)
        add_rows(acc, tails, b * LANES, stage, 0, LANES)
        return 0

    lax.fori_loop(0, edges // LANES, tail_step, 0)
    save = pltpu.make_async_copy(acc.at[pl.ds(0, rows * SLICES)], acc_out, sem)
    save.start()
    save.wait()


def update_kernel(dim, rows, last, *refs):
    if last:
        (core_ref, negs, t4_in, v_in, acc_in, nmine, nother,
         et_out, g_out, t4, v, acc, stage, rt, outbuf, in_sem, out_sem) = refs
    else:
        (core_ref, negs, tails_n, negs_n, t4_in, v_in, acc_in, nmine, nother,
         t4_out, v_out, tb, nk, ns, t4, v, acc, stage, rt, nbuf, in_sem, out_sem) = refs
    core = core_ref[0]
    half = dim // 2
    tops = SLICES * LANES
    load_a = pltpu.make_async_copy(acc_in, acc.at[pl.ds(0, rows * SLICES)], in_sem.at[2])
    load_t = pltpu.make_async_copy(t4_in, t4.at[pl.ds(0, rows * SLICES)], in_sem.at[0])
    load_v = pltpu.make_async_copy(v_in, v, in_sem.at[1])
    load_a.start()
    load_t.start()
    load_v.start()
    acc[pl.ds(rows * SLICES, 32), :] = jnp.zeros((32, LANES), F32)
    t4[pl.ds(rows * SLICES, 32), :] = jnp.zeros((32, LANES), F32)
    rt[pl.ds(dim, tops - dim), :] = jnp.zeros((tops - dim, LANES), F32)
    load_a.wait()

    def neg_step(b, _):
        cols = pl.ds(pl.multiple_of(b * LANES, LANES), LANES)
        rt[pl.ds(pl.multiple_of(core * half, 8), half), :] = nmine[:, cols]
        rt[pl.ds(pl.multiple_of((1 - core) * half, 8), half), :] = nother[:, cols]
        unstage(rt, stage)
        add_rows(acc, negs, b * LANES, stage, 0, LANES)
        return 0

    lax.fori_loop(0, nmine.shape[1] // LANES, neg_step, 0)
    load_t.wait()
    load_v.wait()

    def ada_rows(row0, block):
        parts = [acc[pl.ds(SLICES * row0 + j, block, stride=SLICES), :] for j in range(SLICES)]
        square = parts[0] * parts[0]
        for j in range(1, SLICES):
            square = square + parts[j] * parts[j]
        vrows = pl.ds(pl.multiple_of(row0, 8), block)
        new_v = v[vrows, :] + jnp.sum(square, axis=1, keepdims=True) / dim
        v[vrows, :] = new_v
        rate = LEARN_RATE / jnp.sqrt(new_v + ADA_EPS)
        for j in range(SLICES):
            where = pl.ds(SLICES * row0 + j, block, stride=SLICES)
            t4[where, :] = t4[where, :] - acc[where, :] * rate

    if not last:
        def ada_step(b, _):
            ada_rows(b * LANES, LANES)
            return 0

        lax.fori_loop(0, rows // LANES, ada_step, 0)
        save_v = pltpu.make_async_copy(v, v_out, out_sem.at[1])
        save_t = pltpu.make_async_copy(t4.at[pl.ds(0, rows * SLICES)], t4_out, out_sem.at[0])
        save_v.start()
        gather_negs(dim, core, t4, negs_n, nk, ns, nbuf, stage)
        save_t.start()
        gather_out(dim, t4, tails_n, tb, stage, tb.shape[1])
        save_t.wait()
        save_v.wait()
        return

    width = outbuf.shape[2]
    per = width // LANES
    steps = rows // width

    def save(step, slot):
        return pltpu.make_async_copy(outbuf.at[slot], et_out.at[:, pl.ds(pl.multiple_of(step * width, LANES), width)], out_sem.at[slot])

    def exit_step(step, _):
        slot = lax.rem(step, 2)

        @pl.when(step >= 2)
        def _():
            save(step - 2, slot).wait()

        for b in range(per):
            row0 = (step * per + b) * LANES
            ada_rows(row0, LANES)
            for j in range(SLICES):
                size = min(LANES, dim - j * LANES)
                outbuf[slot, pl.ds(j * LANES, size), pl.ds(b * LANES, LANES)] = t4[pl.ds(SLICES * row0 + j, LANES, stride=SLICES), :].T[:size]
            g_out[pl.ds(step * per + b, 1), :] = v[pl.ds(pl.multiple_of(row0, 8), LANES), :].T[:1]
        save(step, slot).start()
        return 0

    lax.fori_loop(0, steps, exit_step, 0)
    save(steps - 2, (steps - 2) % 2).wait()
    save(steps - 1, (steps - 1) % 2).wait()


def params():
    return pltpu.CompilerParams(vmem_limit_bytes=63 * 1024 * 1024)


def cost(micros):
    return pl.CostEstimate(flops=int(micros * 5e6), bytes_accessed=0, transcendentals=0)


def shape(dims, dtype=F32):
    return jax.ShapeDtypeStruct(dims, dtype)


def solution(mesh):
    ent_size = mesh.shape['ent']
    row_spec = P(('sweep', 'ent'), None)
    flat_spec = P(('sweep', 'ent'))
    rel_spec = P('sweep', None)
    state_spec = P('sweep')
    edge_spec = P(('sweep', 'ent'), None, None)
    swap = [(i, i ^ 1) for i in range(ent_size)]
    cross = [(i, i ^ 2) for i in range(ent_size)]

    def shift(amount):
        return [(i, (i + amount) % ent_size) for i in range(ent_size)]

    tie = lax.optimization_barrier

    def chip_sum(keep, send):
        return keep + lax.ppermute(send, 'ent', swap)

    def send(value, pairs):
        return lax.ppermute(value, 'ent', pairs)

    def link(part):
        return send(part, cross)

    def finish(part, got):
        mine = part + got
        return mine, lax.ppermute(mine, 'ent', swap)

    def device_fn(ent_emb, ent_ada, rel_emb, rel_ada, head_idx, tail_idx, rel_idx, edge_mask, neg_idx):
        rows, dim = ent_emb.shape
        num_rel = rel_emb.shape[0]
        _, rounds, edges = head_idx.shape
        neg_count = neg_idx.shape[1]
        negp = ceil_to(neg_count, 2 * LANES)
        relp = ceil_to(num_rel, LANES)
        half = dim // 2
        my_dev = lax.axis_index('ent')
        core = (my_dev % 2).reshape(1)

        heads = [head_idx[0, s] * SLICES for s in range(rounds)]
        own_tails = [tail_idx[0, s] * SLICES for s in range(rounds)]
        own_rels = [rel_idx[0, s] * SLICES for s in range(rounds)]
        tails, rels = [own_tails[0]], [own_rels[0]]
        for s in range(1, rounds):
            got = lax.ppermute(jnp.stack([own_tails[s], own_rels[s]]), 'ent', shift(s))
            tails.append(got[0])
            rels.append(got[1])
        owned = (neg_idx // rows) == my_dev
        neg_local = jnp.where(owned, neg_idx % rows, rows) * SLICES
        neg_local = jnp.pad(neg_local, ((0, 0), (0, negp - neg_count)), constant_values=rows * SLICES)
        negs = [neg_local[s] for s in range(rounds)]
        weights = edge_mask[0].astype(F32)

        wide_rows = (rows + 8) * SLICES
        stage_shape = pltpu.VMEM((SLICES * LANES, LANES), F32)
        square_shape = pltpu.VMEM((SLICES * LANES, LANES), F32)
        table_shape = pltpu.VMEM((wide_rows, LANES), F32)
        cols_bf = shape((dim, edges), BF16)
        neg_half = shape((dim, negp // 2), BF16)

        def call(kernel, args, kinds, outs, out_kinds, scratch, micros):
            places = {'s': smem, 'h': hbm, 'v': vmem}
            return pl.pallas_call(
                kernel, out_shape=outs, in_specs=[places[k]() for k in kinds], out_specs=[places[k]() for k in out_kinds],
                scratch_shapes=scratch, compiler_params=params(), cost_estimate=cost(micros))(*args)

        def gather(lists, t4):
            return call(functools.partial(gather_kernel, dim, len(lists)), lists + [t4], 's' * len(lists) + 'h',
                        [cols_bf] * len(lists), 'v' * len(lists),
                        [pltpu.VMEM((rows * SLICES, LANES), F32), stage_shape, pltpu.SemaphoreType.DMA], 6 + 5 * len(lists))

        t4, v, nk, ns = call(
            functools.partial(entry_kernel, dim, rows), [core, negs[0], ent_emb.T, ent_ada.reshape(rows // LANES, LANES)], 'sshv',
            [shape((rows * SLICES, LANES)), shape((rows, LANES)), neg_half, neg_half], 'hhvv',
            [table_shape, pltpu.VMEM((rows, LANES), F32), pltpu.VMEM((2, SLICES * LANES, 4 * LANES), F32), stage_shape,
             pltpu.VMEM((dim, negp), BF16), pltpu.SemaphoreType.DMA((2,)), pltpu.SemaphoreType.DMA((2,))], 20)

        rfm = jnp.pad(rel_emb.T, ((0, 0), (0, relp - num_rel)))
        vr = jnp.pad(rel_ada, (0, relp - num_rel), constant_values=1.0).reshape(1, relp)
        losses = []
        rel_grads = None
        for s in range(rounds):
            first, last = s == 0, s == rounds - 1
            neg_part = chip_sum(nk, ns)
            if first:
                neg_part, t4, tails, rels = tie((neg_part, t4, tails, rels))
                neg_got = link(neg_part)
                tail_cols, hb = gather([tails[0], heads[0]], t4)
                head_cols = hb
                neg_got, hb = tie((neg_got, hb))
            else:
                neg_part, t4, tb = tie((neg_part, t4, tb))
                neg_got = link(neg_part)
                tail_cols = send(tb, shift(-s))
                hb, = gather([heads[s]], t4)
                head_cols = send(hb, shift(s))
                rel_got, hb = tie((rel_got, hb))
                rel_grads = finish(rel_part, rel_got)
            wide = shape((dim, edges))
            outs = [wide, wide, shape((relp * SLICES, LANES))]
            args = [core, own_rels[s], hb, rfm]
            if not first:
                outs += [shape((dim, relp)), shape((1, relp))]
                args += [vr] + list(rel_grads)
            res = call(functools.partial(query_kernel, dim, edges, first), args, 'ss' + 'v' * (len(args) - 2), outs, 'v' * len(outs),
                       [stage_shape, pltpu.VMEM((SLICES * LANES, relp), F32)], 10)
            q, r, r4 = res[:3]
            neg_got, q = tie((neg_got, q))
            nmine, nother = finish(neg_part, neg_got)
            if not first:
                rfm, vr = res[3:]
            loss, dp, ds, gk, gs = call(
                functools.partial(score_kernel, dim, neg_count, edges), [core, weights[s].reshape(1, edges), q, tail_cols, nmine, nother], 'svvvvv',
                [shape((1, LANES)), shape((1, edges)), shape((negp, edges), BF16), shape((half, negp)), shape((half, negp))], 'vvvvv',
                [pltpu.VMEM((dim, negp), BF16), pltpu.VMEM((negp, dim), BF16), pltpu.VMEM((negp, CHUNK), F32),
                 pltpu.VMEM((negp, dim), F32), pltpu.VMEM((SLICES * LANES, negp), F32)], 15)
            losses.append(loss[0, 0])
            neg_part = chip_sum(gk, gs)
            neg_part, ds = tie((neg_part, ds))
            neg_got = link(neg_part)
            hg, rk, rs = call(
                functools.partial(grad_kernel, dim, edges), [core, own_rels[s], ds, dp, tail_cols, hb, r, nmine, nother], 'ssvvvvvvv',
                [shape((edges * SLICES, LANES)), shape((half, relp)), shape((half, relp))], 'vvv',
                [pltpu.VMEM((dim, negp), BF16), pltpu.VMEM((relp * SLICES, LANES), F32), pltpu.VMEM((SLICES * CHUNK, LANES), F32),
                 pltpu.VMEM((SLICES * LANES, CHUNK), F32), pltpu.VMEM((SLICES * LANES, relp), F32)], 15)
            rel_part = chip_sum(rk, rs)
            rel_part, hg = tie((rel_part, hg))
            rel_got = link(rel_part)
            if first:
                args, kinds = [heads[s], tails[s], hg, dp, q], 'ssvvv'
            else:
                dp = lax.ppermute(dp, 'ent', shift(s))
                args, kinds = [heads[s], tails[s], rels[s], hg, dp, head_cols, r4], 'sssvvvv'
            acc, = call(functools.partial(scatter_kernel, dim, rows, edges, first), args, kinds, [shape((rows * SLICES, LANES))], 'h',
                        [table_shape, stage_shape, square_shape, pltpu.SemaphoreType.DMA], 25)
            neg_got, acc = tie((neg_got, acc))
            gmine, gother = finish(neg_part, neg_got)
            scratch = [table_shape, pltpu.VMEM((rows, LANES), F32), table_shape, stage_shape, square_shape]
            if last:
                args, kinds = [core, negs[s]], 'sshhhvv'
                outs, out_kinds = [shape((dim, rows)), shape((rows // LANES, LANES))], 'hv'
                scratch += [pltpu.VMEM((2, dim, 4 * LANES), F32)]
            else:
                args, kinds = [core, negs[s], tails[s + 1], negs[s + 1]], 'sssshhhvv'
                outs, out_kinds = [shape((rows * SLICES, LANES)), shape((rows, LANES)), cols_bf, neg_half, neg_half], 'hhvvv'
                scratch += [pltpu.VMEM((dim, negp), BF16)]
            res = call(functools.partial(update_kernel, dim, rows, last), args + [t4, v, acc, gmine, gother], kinds, outs, out_kinds,
                       scratch + [pltpu.SemaphoreType.DMA((3,)), pltpu.SemaphoreType.DMA((2,))], 30)
            if last:
                et, g = res
            else:
                t4, v, tb, nk, ns = res

        even = core[0] == 0
        rel_grads = finish(rel_part, rel_got)
        rg = jnp.where(even, jnp.concatenate(rel_grads, axis=0), jnp.concatenate(rel_grads[::-1], axis=0))
        new_vr = vr + jnp.mean(rg * rg, axis=0, keepdims=True)
        new_r = rfm - LEARN_RATE * rg / jnp.sqrt(new_vr + ADA_EPS)
        return et.T, g.reshape(rows), new_r[:, :num_rel].T, new_vr[0, :num_rel], jnp.stack(losses)[None, :]

    return jax.shard_map(device_fn, mesh=mesh,
                         in_specs=(row_spec, flat_spec, rel_spec, state_spec, edge_spec, edge_spec, edge_spec, edge_spec, rel_spec),
                         out_specs=(row_spec, flat_spec, rel_spec, state_spec, row_spec), check_vma=False)
```

```python
import functools

import jax
import jax.numpy as jnp
from jax import lax
from jax.experimental import pallas as pl
from jax.experimental.pallas import tpu as pltpu
from jax.sharding import PartitionSpec as P


LEARN_RATE = 0.05
ADA_EPS = 1e-10
LANES = 128
SLICES = 4
CHUNK = 256
BATCH = 4
F32 = jnp.float32
BF16 = jnp.bfloat16


def ceil_to(value, unit):
    return -(-value // unit) * unit


def vmem():
    return pl.BlockSpec(memory_space=pltpu.VMEM)


def smem():
    return pl.BlockSpec(memory_space=pltpu.SMEM)


def hbm():
    return pl.BlockSpec(memory_space=pltpu.MemorySpace.HBM)


def four(index):
    return pl.multiple_of(index, SLICES)


def gather_rows(src, ids, base, stage, count):
    for k in range(count):
        stage[pl.ds(SLICES * k, SLICES), :] = src[pl.ds(four(ids[base + k]), SLICES), :]


def stage_cols(stage, slice_no):
    return stage[pl.ds(slice_no, LANES, stride=SLICES), :].T


def add_rows(acc, ids, base, rows, row_base, count):
    for first in range(0, count, BATCH):
        index = [ids[base + first + k] for k in range(BATCH)]
        grads = [rows[pl.ds(four(row_base + SLICES * (first + k)), SLICES), :] for k in range(BATCH)]
        total = [acc[pl.ds(four(index[k]), SLICES), :] + grads[k] for k in range(BATCH)]
        for k in range(1, BATCH):
            for earlier in range(k):
                total[k] = total[k] + jnp.where(index[earlier] == index[k], grads[earlier], 0.0)
        for k in range(BATCH):
            acc[pl.ds(four(index[k]), SLICES), :] = total[k]


def zero_rows(ref, step=1024):
    rows = ref.shape[0]
    whole = rows // step

    def body(i, _):
        ref[pl.ds(pl.multiple_of(i * step, 8), step), :] = jnp.zeros((step, LANES), ref.dtype)
        return 0

    lax.fori_loop(0, whole, body, 0)
    if rows % step:
        ref[pl.ds(whole * step, rows % step), :] = jnp.zeros((rows % step, LANES), ref.dtype)


def gather_out(dim, table, ids, out, stage, count):
    def body(b, _):
        gather_rows(table, ids, b * LANES, stage, LANES)
        cols = pl.ds(pl.multiple_of(b * LANES, LANES), LANES)
        for j in range(SLICES):
            size = min(LANES, dim - j * LANES)
            out[pl.ds(j * LANES, size), cols] = stage_cols(stage, j)[:size].astype(BF16)
        return 0

    lax.fori_loop(0, count // LANES, body, 0)


def gather_negs(dim, core, table, negs, nk, ns, nbuf, stage):
    half = nbuf.shape[1] // 2
    gather_out(dim, table, negs, nbuf, stage, nbuf.shape[1])
    nk[...] = nbuf[:, pl.ds(pl.multiple_of(core * half, LANES), half)]
    ns[...] = nbuf[:, pl.ds(pl.multiple_of((1 - core) * half, LANES), half)]


def entry_kernel(dim, rows, core_ref, negs, et, g, t4, v, nk, ns, inbuf, stage, nbuf, in_sem):
    cols = inbuf.shape[2]
    steps = rows // cols
    per = cols // LANES

    def fetch(step, slot):
        return pltpu.make_async_copy(et.at[:, pl.ds(pl.multiple_of(step * cols, LANES), cols)],
                                     inbuf.at[slot, pl.ds(0, dim)], in_sem.at[slot])

    fetch(0, 0).start()
    for slot in range(2):
        inbuf[slot, pl.ds(dim, SLICES * LANES - dim), :] = jnp.zeros((SLICES * LANES - dim, cols), F32)
    t4[pl.ds(rows * SLICES, 32), :] = jnp.zeros((32, LANES), F32)

    def body(step, _):
        slot = lax.rem(step, 2)

        @pl.when(step + 1 < steps)
        def _():
            fetch(step + 1, 1 - slot).start()

        fetch(step, slot).wait()
        for b in range(per):
            row0 = (step * per + b) * LANES
            for j in range(SLICES):
                t4[pl.ds(SLICES * row0 + j, LANES, stride=SLICES), :] = inbuf[slot, pl.ds(j * LANES, LANES), pl.ds(b * LANES, LANES)].T
            v[pl.ds(pl.multiple_of(row0, 8), LANES), :] = jnp.broadcast_to(g[pl.ds(step * per + b, 1), :], (LANES, LANES)).T
        return 0

    lax.fori_loop(0, steps, body, 0)
    gather_negs(dim, core_ref[0], t4, negs, nk, ns, nbuf, stage)


def gather_kernel(dim, lists, *refs):
    ids, t4, outs, stage = refs[:lists], refs[lists], refs[lists + 1:2 * lists + 1], refs[2 * lists + 1]
    for i in range(lists):
        gather_out(dim, t4, ids[i], outs[i], stage, outs[i].shape[1])


def query_kernel(dim, edges, first, *refs):
    if first:
        core_ref, rel, hb, rfm, q_out, r_out, r4, stage, fm = refs
    else:
        core_ref, rel, hb, rfm_in, vr_in, rmine, rother, q_out, r_out, r4, rfm, vr, stage, fm = refs
        core = core_ref[0]
    half = dim // 2
    relp = rfm.shape[1]
    tops = SLICES * LANES
    if not first:
        fm[pl.ds(pl.multiple_of(core * half, 8), half), :] = rmine[...]
        fm[pl.ds(pl.multiple_of((1 - core) * half, 8), half), :] = rother[...]
        grad = fm[pl.ds(0, dim), :]
        vr[...] = vr_in[...] + jnp.sum(grad * grad, axis=0, keepdims=True) / dim
        rate = LEARN_RATE / jnp.sqrt(vr[...] + ADA_EPS)
        rfm[...] = rfm_in[...] - fm[pl.ds(0, dim), :] * rate
    fm[pl.ds(dim, tops - dim), pl.ds(0, LANES)] = jnp.zeros((tops - dim, LANES), F32)
    for b in range(relp // LANES):
        for j in range(SLICES):
            if (j + 1) * LANES <= dim:
                block = rfm[pl.ds(j * LANES, LANES), pl.ds(b * LANES, LANES)]
            else:
                fm[pl.ds(j * LANES, dim - j * LANES), pl.ds(0, LANES)] = rfm[pl.ds(j * LANES, dim - j * LANES), pl.ds(b * LANES, LANES)]
                block = fm[pl.ds(j * LANES, LANES), pl.ds(0, LANES)]
            r4[pl.ds(SLICES * b * LANES + j, LANES, stride=SLICES), :] = block.T

    def step(b, _):
        cols = pl.ds(pl.multiple_of(b * LANES, LANES), LANES)
        gather_rows(r4, rel, b * LANES, stage, LANES)
        for j in range(SLICES):
            size = min(LANES, dim - j * LANES)
            r_out[pl.ds(j * LANES, size), cols] = stage_cols(stage, j)[:size]
        h = hb[:, cols].astype(F32)
        r_re, r_im = r_out[pl.ds(0, half), cols], r_out[pl.ds(half, half), cols]
        q_out[pl.ds(0, half), cols] = h[:half] * r_re - h[half:] * r_im
        q_out[pl.ds(half, half), cols] = h[:half] * r_im + h[half:] * r_re
        return 0

    lax.fori_loop(0, edges // LANES, step, 0)


def place_negs(core, nb, nfull, nother):
    nhalf = nfull.shape[1]
    nb[:, pl.ds(pl.multiple_of(core * nhalf, LANES), nhalf)] = nfull[...]
    nb[:, pl.ds(pl.multiple_of((1 - core) * nhalf, LANES), nhalf)] = nother[...]


def score_kernel(dim, neg_count, edges, core_ref, w, q, tb, nfull, nother,
                 loss, dp_out, ds, nk, ns, nb, nbt, sc, ng, fm):
    core = core_ref[0]
    half = dim // 2
    negp = nb.shape[1]
    place_negs(core, nb, nfull, nother)
    for b in range(negp // LANES):
        nbt[pl.ds(b * LANES, LANES), :] = nb[:, pl.ds(b * LANES, LANES)].astype(F32).T.astype(BF16)
    ng[...] = jnp.zeros(ng.shape, F32)
    ds[pl.ds(neg_count, negp - neg_count), :] = jnp.zeros((negp - neg_count, edges), BF16)

    def step(c, loss_row):
        cols = pl.ds(pl.multiple_of(c * CHUNK, LANES), CHUNK)
        qb = q[:, cols].astype(BF16)
        pos = jnp.sum(q[:, cols] * tb[:, cols].astype(F32), axis=0, keepdims=True)
        sc[...] = lax.dot_general(nbt[...], qb, (((1,), (0,)), ((), ())), preferred_element_type=F32)
        top = jnp.maximum(pos, jnp.max(sc[pl.ds(0, neg_count), :], axis=0, keepdims=True))
        pos_exp = jnp.exp(pos - top)
        norm = pos_exp
        part = 200
        for i in range(0, neg_count, part):
            size = min(part, neg_count - i)
            e = jnp.exp(sc[pl.ds(i, size), :] - top)
            sc[pl.ds(i, size), :] = e
            norm = norm + jnp.sum(e, axis=0, keepdims=True)
        wt = w[:, cols]
        loss_row = loss_row + wt * (top + jnp.log(norm) - pos)
        dp_out[:, cols] = wt * (pos_exp / norm - 1.0)
        scale = wt / norm
        ds[pl.ds(0, neg_count), cols] = (sc[pl.ds(0, neg_count), :] * scale).astype(BF16)
        ng[...] += lax.dot_general(ds[:, cols], qb, (((1,), (1,)), ((), ())), preferred_element_type=F32)
        return loss_row

    loss_row = lax.fori_loop(0, edges // CHUNK, step, jnp.zeros((1, CHUNK), F32))
    loss[...] = jnp.broadcast_to(jnp.sum(loss_row, axis=1, keepdims=True) / edges, loss.shape)
    for b in range(negp // LANES):
        for j in range(SLICES):
            size = min(LANES, dim - j * LANES)
            fm[pl.ds(j * LANES, size), pl.ds(b * LANES, LANES)] = ng[pl.ds(b * LANES, LANES), pl.ds(j * LANES, size)].T
    nk[...] = fm[pl.ds(pl.multiple_of(core * half, 8), half), :]
    ns[...] = fm[pl.ds(pl.multiple_of((1 - core) * half, 8), half), :]


def grad_kernel(dim, edges, core_ref, rel, ds, dp, tb, hb, r, nfull, nother,
                hg, rk, rs, nb, racc, stage, qs, fm):
    core = core_ref[0]
    half = dim // 2
    relp = rk.shape[1]
    tops = SLICES * LANES
    place_negs(core, nb, nfull, nother)
    zero_rows(racc)
    qs[pl.ds(dim, tops - dim), :] = jnp.zeros((tops - dim, CHUNK), F32)

    def step(c, _):
        cols = pl.ds(pl.multiple_of(c * CHUNK, LANES), CHUNK)
        gq = lax.dot_general(nb[...], ds[:, cols], (((1,), (0,)), ((), ())), preferred_element_type=F32) + dp[:, cols] * tb[:, cols].astype(F32)
        g_re, g_im = gq[:half], gq[half:]
        h = hb[:, cols].astype(F32)
        h_re, h_im = h[:half], h[half:]
        qs[pl.ds(0, half), :] = g_re * h_re + g_im * h_im
        qs[pl.ds(half, half), :] = g_im * h_re - g_re * h_im
        for b in range(CHUNK // LANES):
            for j in range(SLICES):
                stage[pl.ds(SLICES * b * LANES + j, LANES, stride=SLICES), :] = qs[pl.ds(j * LANES, LANES), pl.ds(b * LANES, LANES)].T
        r_re, r_im = r[pl.ds(0, half), cols], r[pl.ds(half, half), cols]
        qs[pl.ds(0, half), :] = g_re * r_re + g_im * r_im
        qs[pl.ds(half, half), :] = g_im * r_re - g_re * r_im
        for b in range(CHUNK // LANES):
            for j in range(SLICES):
                hg[pl.ds(SLICES * (c * CHUNK + b * LANES) + j, LANES, stride=SLICES), :] = qs[pl.ds(j * LANES, LANES), pl.ds(b * LANES, LANES)].T
        add_rows(racc, rel, c * CHUNK, stage, 0, CHUNK)
        return 0

    lax.fori_loop(0, edges // CHUNK, step, 0)
    for b in range(relp // LANES):
        for j in range(SLICES):
            size = min(LANES, dim - j * LANES)
            fm[pl.ds(j * LANES, size), pl.ds(b * LANES, LANES)] = racc[pl.ds(SLICES * b * LANES + j, LANES, stride=SLICES), :].T[:size]
    rk[...] = fm[pl.ds(pl.multiple_of(core * half, 8), half), :]
    rs[...] = fm[pl.ds(pl.multiple_of((1 - core) * half, 8), half), :]


def unstage(rt, stage):
    for j in range(SLICES):
        stage[pl.ds(j, LANES, stride=SLICES), :] = rt[pl.ds(j * LANES, LANES), :].T


def scatter_kernel(dim, edges, own, *refs):
    if own:
        heads, tails, hg, dp, q, acc, stage, rt = refs
    else:
        heads, tails, rel, hg, dp, hb_in, r4, acc, stage, rt = refs
    half = dim // 2
    tops = SLICES * LANES
    zero_rows(acc)
    rt[pl.ds(dim, tops - dim), :] = jnp.zeros((tops - dim, LANES), F32)

    def head_step(b, _):
        add_rows(acc, heads, b * 32, hg, b * 32 * SLICES, 32)
        return 0

    lax.fori_loop(0, edges // 32, head_step, 0)

    def tail_step(b, _):
        cols = pl.ds(pl.multiple_of(b * LANES, LANES), LANES)
        scale = dp[:, cols]
        if own:
            rt[pl.ds(0, dim), :] = q[:, cols] * scale
        else:
            gather_rows(r4, rel, b * LANES, stage, LANES)
            for j in range(SLICES):
                rt[pl.ds(j * LANES, LANES), :] = stage_cols(stage, j)
            h = hb_in[:, cols].astype(F32)
            r_re, r_im = rt[pl.ds(0, half), :], rt[pl.ds(half, half), :]
            q_re = scale * (h[:half] * r_re - h[half:] * r_im)
            q_im = scale * (h[:half] * r_im + h[half:] * r_re)
            rt[pl.ds(0, half), :] = q_re
            rt[pl.ds(half, half), :] = q_im
        unstage(rt, stage)
        add_rows(acc, tails, b * LANES, stage, 0, LANES)
        return 0

    lax.fori_loop(0, edges // LANES, tail_step, 0)


def update_kernel(dim, rows, last, *refs):
    if last:
        core_ref, negs, t4, v, _, nmine, nother, acc, et_out, g_out, stage, rt, outbuf, out_sem = refs
    else:
        core_ref, negs, tails_n, negs_n, t4, v, _, nmine, nother, acc, new_t4, new_v, tb, nk, ns, stage, rt, nbuf = refs
    core = core_ref[0]
    half = dim // 2
    tops = SLICES * LANES
    rt[pl.ds(dim, tops - dim), :] = jnp.zeros((tops - dim, LANES), F32)

    def neg_step(b, _):
        cols = pl.ds(pl.multiple_of(b * LANES, LANES), LANES)
        rt[pl.ds(pl.multiple_of(core * half, 8), half), :] = nmine[:, cols]
        rt[pl.ds(pl.multiple_of((1 - core) * half, 8), half), :] = nother[:, cols]
        unstage(rt, stage)
        add_rows(acc, negs, b * LANES, stage, 0, LANES)
        return 0

    lax.fori_loop(0, nmine.shape[1] // LANES, neg_step, 0)

    def ada_rows(row0):
        where = [pl.ds(SLICES * row0 + j, LANES, stride=SLICES) for j in range(SLICES)]
        square = acc[where[0], :] * acc[where[0], :]
        for j in range(1, SLICES):
            square = square + acc[where[j], :] * acc[where[j], :]
        state = v[pl.ds(pl.multiple_of(row0, 8), LANES), :] + jnp.sum(square, axis=1, keepdims=True) / dim
        rate = LEARN_RATE / jnp.sqrt(state + ADA_EPS)
        return state, where, [t4[w, :] - acc[w, :] * rate for w in where]

    if not last:
        def ada_step(b, _):
            state, where, values = ada_rows(b * LANES)
            new_v[pl.ds(pl.multiple_of(b * LANES, 8), LANES), :] = state
            for w, value in zip(where, values):
                new_t4[w, :] = value
            return 0

        lax.fori_loop(0, rows // LANES, ada_step, 0)
        new_t4[pl.ds(rows * SLICES, 32), :] = jnp.zeros((32, LANES), F32)
        gather_negs(dim, core, new_t4, negs_n, nk, ns, nbuf, stage)
        gather_out(dim, new_t4, tails_n, tb, stage, tb.shape[1])
        return

    width = outbuf.shape[2]
    per = width // LANES
    steps = rows // width

    def save(step, slot):
        return pltpu.make_async_copy(outbuf.at[slot], et_out.at[:, pl.ds(pl.multiple_of(step * width, LANES), width)], out_sem.at[slot])

    def exit_step(step, _):
        slot = lax.rem(step, 2)

        @pl.when(step >= 2)
        def _():
            save(step - 2, slot).wait()

        for b in range(per):
            state, _, values = ada_rows((step * per + b) * LANES)
            for j in range(SLICES):
                size = min(LANES, dim - j * LANES)
                outbuf[slot, pl.ds(j * LANES, size), pl.ds(b * LANES, LANES)] = values[j].T[:size]
            g_out[pl.ds(step * per + b, 1), :] = state.T[:1]
        save(step, slot).start()
        return 0

    lax.fori_loop(0, steps, exit_step, 0)
    save(steps - 2, (steps - 2) % 2).wait()
    save(steps - 1, (steps - 1) % 2).wait()


def padded_bytes(dims, dtype):
    size = jnp.dtype(dtype).itemsize
    dims = (1,) * (2 - len(dims)) + tuple(dims)
    total = ceil_to(dims[-2], 32 // size) * ceil_to(dims[-1], LANES) * size
    for d in dims[:-2]:
        total *= d
    return total


def cost(micros):
    return pl.CostEstimate(flops=int(micros * 5e6), bytes_accessed=0, transcendentals=0)


def shape(dims, dtype=F32):
    return jax.ShapeDtypeStruct(dims, dtype)


def solution(mesh):
    ent_size = mesh.shape['ent']
    row_spec = P(('sweep', 'ent'), None)
    flat_spec = P(('sweep', 'ent'))
    rel_spec = P('sweep', None)
    state_spec = P('sweep')
    edge_spec = P(('sweep', 'ent'), None, None)
    swap = [(i, i ^ 1) for i in range(ent_size)]
    cross = [(i, i ^ 2) for i in range(ent_size)]

    def shift(amount):
        return [(i, (i + amount) % ent_size) for i in range(ent_size)]

    tie = lax.optimization_barrier

    def chip_sum(keep, send):
        return keep + lax.ppermute(send, 'ent', swap)

    def send(value, pairs):
        return lax.ppermute(value, 'ent', pairs)

    def link(part):
        return send(part, cross)

    def finish(part, got):
        mine = part + got
        return mine, lax.ppermute(mine, 'ent', swap)

    def device_fn(ent_emb, ent_ada, rel_emb, rel_ada, head_idx, tail_idx, rel_idx, edge_mask, neg_idx):
        rows, dim = ent_emb.shape
        num_rel = rel_emb.shape[0]
        _, rounds, edges = head_idx.shape
        neg_count = neg_idx.shape[1]
        negp = ceil_to(neg_count, 2 * LANES)
        relp = ceil_to(num_rel, LANES)
        half = dim // 2
        my_dev = lax.axis_index('ent')
        core = (my_dev % 2).reshape(1)

        heads = [head_idx[0, s] * SLICES for s in range(rounds)]
        own_tails = [tail_idx[0, s] * SLICES for s in range(rounds)]
        own_rels = [rel_idx[0, s] * SLICES for s in range(rounds)]
        tails, rels = [own_tails[0]], [own_rels[0]]
        for s in range(1, rounds):
            got = lax.ppermute(jnp.stack([own_tails[s], own_rels[s]]), 'ent', shift(s))
            tails.append(got[0])
            rels.append(got[1])
        owned = (neg_idx // rows) == my_dev
        neg_local = jnp.where(owned, neg_idx % rows, rows) * SLICES
        neg_local = jnp.pad(neg_local, ((0, 0), (0, negp - neg_count)), constant_values=rows * SLICES)
        negs = [neg_local[s] for s in range(rounds)]
        weights = edge_mask[0].astype(F32)

        wide_rows = (rows + 8) * SLICES
        stage_shape = pltpu.VMEM((SLICES * LANES, LANES), F32)
        square_shape = pltpu.VMEM((SLICES * LANES, LANES), F32)
        table_out, state_out = shape((wide_rows, LANES)), shape((rows, LANES))
        cols_bf = shape((dim, edges), BF16)
        neg_half = shape((dim, negp // 2), BF16)

        def call(kernel, args, kinds, outs, out_kinds, scratch, micros, aliases=None):
            places = {'s': smem, 'h': hbm, 'v': vmem, 'V': vmem}
            windows = [a for a, k in zip(list(args) + outs, kinds + out_kinds) if k == 'v']
            limit = 3 * 2 ** 20 + sum(padded_bytes(a.shape, a.dtype) for a in windows)
            limit += sum(padded_bytes(a.shape, a.dtype) for a in scratch if a.memory_space == pltpu.VMEM)
            args = [pltpu.with_memory_space_constraint(a, pltpu.VMEM) if k == 'V' else a for a, k in zip(args, kinds)]
            outs = [pltpu.VMEM(o.shape, o.dtype) if k == 'V' else o for o, k in zip(outs, out_kinds)]
            return pl.pallas_call(
                kernel, out_shape=outs, in_specs=[places[k]() for k in kinds], out_specs=[places[k]() for k in out_kinds],
                scratch_shapes=scratch, compiler_params=pltpu.CompilerParams(vmem_limit_bytes=limit),
                input_output_aliases=aliases or {}, cost_estimate=cost(micros))(*args)

        def gather(lists, t4):
            return call(functools.partial(gather_kernel, dim, len(lists)), lists + [t4], 's' * len(lists) + 'V',
                        [cols_bf] * len(lists), 'V' * len(lists), [stage_shape], 1 + 5 * len(lists))

        t4, v, nk, ns = call(
            functools.partial(entry_kernel, dim, rows), [core, negs[0], ent_emb.T, ent_ada.reshape(rows // LANES, LANES)], 'sshv',
            [table_out, state_out, neg_half, neg_half], 'VVVV',
            [pltpu.VMEM((2, SLICES * LANES, 4 * LANES), F32), stage_shape, pltpu.VMEM((dim, negp), BF16), pltpu.SemaphoreType.DMA((2,))], 20)

        rfm = jnp.pad(rel_emb.T, ((0, 0), (0, relp - num_rel)))
        vr = jnp.pad(rel_ada, (0, relp - num_rel), constant_values=1.0).reshape(1, relp)
        losses = []
        rel_grads = None
        for s in range(rounds):
            first, last = s == 0, s == rounds - 1
            neg_part = chip_sum(nk, ns)
            if first:
                neg_part, t4, tails, rels = tie((neg_part, t4, tails, rels))
                neg_got = link(neg_part)
                tail_cols, hb = gather([tails[0], heads[0]], t4)
                head_cols = hb
                neg_got, hb = tie((neg_got, hb))
            else:
                neg_part, t4, tb = tie((neg_part, t4, tb))
                neg_got = link(neg_part)
                tail_cols = send(tb, shift(-s))
                hb, = gather([heads[s]], t4)
                head_cols = send(hb, shift(s))
                rel_got, hb = tie((rel_got, hb))
                rel_grads = finish(rel_part, rel_got)
            wide = shape((dim, edges))
            outs, out_kinds = [wide, wide, shape((relp * SLICES, LANES))], 'VVV'
            args, kinds = [core, own_rels[s], hb, rfm], 'ssV' + ('v' if first else 'V')
            if not first:
                outs += [shape((dim, relp)), shape((1, relp))]
                out_kinds += 'Vv'
                args += [vr] + list(rel_grads)
                kinds += 'vVV'
            res = call(functools.partial(query_kernel, dim, edges, first), args, kinds, outs, out_kinds,
                       [stage_shape, pltpu.VMEM((SLICES * LANES, relp), F32)], 10)
            q, r, r4 = res[:3]
            neg_got, q = tie((neg_got, q))
            nmine, nother = finish(neg_part, neg_got)
            if not first:
                rfm, vr = res[3:]
            loss, dp, ds, gk, gs = call(
                functools.partial(score_kernel, dim, neg_count, edges), [core, weights[s].reshape(1, edges), q, tail_cols, nmine, nother], 'svVVVV',
                [shape((1, LANES)), shape((1, edges)), shape((negp, edges), BF16), shape((half, negp)), shape((half, negp))], 'vvVVV',
                [pltpu.VMEM((dim, negp), BF16), pltpu.VMEM((negp, dim), BF16), pltpu.VMEM((negp, CHUNK), F32),
                 pltpu.VMEM((negp, dim), F32), pltpu.VMEM((SLICES * LANES, negp), F32)], 15)
            losses.append(loss[0, 0])
            neg_part = chip_sum(gk, gs)
            neg_part, ds = tie((neg_part, ds))
            neg_got = link(neg_part)
            hg, rk, rs = call(
                functools.partial(grad_kernel, dim, edges), [core, own_rels[s], ds, dp, tail_cols, hb, r, nmine, nother], 'ssVvVVVVV',
                [shape((edges * SLICES, LANES)), shape((half, relp)), shape((half, relp))], 'VVV',
                [pltpu.VMEM((dim, negp), BF16), pltpu.VMEM((relp * SLICES, LANES), F32), pltpu.VMEM((SLICES * CHUNK, LANES), F32),
                 pltpu.VMEM((SLICES * LANES, CHUNK), F32), pltpu.VMEM((SLICES * LANES, relp), F32)], 15)
            rel_part = chip_sum(rk, rs)
            rel_part, hg = tie((rel_part, hg))
            rel_got = link(rel_part)
            if first:
                args, kinds = [heads[s], tails[s], hg, dp, q], 'ssVvV'
            else:
                dp = lax.ppermute(dp, 'ent', shift(s))
                args, kinds = [heads[s], tails[s], rels[s], hg, dp, head_cols, r4], 'sssVvVV'
            acc, = call(functools.partial(scatter_kernel, dim, edges, first), args, kinds, [table_out], 'V',
                        [stage_shape, square_shape], 25)
            neg_got, acc = tie((neg_got, acc))
            gmine, gother = finish(neg_part, neg_got)
            scratch = [stage_shape, square_shape]
            if last:
                args, outs, out_kinds = [core, negs[s]], [table_out, shape((dim, rows)), shape((rows // LANES, LANES))], 'Vhv'
                scratch += [pltpu.VMEM((2, dim, 4 * LANES), F32), pltpu.SemaphoreType.DMA((2,))]
                aliases = {4: 0}
            else:
                args = [core, negs[s], tails[s + 1], negs[s + 1]]
                outs, out_kinds = [table_out, table_out, state_out, cols_bf, neg_half, neg_half], 'VVVVVV'
                scratch += [pltpu.VMEM((dim, negp), BF16)]
                aliases = {6: 0, 4: 1, 5: 2}
            res = call(functools.partial(update_kernel, dim, rows, last), args + [t4, v, acc, gmine, gother], 's' * len(args) + 'VVVVV',
                       outs, out_kinds, scratch, 30, aliases)
            if last:
                _, et, g = res
            else:
                _, t4, v, tb, nk, ns = res

        even = core[0] == 0
        rel_grads = finish(rel_part, rel_got)
        rg = jnp.where(even, jnp.concatenate(rel_grads, axis=0), jnp.concatenate(rel_grads[::-1], axis=0))
        new_vr = vr + jnp.mean(rg * rg, axis=0, keepdims=True)
        new_r = rfm - LEARN_RATE * rg / jnp.sqrt(new_vr + ADA_EPS)
        return et.T, g.reshape(rows), new_r[:, :num_rel].T, new_vr[0, :num_rel], jnp.stack(losses)[None, :]

    return jax.shard_map(device_fn, mesh=mesh,
                         in_specs=(row_spec, flat_spec, rel_spec, state_spec, edge_spec, edge_spec, edge_spec, edge_spec, rel_spec),
                         out_specs=(row_spec, flat_spec, rel_spec, state_spec, row_spec), check_vma=False)
```

```python
import functools

import jax
import jax.numpy as jnp
from jax import lax
from jax.experimental import pallas as pl
from jax.experimental.pallas import tpu as pltpu
from jax.sharding import PartitionSpec as P


LEARN_RATE = 0.05
ADA_EPS = 1e-10
LANES = 128
SLICES = 4
CHUNK = 256
BATCH = 4
F32 = jnp.float32
BF16 = jnp.bfloat16


def ceil_to(value, unit):
    return -(-value // unit) * unit


def vmem():
    return pl.BlockSpec(memory_space=pltpu.VMEM)


def smem():
    return pl.BlockSpec(memory_space=pltpu.SMEM)


def hbm():
    return pl.BlockSpec(memory_space=pltpu.MemorySpace.HBM)


def four(index):
    return pl.multiple_of(index, SLICES)


def gather_rows(src, ids, base, stage, count):
    for k in range(count):
        stage[pl.ds(SLICES * k, SLICES), :] = src[pl.ds(four(ids[base + k]), SLICES), :]


def stage_cols(stage, slice_no):
    return stage[pl.ds(slice_no, LANES, stride=SLICES), :].T


def add_rows(acc, ids, base, rows, row_base, count):
    for first in range(0, count, BATCH):
        index = [ids[base + first + k] for k in range(BATCH)]
        grads = [rows[pl.ds(four(row_base + SLICES * (first + k)), SLICES), :] for k in range(BATCH)]
        total = [acc[pl.ds(four(index[k]), SLICES), :] + grads[k] for k in range(BATCH)]
        for k in range(1, BATCH):
            for earlier in range(k):
                total[k] = total[k] + jnp.where(index[earlier] == index[k], grads[earlier], 0.0)
        for k in range(BATCH):
            acc[pl.ds(four(index[k]), SLICES), :] = total[k]


def zero_rows(ref, step=1024):
    rows = ref.shape[0]
    whole = rows // step

    def body(i, _):
        ref[pl.ds(pl.multiple_of(i * step, 8), step), :] = jnp.zeros((step, LANES), ref.dtype)
        return 0

    lax.fori_loop(0, whole, body, 0)
    if rows % step:
        ref[pl.ds(whole * step, rows % step), :] = jnp.zeros((rows % step, LANES), ref.dtype)


def gather_out(dim, table, ids, out, stage, count):
    def body(b, _):
        gather_rows(table, ids, b * LANES, stage, LANES)
        cols = pl.ds(pl.multiple_of(b * LANES, LANES), LANES)
        for j in range(SLICES):
            size = min(LANES, dim - j * LANES)
            out[pl.ds(j * LANES, size), cols] = stage_cols(stage, j)[:size].astype(BF16)
        return 0

    lax.fori_loop(0, count // LANES, body, 0)


def gather_negs(dim, core, table, negs, nk, ns, nbuf, stage):
    half = nbuf.shape[1] // 2
    gather_out(dim, table, negs, nbuf, stage, nbuf.shape[1])
    nk[...] = nbuf[:, pl.ds(pl.multiple_of(core * half, LANES), half)]
    ns[...] = nbuf[:, pl.ds(pl.multiple_of((1 - core) * half, LANES), half)]


def entry_kernel(dim, rows, core_ref, negs, et, g, t4, v, nk, ns, inbuf, stage, nbuf, in_sem):
    cols = inbuf.shape[2]
    steps = rows // cols
    per = cols // LANES

    def fetch(step, slot):
        return pltpu.make_async_copy(et.at[:, pl.ds(pl.multiple_of(step * cols, LANES), cols)],
                                     inbuf.at[slot, pl.ds(0, dim)], in_sem.at[slot])

    fetch(0, 0).start()
    for slot in range(2):
        inbuf[slot, pl.ds(dim, SLICES * LANES - dim), :] = jnp.zeros((SLICES * LANES - dim, cols), F32)
    t4[pl.ds(rows * SLICES, 32), :] = jnp.zeros((32, LANES), F32)

    def body(step, _):
        slot = lax.rem(step, 2)

        @pl.when(step + 1 < steps)
        def _():
            fetch(step + 1, 1 - slot).start()

        fetch(step, slot).wait()
        for b in range(per):
            row0 = (step * per + b) * LANES
            for j in range(SLICES):
                t4[pl.ds(SLICES * row0 + j, LANES, stride=SLICES), :] = inbuf[slot, pl.ds(j * LANES, LANES), pl.ds(b * LANES, LANES)].T
            v[pl.ds(pl.multiple_of(row0, 8), LANES), :] = jnp.broadcast_to(g[pl.ds(step * per + b, 1), :], (LANES, LANES)).T
        return 0

    lax.fori_loop(0, steps, body, 0)
    gather_negs(dim, core_ref[0], t4, negs, nk, ns, nbuf, stage)


def gather_kernel(dim, lists, *refs):
    ids, t4, outs, stage = refs[:lists], refs[lists], refs[lists + 1:2 * lists + 1], refs[2 * lists + 1]
    for i in range(lists):
        gather_out(dim, t4, ids[i], outs[i], stage, outs[i].shape[1])


def query_kernel(dim, edges, first, *refs):
    if first:
        core_ref, rel, hb, rfm, q_out, r_out, r4, stage, fm = refs
    else:
        core_ref, rel, hb, rfm_in, vr_in, rmine, rother, q_out, r_out, r4, rfm, vr, stage, fm = refs
        core = core_ref[0]
    half = dim // 2
    relp = rfm.shape[1]
    tops = SLICES * LANES
    if not first:
        fm[pl.ds(pl.multiple_of(core * half, 8), half), :] = rmine[...]
        fm[pl.ds(pl.multiple_of((1 - core) * half, 8), half), :] = rother[...]
        grad = fm[pl.ds(0, dim), :]
        vr[...] = vr_in[...] + jnp.sum(grad * grad, axis=0, keepdims=True) / dim
        rate = LEARN_RATE / jnp.sqrt(vr[...] + ADA_EPS)
        rfm[...] = rfm_in[...] - fm[pl.ds(0, dim), :] * rate
    fm[pl.ds(dim, tops - dim), pl.ds(0, LANES)] = jnp.zeros((tops - dim, LANES), F32)
    for b in range(relp // LANES):
        for j in range(SLICES):
            if (j + 1) * LANES <= dim:
                block = rfm[pl.ds(j * LANES, LANES), pl.ds(b * LANES, LANES)]
            else:
                fm[pl.ds(j * LANES, dim - j * LANES), pl.ds(0, LANES)] = rfm[pl.ds(j * LANES, dim - j * LANES), pl.ds(b * LANES, LANES)]
                block = fm[pl.ds(j * LANES, LANES), pl.ds(0, LANES)]
            r4[pl.ds(SLICES * b * LANES + j, LANES, stride=SLICES), :] = block.T

    def step(b, _):
        cols = pl.ds(pl.multiple_of(b * LANES, LANES), LANES)
        gather_rows(r4, rel, b * LANES, stage, LANES)
        for j in range(SLICES):
            size = min(LANES, dim - j * LANES)
            r_out[pl.ds(j * LANES, size), cols] = stage_cols(stage, j)[:size]
        h = hb[:, cols].astype(F32)
        r_re, r_im = r_out[pl.ds(0, half), cols], r_out[pl.ds(half, half), cols]
        q_out[pl.ds(0, half), cols] = h[:half] * r_re - h[half:] * r_im
        q_out[pl.ds(half, half), cols] = h[:half] * r_im + h[half:] * r_re
        return 0

    lax.fori_loop(0, edges // LANES, step, 0)


def place_negs(core, nb, nfull, nother):
    nhalf = nfull.shape[1]
    nb[:, pl.ds(pl.multiple_of(core * nhalf, LANES), nhalf)] = nfull[...]
    nb[:, pl.ds(pl.multiple_of((1 - core) * nhalf, LANES), nhalf)] = nother[...]


def exp_kernel(neg_count, edges, core_ref, q, nfull, nother, e_out, top_out, sum_out, nb, nbt, sc):
    negp = nb.shape[1]
    place_negs(core_ref[0], nb, nfull, nother)
    for b in range(negp // LANES):
        nbt[pl.ds(b * LANES, LANES), :] = nb[:, pl.ds(b * LANES, LANES)].astype(F32).T.astype(BF16)

    def step(c, _):
        cols = pl.ds(pl.multiple_of(c * CHUNK, LANES), CHUNK)
        sc[...] = lax.dot_general(nbt[pl.ds(0, neg_count), :], q[:, cols].astype(BF16), (((1,), (0,)), ((), ())), preferred_element_type=F32)
        top = jnp.max(sc[...], axis=0, keepdims=True)
        top_out[:, cols] = top
        total = jnp.zeros((1, CHUNK), F32)
        part = 200
        for i in range(0, neg_count, part):
            size = min(part, neg_count - i)
            e = jnp.exp(sc[pl.ds(i, size), :] - top)
            e_out[pl.ds(i, size), cols] = e
            total = total + jnp.sum(e, axis=0, keepdims=True)
        sum_out[:, cols] = total
        return 0

    lax.fori_loop(0, edges // CHUNK, step, 0)


def score_kernel(dim, neg_count, edges, core_ref, w, q, tb, e, neg_top, neg_sum,
                 loss, dp_out, ds, nk, ns, ng, fm):
    core = core_ref[0]
    half = dim // 2
    negp = ds.shape[0]
    ng[...] = jnp.zeros(ng.shape, F32)
    ds[pl.ds(neg_count, negp - neg_count), :] = jnp.zeros((negp - neg_count, edges), BF16)

    def step(c, loss_row):
        cols = pl.ds(pl.multiple_of(c * CHUNK, LANES), CHUNK)
        pos = jnp.sum(q[:, cols] * tb[:, cols].astype(F32), axis=0, keepdims=True)
        top = jnp.maximum(pos, neg_top[:, cols])
        pos_exp = jnp.exp(pos - top)
        shrink = jnp.exp(neg_top[:, cols] - top)
        norm = pos_exp + shrink * neg_sum[:, cols]
        wt = w[:, cols]
        loss_row = loss_row + wt * (top + jnp.log(norm) - pos)
        dp_out[:, cols] = wt * (pos_exp / norm - 1.0)
        ds[pl.ds(0, neg_count), cols] = (e[:, cols] * (wt * shrink / norm)).astype(BF16)
        ng[...] += lax.dot_general(ds[:, cols], q[:, cols].astype(BF16), (((1,), (1,)), ((), ())), preferred_element_type=F32)
        return loss_row

    loss_row = lax.fori_loop(0, edges // CHUNK, step, jnp.zeros((1, CHUNK), F32))
    loss[...] = jnp.broadcast_to(jnp.sum(loss_row, axis=1, keepdims=True) / edges, loss.shape)
    for b in range(negp // LANES):
        for j in range(SLICES):
            size = min(LANES, dim - j * LANES)
            fm[pl.ds(j * LANES, size), pl.ds(b * LANES, LANES)] = ng[pl.ds(b * LANES, LANES), pl.ds(j * LANES, size)].T
    nk[...] = fm[pl.ds(pl.multiple_of(core * half, 8), half), :]
    ns[...] = fm[pl.ds(pl.multiple_of((1 - core) * half, 8), half), :]


def grad_kernel(dim, edges, core_ref, rel, ds, dp, tb, hb, r, nfull, nother,
                hg, rk, rs, nb, racc, stage, qs, fm):
    core = core_ref[0]
    half = dim // 2
    relp = rk.shape[1]
    tops = SLICES * LANES
    place_negs(core, nb, nfull, nother)
    zero_rows(racc)
    qs[pl.ds(dim, tops - dim), :] = jnp.zeros((tops - dim, CHUNK), F32)

    def step(c, _):
        cols = pl.ds(pl.multiple_of(c * CHUNK, LANES), CHUNK)
        gq = lax.dot_general(nb[...], ds[:, cols], (((1,), (0,)), ((), ())), preferred_element_type=F32) + dp[:, cols] * tb[:, cols].astype(F32)
        g_re, g_im = gq[:half], gq[half:]
        h = hb[:, cols].astype(F32)
        h_re, h_im = h[:half], h[half:]
        qs[pl.ds(0, half), :] = g_re * h_re + g_im * h_im
        qs[pl.ds(half, half), :] = g_im * h_re - g_re * h_im
        for b in range(CHUNK // LANES):
            for j in range(SLICES):
                stage[pl.ds(SLICES * b * LANES + j, LANES, stride=SLICES), :] = qs[pl.ds(j * LANES, LANES), pl.ds(b * LANES, LANES)].T
        r_re, r_im = r[pl.ds(0, half), cols], r[pl.ds(half, half), cols]
        qs[pl.ds(0, half), :] = g_re * r_re + g_im * r_im
        qs[pl.ds(half, half), :] = g_im * r_re - g_re * r_im
        for b in range(CHUNK // LANES):
            for j in range(SLICES):
                hg[pl.ds(SLICES * (c * CHUNK + b * LANES) + j, LANES, stride=SLICES), :] = qs[pl.ds(j * LANES, LANES), pl.ds(b * LANES, LANES)].T
        add_rows(racc, rel, c * CHUNK, stage, 0, CHUNK)
        return 0

    lax.fori_loop(0, edges // CHUNK, step, 0)
    for b in range(relp // LANES):
        for j in range(SLICES):
            size = min(LANES, dim - j * LANES)
            fm[pl.ds(j * LANES, size), pl.ds(b * LANES, LANES)] = racc[pl.ds(SLICES * b * LANES + j, LANES, stride=SLICES), :].T[:size]
    rk[...] = fm[pl.ds(pl.multiple_of(core * half, 8), half), :]
    rs[...] = fm[pl.ds(pl.multiple_of((1 - core) * half, 8), half), :]


def unstage(rt, stage):
    for j in range(SLICES):
        stage[pl.ds(j, LANES, stride=SLICES), :] = rt[pl.ds(j * LANES, LANES), :].T


def scatter_kernel(dim, edges, own, *refs):
    if own:
        heads, tails, hg, dp, q, acc, stage, rt = refs
    else:
        heads, tails, rel, hg, dp, hb_in, r4, acc, stage, rt = refs
    half = dim // 2
    tops = SLICES * LANES
    zero_rows(acc)
    rt[pl.ds(dim, tops - dim), :] = jnp.zeros((tops - dim, LANES), F32)

    def head_step(b, _):
        add_rows(acc, heads, b * 32, hg, b * 32 * SLICES, 32)
        return 0

    lax.fori_loop(0, edges // 32, head_step, 0)

    def tail_step(b, _):
        cols = pl.ds(pl.multiple_of(b * LANES, LANES), LANES)
        scale = dp[:, cols]
        if own:
            rt[pl.ds(0, dim), :] = q[:, cols] * scale
        else:
            gather_rows(r4, rel, b * LANES, stage, LANES)
            for j in range(SLICES):
                rt[pl.ds(j * LANES, LANES), :] = stage_cols(stage, j)
            h = hb_in[:, cols].astype(F32)
            r_re, r_im = rt[pl.ds(0, half), :], rt[pl.ds(half, half), :]
            q_re = scale * (h[:half] * r_re - h[half:] * r_im)
            q_im = scale * (h[:half] * r_im + h[half:] * r_re)
            rt[pl.ds(0, half), :] = q_re
            rt[pl.ds(half, half), :] = q_im
        unstage(rt, stage)
        add_rows(acc, tails, b * LANES, stage, 0, LANES)
        return 0

    lax.fori_loop(0, edges // LANES, tail_step, 0)


def update_kernel(dim, rows, last, *refs):
    if last:
        core_ref, negs, t4, v, _, nmine, nother, acc, et_out, g_out, stage, rt, outbuf, out_sem = refs
    else:
        core_ref, negs, tails_n, negs_n, t4, v, _, nmine, nother, acc, new_t4, new_v, tb, nk, ns, stage, rt, nbuf = refs
    core = core_ref[0]
    half = dim // 2
    tops = SLICES * LANES
    rt[pl.ds(dim, tops - dim), :] = jnp.zeros((tops - dim, LANES), F32)

    def neg_step(b, _):
        cols = pl.ds(pl.multiple_of(b * LANES, LANES), LANES)
        rt[pl.ds(pl.multiple_of(core * half, 8), half), :] = nmine[:, cols]
        rt[pl.ds(pl.multiple_of((1 - core) * half, 8), half), :] = nother[:, cols]
        unstage(rt, stage)
        add_rows(acc, negs, b * LANES, stage, 0, LANES)
        return 0

    lax.fori_loop(0, nmine.shape[1] // LANES, neg_step, 0)

    def ada_rows(row0):
        where = [pl.ds(SLICES * row0 + j, LANES, stride=SLICES) for j in range(SLICES)]
        square = acc[where[0], :] * acc[where[0], :]
        for j in range(1, SLICES):
            square = square + acc[where[j], :] * acc[where[j], :]
        state = v[pl.ds(pl.multiple_of(row0, 8), LANES), :] + jnp.sum(square, axis=1, keepdims=True) / dim
        rate = LEARN_RATE / jnp.sqrt(state + ADA_EPS)
        return state, where, [t4[w, :] - acc[w, :] * rate for w in where]

    if not last:
        def ada_step(b, _):
            state, where, values = ada_rows(b * LANES)
            new_v[pl.ds(pl.multiple_of(b * LANES, 8), LANES), :] = state
            for w, value in zip(where, values):
                new_t4[w, :] = value
            return 0

        lax.fori_loop(0, rows // LANES, ada_step, 0)
        new_t4[pl.ds(rows * SLICES, 32), :] = jnp.zeros((32, LANES), F32)
        gather_negs(dim, core, new_t4, negs_n, nk, ns, nbuf, stage)
        gather_out(dim, new_t4, tails_n, tb, stage, tb.shape[1])
        return

    width = outbuf.shape[2]
    per = width // LANES
    steps = rows // width

    def save(step, slot):
        return pltpu.make_async_copy(outbuf.at[slot], et_out.at[:, pl.ds(pl.multiple_of(step * width, LANES), width)], out_sem.at[slot])

    def exit_step(step, _):
        slot = lax.rem(step, 2)

        @pl.when(step >= 2)
        def _():
            save(step - 2, slot).wait()

        for b in range(per):
            state, _, values = ada_rows((step * per + b) * LANES)
            for j in range(SLICES):
                size = min(LANES, dim - j * LANES)
                outbuf[slot, pl.ds(j * LANES, size), pl.ds(b * LANES, LANES)] = values[j].T[:size]
            g_out[pl.ds(step * per + b, 1), :] = state.T[:1]
        save(step, slot).start()
        return 0

    lax.fori_loop(0, steps, exit_step, 0)
    save(steps - 2, (steps - 2) % 2).wait()
    save(steps - 1, (steps - 1) % 2).wait()


def padded_bytes(dims, dtype):
    size = jnp.dtype(dtype).itemsize
    dims = (1,) * (2 - len(dims)) + tuple(dims)
    total = ceil_to(dims[-2], 32 // size) * ceil_to(dims[-1], LANES) * size
    for d in dims[:-2]:
        total *= d
    return total


def cost(micros):
    return pl.CostEstimate(flops=int(micros * 5e6), bytes_accessed=0, transcendentals=0)


def shape(dims, dtype=F32):
    return jax.ShapeDtypeStruct(dims, dtype)


def solution(mesh):
    ent_size = mesh.shape['ent']
    row_spec = P(('sweep', 'ent'), None)
    flat_spec = P(('sweep', 'ent'))
    rel_spec = P('sweep', None)
    state_spec = P('sweep')
    edge_spec = P(('sweep', 'ent'), None, None)
    swap = [(i, i ^ 1) for i in range(ent_size)]
    cross = [(i, i ^ 2) for i in range(ent_size)]

    def shift(amount):
        return [(i, (i + amount) % ent_size) for i in range(ent_size)]

    tie = lax.optimization_barrier

    def chip_sum(keep, send):
        return keep + lax.ppermute(send, 'ent', swap)

    def send(value, pairs):
        return lax.ppermute(value, 'ent', pairs)

    def link(part):
        return send(part, cross)

    def finish(part, got):
        mine = part + got
        return mine, lax.ppermute(mine, 'ent', swap)

    def device_fn(ent_emb, ent_ada, rel_emb, rel_ada, head_idx, tail_idx, rel_idx, edge_mask, neg_idx):
        rows, dim = ent_emb.shape
        num_rel = rel_emb.shape[0]
        _, rounds, edges = head_idx.shape
        neg_count = neg_idx.shape[1]
        negp = ceil_to(neg_count, 2 * LANES)
        relp = ceil_to(num_rel, LANES)
        half = dim // 2
        my_dev = lax.axis_index('ent')
        core = (my_dev % 2).reshape(1)

        heads = [head_idx[0, s] * SLICES for s in range(rounds)]
        own_tails = [tail_idx[0, s] * SLICES for s in range(rounds)]
        own_rels = [rel_idx[0, s] * SLICES for s in range(rounds)]
        tails, rels = [own_tails[0]], [own_rels[0]]
        for s in range(1, rounds):
            got = send(jnp.stack([own_tails[s], own_rels[s]]), shift(s))
            tails.append(got[0])
            rels.append(got[1])
        owned = (neg_idx // rows) == my_dev
        neg_local = jnp.where(owned, neg_idx % rows, rows) * SLICES
        neg_local = jnp.pad(neg_local, ((0, 0), (0, negp - neg_count)), constant_values=rows * SLICES)
        negs = [neg_local[s] for s in range(rounds)]
        weights = edge_mask[0].astype(F32)

        wide_rows = (rows + 8) * SLICES
        stage_shape = pltpu.VMEM((SLICES * LANES, LANES), F32)
        square_shape = pltpu.VMEM((SLICES * LANES, LANES), F32)
        table_out, state_out = shape((wide_rows, LANES)), shape((rows, LANES))
        cols_bf = shape((dim, edges), BF16)
        neg_half = shape((dim, negp // 2), BF16)

        def call(kernel, args, kinds, outs, out_kinds, scratch, micros, aliases=None):
            places = {'s': smem, 'h': hbm, 'v': vmem, 'V': vmem}
            windows = [a for a, k in zip(list(args) + outs, kinds + out_kinds) if k == 'v']
            limit = 3 * 2 ** 20 + sum(padded_bytes(a.shape, a.dtype) for a in windows)
            limit += sum(padded_bytes(a.shape, a.dtype) for a in scratch if a.memory_space == pltpu.VMEM)
            args = [pltpu.with_memory_space_constraint(a, pltpu.VMEM) if k == 'V' else a for a, k in zip(args, kinds)]
            outs = [pltpu.VMEM(o.shape, o.dtype) if k == 'V' else o for o, k in zip(outs, out_kinds)]
            return pl.pallas_call(
                kernel, out_shape=outs, in_specs=[places[k]() for k in kinds], out_specs=[places[k]() for k in out_kinds],
                scratch_shapes=scratch, compiler_params=pltpu.CompilerParams(vmem_limit_bytes=limit),
                input_output_aliases=aliases or {}, cost_estimate=cost(micros))(*args)

        def gather(lists, t4):
            return call(functools.partial(gather_kernel, dim, len(lists)), lists + [t4], 's' * len(lists) + 'V',
                        [cols_bf] * len(lists), 'V' * len(lists), [stage_shape], 1 + 5 * len(lists))

        t4, v, nk, ns = call(
            functools.partial(entry_kernel, dim, rows), [core, negs[0], pltpu.with_memory_space_constraint(ent_emb.T, pltpu.HBM), ent_ada.reshape(rows // LANES, LANES)], 'sshv',
            [table_out, state_out, neg_half, neg_half], 'VVVV',
            [pltpu.VMEM((2, SLICES * LANES, 4 * LANES), F32), stage_shape, pltpu.VMEM((dim, negp), BF16), pltpu.SemaphoreType.DMA((2,))], 20)

        rfm = jnp.pad(rel_emb.T, ((0, 0), (0, relp - num_rel)))
        vr = jnp.pad(rel_ada, (0, relp - num_rel), constant_values=1.0).reshape(1, relp)
        losses = []
        rel_grads = None
        for s in range(rounds):
            first, last = s == 0, s == rounds - 1
            neg_part = chip_sum(nk, ns)
            if first:
                neg_part, t4, tails, rels = tie((neg_part, t4, tails, rels))
                neg_got = link(neg_part)
                tail_cols, hb = gather([tails[0], heads[0]], t4)
                head_cols = hb
                neg_got, hb = tie((neg_got, hb))
            else:
                neg_part, t4, tb = tie((neg_part, t4, tb))
                neg_got = link(neg_part)
                tail_cols = send(tb, shift(-s))
                hb, = gather([heads[s]], t4)
                rel_got, hb = tie((rel_got, hb))
                rel_grads = finish(rel_part, rel_got)
            wide = shape((dim, edges))
            outs, out_kinds = [wide, wide, shape((relp * SLICES, LANES))], 'VVV'
            args, kinds = [core, own_rels[s], hb, rfm], 'ssV' + ('v' if first else 'V')
            if not first:
                outs += [shape((dim, relp)), shape((1, relp))]
                out_kinds += 'Vv'
                args += [vr] + list(rel_grads)
                kinds += 'vVV'
            res = call(functools.partial(query_kernel, dim, edges, first), args, kinds, outs, out_kinds,
                       [stage_shape, pltpu.VMEM((SLICES * LANES, relp), F32)], 10)
            q, r, r4 = res[:3]
            neg_got, q = tie((neg_got, q))
            nmine, nother = finish(neg_part, neg_got)
            if not first:
                rfm, vr = res[3:]
            e, neg_top, neg_total = call(
                functools.partial(exp_kernel, neg_count, edges), [core, q, nmine, nother], 'sVVV',
                [shape((neg_count, edges)), shape((1, edges)), shape((1, edges))], 'Vvv',
                [pltpu.VMEM((dim, negp), BF16), pltpu.VMEM((negp, dim), BF16), pltpu.VMEM((neg_count, CHUNK), F32)], 8)
            if not first:
                e, tail_cols = tie((e, tail_cols))
                tail_cols, hb = tie((tail_cols, hb))
                head_cols = send(hb, shift(s))
            loss, dp, ds, gk, gs = call(
                functools.partial(score_kernel, dim, neg_count, edges), [core, weights[s].reshape(1, edges), q, tail_cols, e, neg_top, neg_total], 'svVVVvv',
                [shape((1, LANES)), shape((1, edges)), shape((negp, edges), BF16), shape((half, negp)), shape((half, negp))], 'vvVVV',
                [pltpu.VMEM((negp, dim), F32), pltpu.VMEM((SLICES * LANES, negp), F32)], 8)
            losses.append(loss[0, 0])
            if not first:
                dp_away = send(dp, shift(s))
            neg_part = chip_sum(gk, gs)
            neg_part, ds = tie((neg_part, ds))
            neg_got = link(neg_part)
            hg, rk, rs = call(
                functools.partial(grad_kernel, dim, edges), [core, own_rels[s], ds, dp, tail_cols, hb, r, nmine, nother], 'ssVvVVVVV',
                [shape((edges * SLICES, LANES)), shape((half, relp)), shape((half, relp))], 'VVV',
                [pltpu.VMEM((dim, negp), BF16), pltpu.VMEM((relp * SLICES, LANES), F32), pltpu.VMEM((SLICES * CHUNK, LANES), F32),
                 pltpu.VMEM((SLICES * LANES, CHUNK), F32), pltpu.VMEM((SLICES * LANES, relp), F32)], 15)
            rel_part = chip_sum(rk, rs)
            rel_part, hg = tie((rel_part, hg))
            rel_got = link(rel_part)
            if first:
                args, kinds = [heads[s], tails[s], hg, dp, q], 'ssVvV'
            else:
                args, kinds = [heads[s], tails[s], rels[s], hg, dp_away, head_cols, r4], 'sssVvVV'
            acc, = call(functools.partial(scatter_kernel, dim, edges, first), args, kinds, [table_out], 'V',
                        [stage_shape, square_shape], 25)
            neg_got, acc = tie((neg_got, acc))
            gmine, gother = finish(neg_part, neg_got)
            scratch = [stage_shape, square_shape]
            if last:
                args, outs, out_kinds = [core, negs[s]], [table_out, shape((dim, rows)), shape((rows // LANES, LANES))], 'Vhv'
                scratch += [pltpu.VMEM((2, dim, 4 * LANES), F32), pltpu.SemaphoreType.DMA((2,))]
                aliases = {4: 0}
            else:
                args = [core, negs[s], tails[s + 1], negs[s + 1]]
                outs, out_kinds = [table_out, table_out, state_out, cols_bf, neg_half, neg_half], 'VVVVVV'
                scratch += [pltpu.VMEM((dim, negp), BF16)]
                aliases = {6: 0, 4: 1, 5: 2}
            res = call(functools.partial(update_kernel, dim, rows, last), args + [t4, v, acc, gmine, gother], 's' * len(args) + 'VVVVV',
                       outs, out_kinds, scratch, 30, aliases)
            if last:
                _, et, g = res
            else:
                _, t4, v, tb, nk, ns = res

        even = core[0] == 0
        rel_grads = finish(rel_part, rel_got)
        rg = jnp.where(even, jnp.concatenate(rel_grads, axis=0), jnp.concatenate(rel_grads[::-1], axis=0))
        new_vr = vr + jnp.mean(rg * rg, axis=0, keepdims=True)
        new_r = rfm - LEARN_RATE * rg / jnp.sqrt(new_vr + ADA_EPS)
        return et.T, g.reshape(rows), new_r[:, :num_rel].T, new_vr[0, :num_rel], jnp.stack(losses)[None, :]

    return jax.shard_map(device_fn, mesh=mesh,
                         in_specs=(row_spec, flat_spec, rel_spec, state_spec, edge_spec, edge_spec, edge_spec, edge_spec, rel_spec),
                         out_specs=(row_spec, flat_spec, rel_spec, state_spec, row_spec), check_vma=False)
```

```python
import functools

import jax
import jax.numpy as jnp
from jax import lax
from jax.experimental import pallas as pl
from jax.experimental.pallas import tpu as pltpu
from jax.sharding import PartitionSpec as P


LEARN_RATE = 0.05
ADA_EPS = 1e-10
LANES = 128
SLICES = 4
CHUNK = 256
BATCH = 4
F32 = jnp.float32
BF16 = jnp.bfloat16


def ceil_to(value, unit):
    return -(-value // unit) * unit


def vmem():
    return pl.BlockSpec(memory_space=pltpu.VMEM)


def smem():
    return pl.BlockSpec(memory_space=pltpu.SMEM)


def hbm():
    return pl.BlockSpec(memory_space=pltpu.MemorySpace.HBM)


def four(index):
    return pl.multiple_of(index, SLICES)


def gather_rows(src, ids, base, stage, count):
    for k in range(count):
        stage[pl.ds(SLICES * k, SLICES), :] = src[pl.ds(four(ids[base + k]), SLICES), :]


def stage_cols(stage, slice_no):
    return stage[pl.ds(slice_no, LANES, stride=SLICES), :].T


def batch_sums(acc, ids, base, rows, row_base):
    index = [ids[base + k] for k in range(BATCH)]
    grads = [rows[pl.ds(four(row_base + SLICES * k), SLICES), :] for k in range(BATCH)]
    total = [acc[pl.ds(four(index[k]), SLICES), :] + grads[k] for k in range(BATCH)]
    for k in range(1, BATCH):
        for earlier in range(k):
            total[k] = total[k] + jnp.where(index[earlier] == index[k], grads[earlier], 0.0)
    return index, total


def add_rows(chains, count):
    for first in range(0, count, BATCH):
        done = [batch_sums(acc, ids, base + first, rows, row_base + SLICES * first) for acc, ids, base, rows, row_base in chains]
        for (acc, *_), (index, total) in zip(chains, done):
            for k in range(BATCH):
                acc[pl.ds(four(index[k]), SLICES), :] = total[k]


def put_halves(core, keep, sent, cols, block_of, dim):
    half = dim // 2
    for side in range(2):
        @pl.when(core == side)
        def _():
            for j in range(SLICES):
                block = block_of(j)
                for h in range(2):
                    lo, hi = max(j * LANES, h * half), min((j + 1) * LANES, (h + 1) * half)
                    if lo < hi:
                        (keep if h == side else sent)[pl.ds(lo - h * half, hi - lo), cols] = block[lo - j * LANES:hi - j * LANES]


def zero_rows(ref, step=1024):
    rows = ref.shape[0]
    whole = rows // step

    def body(i, _):
        ref[pl.ds(pl.multiple_of(i * step, 8), step), :] = jnp.zeros((step, LANES), ref.dtype)
        return 0

    lax.fori_loop(0, whole, body, 0)
    if rows % step:
        ref[pl.ds(whole * step, rows % step), :] = jnp.zeros((rows % step, LANES), ref.dtype)


def gather_out(dim, table, ids, out, stage, count):
    def body(b, _):
        gather_rows(table, ids, b * LANES, stage, LANES)
        cols = pl.ds(pl.multiple_of(b * LANES, LANES), LANES)
        for j in range(SLICES):
            size = min(LANES, dim - j * LANES)
            out[pl.ds(j * LANES, size), cols] = stage_cols(stage, j)[:size].astype(BF16)
        return 0

    lax.fori_loop(0, count // LANES, body, 0)


def gather_negs(dim, core, table, negs, nk, ns, nbuf, stage):
    half = nbuf.shape[1] // 2
    gather_out(dim, table, negs, nbuf, stage, nbuf.shape[1])
    nk[...] = nbuf[:, pl.ds(pl.multiple_of(core * half, LANES), half)]
    ns[...] = nbuf[:, pl.ds(pl.multiple_of((1 - core) * half, LANES), half)]


def entry_kernel(dim, rows, core_ref, negs, et, g, t4, v, nk, ns, inbuf, stage, nbuf, in_sem):
    cols = inbuf.shape[2]
    steps = rows // cols
    per = cols // LANES

    def fetch(step, slot):
        return pltpu.make_async_copy(et.at[:, pl.ds(pl.multiple_of(step * cols, LANES), cols)],
                                     inbuf.at[slot, pl.ds(0, dim)], in_sem.at[slot])

    slots = inbuf.shape[0]
    for slot in range(slots - 1):
        fetch(slot, slot).start()
    for slot in range(slots):
        inbuf[slot, pl.ds(dim, SLICES * LANES - dim), :] = jnp.zeros((SLICES * LANES - dim, cols), F32)
    t4[pl.ds(rows * SLICES, 32), :] = jnp.zeros((32, LANES), F32)

    def body(step, _):
        slot = lax.rem(step, slots)

        @pl.when(step + slots - 1 < steps)
        def _():
            fetch(step + slots - 1, lax.rem(step + slots - 1, slots)).start()

        fetch(step, slot).wait()
        for b in range(per):
            row0 = (step * per + b) * LANES
            for j in range(SLICES):
                t4[pl.ds(SLICES * row0 + j, LANES, stride=SLICES), :] = inbuf[slot, pl.ds(j * LANES, LANES), pl.ds(b * LANES, LANES)].T
            v[pl.ds(pl.multiple_of(row0, 8), LANES), :] = jnp.broadcast_to(g[pl.ds(step * per + b, 1), :], (LANES, LANES)).T
        return 0

    lax.fori_loop(0, steps, body, 0)
    gather_negs(dim, core_ref[0], t4, negs, nk, ns, nbuf, stage)


def gather_kernel(dim, lists, *refs):
    ids, t4, outs, stage = refs[:lists], refs[lists], refs[lists + 1:2 * lists + 1], refs[2 * lists + 1]
    for i in range(lists):
        gather_out(dim, t4, ids[i], outs[i], stage, outs[i].shape[1])


def query_kernel(dim, edges, first, *refs):
    if first:
        core_ref, rel, hb, rfm, q_out, r_out, r4, stage, fm = refs
    else:
        core_ref, rel, hb, rfm_in, vr_in, rmine, rother, q_out, r_out, r4, rfm, vr, stage, fm = refs
        core = core_ref[0]
    half = dim // 2
    relp = rfm.shape[1]
    tops = SLICES * LANES
    if not first:
        fm[pl.ds(pl.multiple_of(core * half, 8), half), :] = rmine[...]
        fm[pl.ds(pl.multiple_of((1 - core) * half, 8), half), :] = rother[...]
        grad = fm[pl.ds(0, dim), :]
        vr[...] = vr_in[...] + jnp.sum(grad * grad, axis=0, keepdims=True) / dim
        rate = LEARN_RATE / jnp.sqrt(vr[...] + ADA_EPS)
        rfm[...] = rfm_in[...] - fm[pl.ds(0, dim), :] * rate
    fm[pl.ds(dim, tops - dim), pl.ds(0, LANES)] = jnp.zeros((tops - dim, LANES), F32)
    for b in range(relp // LANES):
        for j in range(SLICES):
            if (j + 1) * LANES <= dim:
                block = rfm[pl.ds(j * LANES, LANES), pl.ds(b * LANES, LANES)]
            else:
                fm[pl.ds(j * LANES, dim - j * LANES), pl.ds(0, LANES)] = rfm[pl.ds(j * LANES, dim - j * LANES), pl.ds(b * LANES, LANES)]
                block = fm[pl.ds(j * LANES, LANES), pl.ds(0, LANES)]
            r4[pl.ds(SLICES * b * LANES + j, LANES, stride=SLICES), :] = block.T

    def step(b, _):
        cols = pl.ds(pl.multiple_of(b * LANES, LANES), LANES)
        gather_rows(r4, rel, b * LANES, stage, LANES)
        for j in range(SLICES):
            size = min(LANES, dim - j * LANES)
            r_out[pl.ds(j * LANES, size), cols] = stage_cols(stage, j)[:size]
        h = hb[:, cols].astype(F32)
        r_re, r_im = r_out[pl.ds(0, half), cols], r_out[pl.ds(half, half), cols]
        q_out[pl.ds(0, half), cols] = h[:half] * r_re - h[half:] * r_im
        q_out[pl.ds(half, half), cols] = h[:half] * r_im + h[half:] * r_re
        return 0

    lax.fori_loop(0, edges // LANES, step, 0)


def place_negs(core, nb, nfull, nother):
    nhalf = nfull.shape[1]
    nb[:, pl.ds(pl.multiple_of(core * nhalf, LANES), nhalf)] = nfull[...]
    nb[:, pl.ds(pl.multiple_of((1 - core) * nhalf, LANES), nhalf)] = nother[...]


def exp_kernel(neg_count, edges, core_ref, q, nfull, nother, e_out, top_out, sum_out, nb, nbt, sc):
    negp = nb.shape[1]
    place_negs(core_ref[0], nb, nfull, nother)
    for b in range(negp // LANES):
        nbt[pl.ds(b * LANES, LANES), :] = nb[:, pl.ds(b * LANES, LANES)].astype(F32).T.astype(BF16)

    def step(c, _):
        cols = pl.ds(pl.multiple_of(c * CHUNK, LANES), CHUNK)
        sc[...] = lax.dot_general(nbt[pl.ds(0, neg_count), :], q[:, cols].astype(BF16), (((1,), (0,)), ((), ())), preferred_element_type=F32)
        top = jnp.max(sc[...], axis=0, keepdims=True)
        top_out[:, cols] = top
        total = jnp.zeros((1, CHUNK), F32)
        part = 200
        for i in range(0, neg_count, part):
            size = min(part, neg_count - i)
            e = jnp.exp(sc[pl.ds(i, size), :] - top)
            e_out[pl.ds(i, size), cols] = e
            total = total + jnp.sum(e, axis=0, keepdims=True)
        sum_out[:, cols] = total
        return 0

    lax.fori_loop(0, edges // CHUNK, step, 0)


def score_kernel(dim, neg_count, edges, core_ref, w, q, tb, e, neg_top, neg_sum,
                 loss, dp_out, ds, nk, ns, ng):
    core = core_ref[0]
    negp = ds.shape[0]
    ng[...] = jnp.zeros(ng.shape, F32)
    ds[pl.ds(neg_count, negp - neg_count), :] = jnp.zeros((negp - neg_count, edges), BF16)

    def step(c, loss_row):
        cols = pl.ds(pl.multiple_of(c * CHUNK, LANES), CHUNK)
        pos = jnp.sum(q[:, cols] * tb[:, cols].astype(F32), axis=0, keepdims=True)
        top = jnp.maximum(pos, neg_top[:, cols])
        pos_exp = jnp.exp(pos - top)
        shrink = jnp.exp(neg_top[:, cols] - top)
        norm = pos_exp + shrink * neg_sum[:, cols]
        wt = w[:, cols]
        loss_row = loss_row + wt * (top + jnp.log(norm) - pos)
        dp_out[:, cols] = wt * (pos_exp / norm - 1.0)
        ds[pl.ds(0, neg_count), cols] = (e[:, cols] * (wt * shrink / norm)).astype(BF16)
        ng[...] += lax.dot_general(ds[:, cols], q[:, cols].astype(BF16), (((1,), (1,)), ((), ())), preferred_element_type=F32)
        return loss_row

    loss_row = lax.fori_loop(0, edges // CHUNK, step, jnp.zeros((1, CHUNK), F32))
    loss[...] = jnp.broadcast_to(jnp.sum(loss_row, axis=1, keepdims=True) / edges, loss.shape)

    def save(b, _):
        rows = pl.ds(pl.multiple_of(b * LANES, LANES), LANES)
        put_halves(core, nk, ns, rows, lambda j: ng[rows, pl.ds(j * LANES, min(LANES, dim - j * LANES))].T, dim)
        return 0

    lax.fori_loop(0, negp // LANES, save, 0)


def grad_kernel(dim, edges, core_ref, rel, heads, ds, dp, tb, hb, r, nfull, nother,
                acc, rk, rs, nb, racc, stage_r, stage_h, qs):
    core = core_ref[0]
    half = dim // 2
    relp = rk.shape[1]
    tops = SLICES * LANES
    place_negs(core, nb, nfull, nother)
    zero_rows(racc)
    zero_rows(acc)
    qs[pl.ds(dim, tops - dim), :] = jnp.zeros((tops - dim, CHUNK), F32)

    def step(c, _):
        cols = pl.ds(pl.multiple_of(c * CHUNK, LANES), CHUNK)
        gq = lax.dot_general(nb[...], ds[:, cols], (((1,), (0,)), ((), ())), preferred_element_type=F32) + dp[:, cols] * tb[:, cols].astype(F32)
        g_re, g_im = gq[:half], gq[half:]
        h = hb[:, cols].astype(F32)
        h_re, h_im = h[:half], h[half:]
        r_re, r_im = r[pl.ds(0, half), cols], r[pl.ds(half, half), cols]
        for stage, f_re, f_im in ((stage_r, h_re, h_im), (stage_h, r_re, r_im)):
            qs[pl.ds(0, half), :] = g_re * f_re + g_im * f_im
            qs[pl.ds(half, half), :] = g_im * f_re - g_re * f_im
            for b in range(CHUNK // LANES):
                for j in range(SLICES):
                    stage[pl.ds(SLICES * b * LANES + j, LANES, stride=SLICES), :] = qs[pl.ds(j * LANES, LANES), pl.ds(b * LANES, LANES)].T
        add_rows([(racc, rel, c * CHUNK, stage_r, 0), (acc, heads, c * CHUNK, stage_h, 0)], CHUNK)
        return 0

    lax.fori_loop(0, edges // CHUNK, step, 0)

    def save(b, _):
        cols = pl.ds(pl.multiple_of(b * LANES, LANES), LANES)
        put_halves(core, rk, rs, cols, lambda j: racc[pl.ds(SLICES * LANES * b + j, LANES, stride=SLICES), :].T, dim)
        return 0

    lax.fori_loop(0, relp // LANES, save, 0)


def unstage(rt, stage):
    for j in range(SLICES):
        stage[pl.ds(j, LANES, stride=SLICES), :] = rt[pl.ds(j * LANES, LANES), :].T


def scatter_kernel(dim, edges, own, *refs):
    if own:
        tails, dp, q, _, acc, stage, rt = refs
    else:
        tails, rel, dp, hb_in, r4, _, acc, stage, rt = refs
    half = dim // 2
    tops = SLICES * LANES
    rt[pl.ds(dim, tops - dim), :] = jnp.zeros((tops - dim, LANES), F32)

    def tail_step(b, _):
        cols = pl.ds(pl.multiple_of(b * LANES, LANES), LANES)
        scale = dp[:, cols]
        if own:
            rt[pl.ds(0, dim), :] = q[:, cols] * scale
        else:
            gather_rows(r4, rel, b * LANES, stage, LANES)
            for j in range(SLICES):
                rt[pl.ds(j * LANES, LANES), :] = stage_cols(stage, j)
            h = hb_in[:, cols].astype(F32)
            r_re, r_im = rt[pl.ds(0, half), :], rt[pl.ds(half, half), :]
            q_re = scale * (h[:half] * r_re - h[half:] * r_im)
            q_im = scale * (h[:half] * r_im + h[half:] * r_re)
            rt[pl.ds(0, half), :] = q_re
            rt[pl.ds(half, half), :] = q_im
        unstage(rt, stage)
        add_rows([(acc, tails, b * LANES, stage, 0)], LANES)
        return 0

    lax.fori_loop(0, edges // LANES, tail_step, 0)


def update_kernel(dim, rows, last, *refs):
    if last:
        core_ref, negs, t4, v, _, nmine, nother, acc, et_out, g_out, stage, rt, rate, outbuf, out_sem = refs
    else:
        core_ref, negs, negs_n, t4, v, _, nmine, nother, acc, new_t4, new_v, nk, ns, stage, rt, rate, nbuf = refs
    core = core_ref[0]
    half = dim // 2
    tops = SLICES * LANES
    rt[pl.ds(dim, tops - dim), :] = jnp.zeros((tops - dim, LANES), F32)

    def neg_step(b, _):
        cols = pl.ds(pl.multiple_of(b * LANES, LANES), LANES)
        rt[pl.ds(pl.multiple_of(core * half, 8), half), :] = nmine[:, cols]
        rt[pl.ds(pl.multiple_of((1 - core) * half, 8), half), :] = nother[:, cols]
        unstage(rt, stage)
        add_rows([(acc, negs, b * LANES, stage, 0)], LANES)
        return 0

    lax.fori_loop(0, nmine.shape[1] // LANES, neg_step, 0)

    blocks = rows // LANES

    def slices(b):
        return [pl.ds(SLICES * LANES * b + j, LANES, stride=SLICES) for j in range(SLICES)]

    def advance(b):
        where = slices(b)
        square = acc[where[0], :] * acc[where[0], :]
        for j in range(1, SLICES):
            square = square + acc[where[j], :] * acc[where[j], :]
        state = v[pl.ds(pl.multiple_of(b * LANES, 8), LANES), :] + jnp.sum(square, axis=1, keepdims=True) / dim
        return state, LEARN_RATE / jnp.sqrt(state + ADA_EPS)

    if not last:
        def open_block(b):
            state, step_size = advance(b)
            new_v[pl.ds(pl.multiple_of(b * LANES, 8), LANES), :] = state
            rate[...] = step_size

        def close_block(b, step_size):
            for w in slices(b):
                new_t4[w, :] = t4[w, :] - acc[w, :] * step_size

        def ada_step(b, _):
            step_size = rate[...]
            close_block(b - 1, step_size)
            open_block(b)
            return 0

        open_block(0)
        lax.fori_loop(1, blocks, ada_step, 0)
        close_block(blocks - 1, rate[...])
        new_t4[pl.ds(rows * SLICES, 32), :] = jnp.zeros((32, LANES), F32)
        gather_negs(dim, core, new_t4, negs_n, nk, ns, nbuf, stage)
        return

    width = outbuf.shape[2]
    per = width // LANES
    steps = rows // width

    def save(step, slot):
        return pltpu.make_async_copy(outbuf.at[slot], et_out.at[:, pl.ds(pl.multiple_of(step * width, LANES), width)], out_sem.at[slot])

    def open_last(b):
        state, step_size = advance(b)
        g_out[pl.ds(b, 1), :] = state.T[:1]
        rate[...] = step_size

    open_last(0)

    def exit_step(step, _):
        slot = lax.rem(step, 2)

        @pl.when(step >= 2)
        def _():
            save(step - 2, slot).wait()

        for i in range(per):
            b = step * per + i
            step_size = rate[...]
            for j, w in enumerate(slices(b)):
                size = min(LANES, dim - j * LANES)
                outbuf[slot, pl.ds(j * LANES, size), pl.ds(i * LANES, LANES)] = (t4[w, :] - acc[w, :] * step_size).T[:size]
            open_last(jnp.minimum(b + 1, blocks - 1))
        save(step, slot).start()
        return 0

    lax.fori_loop(0, steps, exit_step, 0)
    save(steps - 2, (steps - 2) % 2).wait()
    save(steps - 1, (steps - 1) % 2).wait()


def padded_bytes(dims, dtype):
    size = jnp.dtype(dtype).itemsize
    dims = (1,) * (2 - len(dims)) + tuple(dims)
    total = ceil_to(dims[-2], 32 // size) * ceil_to(dims[-1], LANES) * size
    for d in dims[:-2]:
        total *= d
    return total


def cost(micros):
    return pl.CostEstimate(flops=int(micros * 5e6), bytes_accessed=0, transcendentals=0)


def shape(dims, dtype=F32):
    return jax.ShapeDtypeStruct(dims, dtype)


def solution(mesh):
    ent_size = mesh.shape['ent']
    row_spec = P(('sweep', 'ent'), None)
    flat_spec = P(('sweep', 'ent'))
    rel_spec = P('sweep', None)
    state_spec = P('sweep')
    edge_spec = P(('sweep', 'ent'), None, None)
    swap = [(i, i ^ 1) for i in range(ent_size)]
    cross = [(i, i ^ 2) for i in range(ent_size)]

    def shift(amount):
        return [(i, (i + amount) % ent_size) for i in range(ent_size)]

    tie = lax.optimization_barrier

    def chip_sum(keep, send):
        return keep + lax.ppermute(send, 'ent', swap)

    def send(value, pairs):
        return lax.ppermute(value, 'ent', pairs)

    def link(part):
        return send(part, cross)

    def finish(part, got):
        mine = part + got
        return mine, lax.ppermute(mine, 'ent', swap)

    def device_fn(ent_emb, ent_ada, rel_emb, rel_ada, head_idx, tail_idx, rel_idx, edge_mask, neg_idx):
        rows, dim = ent_emb.shape
        num_rel = rel_emb.shape[0]
        _, rounds, edges = head_idx.shape
        neg_count = neg_idx.shape[1]
        negp = ceil_to(neg_count, 2 * LANES)
        relp = ceil_to(num_rel, LANES)
        half = dim // 2
        my_dev = lax.axis_index('ent')
        core = (my_dev % 2).reshape(1)

        heads = [head_idx[0, s] * SLICES for s in range(rounds)]
        own_tails = [tail_idx[0, s] * SLICES for s in range(rounds)]
        own_rels = [rel_idx[0, s] * SLICES for s in range(rounds)]
        tails, rels = [own_tails[0]], [own_rels[0]]
        for s in range(1, rounds):
            got = send(jnp.stack([own_tails[s], own_rels[s]]), shift(s))
            tails.append(got[0])
            rels.append(got[1])
        owned = (neg_idx // rows) == my_dev
        neg_local = jnp.where(owned, neg_idx % rows, rows) * SLICES
        neg_local = jnp.pad(neg_local, ((0, 0), (0, negp - neg_count)), constant_values=rows * SLICES)
        negs = [neg_local[s] for s in range(rounds)]
        weights = edge_mask[0].astype(F32)

        wide_rows = (rows + 8) * SLICES
        stage_shape = pltpu.VMEM((SLICES * LANES, LANES), F32)
        square_shape = pltpu.VMEM((SLICES * LANES, LANES), F32)
        table_out, state_out = shape((wide_rows, LANES)), shape((rows, LANES))
        cols_bf = shape((dim, edges), BF16)
        neg_half = shape((dim, negp // 2), BF16)

        def call(kernel, args, kinds, outs, out_kinds, scratch, micros, aliases=None):
            places = {'s': smem, 'h': hbm, 'v': vmem, 'V': vmem}
            windows = [a for a, k in zip(list(args) + outs, kinds + out_kinds) if k == 'v']
            limit = 3 * 2 ** 20 + sum(padded_bytes(a.shape, a.dtype) for a in windows)
            limit += sum(padded_bytes(a.shape, a.dtype) for a in scratch if a.memory_space == pltpu.VMEM)
            args = [pltpu.with_memory_space_constraint(a, pltpu.VMEM) if k == 'V' else a for a, k in zip(args, kinds)]
            outs = [pltpu.VMEM(o.shape, o.dtype) if k == 'V' else o for o, k in zip(outs, out_kinds)]
            return pl.pallas_call(
                kernel, out_shape=outs, in_specs=[places[k]() for k in kinds], out_specs=[places[k]() for k in out_kinds],
                scratch_shapes=scratch, compiler_params=pltpu.CompilerParams(vmem_limit_bytes=limit),
                input_output_aliases=aliases or {}, cost_estimate=cost(micros))(*args)

        def gather(lists, t4):
            return call(functools.partial(gather_kernel, dim, len(lists)), lists + [t4], 's' * len(lists) + 'V',
                        [cols_bf] * len(lists), 'V' * len(lists), [stage_shape], 1 + 5 * len(lists))

        t4, v, nk, ns = call(
            functools.partial(entry_kernel, dim, rows), [core, negs[0], pltpu.with_memory_space_constraint(ent_emb.T, pltpu.HBM), ent_ada.reshape(rows // LANES, LANES)], 'sshv',
            [table_out, state_out, neg_half, neg_half], 'VVVV',
            [pltpu.VMEM((4, SLICES * LANES, 4 * LANES), F32), stage_shape, pltpu.VMEM((dim, negp), BF16), pltpu.SemaphoreType.DMA((4,))], 20)

        rfm = jnp.pad(rel_emb.T, ((0, 0), (0, relp - num_rel)))
        vr = jnp.pad(rel_ada, (0, relp - num_rel), constant_values=1.0).reshape(1, relp)
        losses = []
        rel_grads = None
        for s in range(rounds):
            first, last = s == 0, s == rounds - 1
            neg_part = chip_sum(nk, ns)
            if first:
                neg_part, t4, tails, rels = tie((neg_part, t4, tails, rels))
                neg_got = link(neg_part)
                tail_cols, hb = gather([tails[0], heads[0]], t4)
                head_cols = hb
                neg_got, hb = tie((neg_got, hb))
            else:
                neg_part, t4 = tie((neg_part, t4))
                neg_got = link(neg_part)
                tb, = gather([tails[s]], t4)
                tail_cols = send(tb, shift(-s))
                t4, tb = tie((t4, tb))
                hb, = gather([heads[s]], t4)
                rel_got, hb = tie((rel_got, hb))
                rel_grads = finish(rel_part, rel_got)
            wide = shape((dim, edges))
            outs, out_kinds = [wide, wide, shape((relp * SLICES, LANES))], 'VVV'
            args, kinds = [core, own_rels[s], hb, rfm], 'ssV' + ('v' if first else 'V')
            if not first:
                outs += [shape((dim, relp)), shape((1, relp))]
                out_kinds += 'Vv'
                args += [vr] + list(rel_grads)
                kinds += 'vVV'
            res = call(functools.partial(query_kernel, dim, edges, first), args, kinds, outs, out_kinds,
                       [stage_shape, pltpu.VMEM((SLICES * LANES, relp), F32)], 10)
            q, r, r4 = res[:3]
            neg_got, q = tie((neg_got, q))
            nmine, nother = finish(neg_part, neg_got)
            if not first:
                rfm, vr = res[3:]
            e, neg_top, neg_total = call(
                functools.partial(exp_kernel, neg_count, edges), [core, q, nmine, nother], 'sVVV',
                [shape((neg_count, edges)), shape((1, edges)), shape((1, edges))], 'Vvv',
                [pltpu.VMEM((dim, negp), BF16), pltpu.VMEM((negp, dim), BF16), pltpu.VMEM((neg_count, CHUNK), F32)], 8)
            if not first:
                e, tail_cols = tie((e, tail_cols))
                tail_cols, hb = tie((tail_cols, hb))
                head_cols = send(hb, shift(s))
            loss, dp, ds, gk, gs = call(
                functools.partial(score_kernel, dim, neg_count, edges), [core, weights[s].reshape(1, edges), q, tail_cols, e, neg_top, neg_total], 'svVVVvv',
                [shape((1, LANES)), shape((1, edges)), shape((negp, edges), BF16), shape((half, negp)), shape((half, negp))], 'vvVVV',
                [pltpu.VMEM((negp, dim), F32)], 8)
            losses.append(loss[0, 0])
            if not first:
                dp_away = send(dp, shift(s))
            neg_part = chip_sum(gk, gs)
            neg_part, ds = tie((neg_part, ds))
            neg_got = link(neg_part)
            acc, rk, rs = call(
                functools.partial(grad_kernel, dim, edges), [core, own_rels[s], heads[s], ds, dp, tail_cols, hb, r, nmine, nother], 'sssVvVVVVV',
                [table_out, shape((half, relp)), shape((half, relp))], 'VVV',
                [pltpu.VMEM((dim, negp), BF16), pltpu.VMEM((relp * SLICES, LANES), F32), pltpu.VMEM((SLICES * CHUNK, LANES), F32),
                 pltpu.VMEM((SLICES * CHUNK, LANES), F32), pltpu.VMEM((SLICES * LANES, CHUNK), F32)], 15)
            rel_part = chip_sum(rk, rs)
            rel_part, acc = tie((rel_part, acc))
            rel_got = link(rel_part)
            if first:
                args, kinds = [tails[s], dp, q, acc], 'svVV'
            else:
                args, kinds = [tails[s], rels[s], dp_away, head_cols, r4, acc], 'ssvVVV'
            acc, = call(functools.partial(scatter_kernel, dim, edges, first), args, kinds, [table_out], 'V',
                        [stage_shape, square_shape], 12, {len(args) - 1: 0})
            neg_got, acc = tie((neg_got, acc))
            gmine, gother = finish(neg_part, neg_got)
            scratch = [stage_shape, square_shape, pltpu.VMEM((LANES, LANES), F32)]
            if last:
                args, outs, out_kinds = [core, negs[s]], [table_out, shape((dim, rows)), shape((rows // LANES, LANES))], 'Vhv'
                scratch += [pltpu.VMEM((2, dim, 4 * LANES), F32), pltpu.SemaphoreType.DMA((2,))]
                aliases = {4: 0}
            else:
                args = [core, negs[s], negs[s + 1]]
                outs, out_kinds = [table_out, table_out, state_out, neg_half, neg_half], 'VVVVV'
                scratch += [pltpu.VMEM((dim, negp), BF16)]
                aliases = {5: 0, 3: 1, 4: 2}
            res = call(functools.partial(update_kernel, dim, rows, last), args + [t4, v, acc, gmine, gother], 's' * len(args) + 'VVVVV',
                       outs, out_kinds, scratch, 30, aliases)
            if last:
                _, et, g = res
            else:
                _, t4, v, nk, ns = res

        even = core[0] == 0
        rel_grads = finish(rel_part, rel_got)
        rg = jnp.where(even, jnp.concatenate(rel_grads, axis=0), jnp.concatenate(rel_grads[::-1], axis=0))
        new_vr = vr + jnp.mean(rg * rg, axis=0, keepdims=True)
        new_r = rfm - LEARN_RATE * rg / jnp.sqrt(new_vr + ADA_EPS)
        return et.T, g.reshape(rows), new_r[:, :num_rel].T, new_vr[0, :num_rel], jnp.stack(losses)[None, :]

    return jax.shard_map(device_fn, mesh=mesh,
                         in_specs=(row_spec, flat_spec, rel_spec, state_spec, edge_spec, edge_spec, edge_spec, edge_spec, rel_spec),
                         out_specs=(row_spec, flat_spec, rel_spec, state_spec, row_spec), check_vma=False)
```

```python
import functools

import jax
import jax.numpy as jnp
from jax import lax
from jax.experimental import pallas as pl
from jax.experimental.pallas import tpu as pltpu
from jax.sharding import PartitionSpec as P


LEARN_RATE = 0.05
ADA_EPS = 1e-10
LANES = 128
SLICES = 4
CHUNK = 256
BATCH = 4
F32 = jnp.float32
BF16 = jnp.bfloat16


def ceil_to(value, unit):
    return -(-value // unit) * unit


def vmem():
    return pl.BlockSpec(memory_space=pltpu.VMEM)


def smem():
    return pl.BlockSpec(memory_space=pltpu.SMEM)


def hbm():
    return pl.BlockSpec(memory_space=pltpu.MemorySpace.HBM)


def four(index):
    return pl.multiple_of(index, SLICES)


def gather_rows(src, ids, base, stage, count):
    for k in range(count):
        stage[pl.ds(SLICES * k, SLICES), :] = src[pl.ds(four(ids[base + k]), SLICES), :]


def stage_cols(stage, slice_no):
    return stage[pl.ds(slice_no, LANES, stride=SLICES), :].T


def batch_sums(acc, ids, base, rows, row_base):
    index = [ids[base + k] for k in range(BATCH)]
    grads = [rows[pl.ds(four(row_base + SLICES * k), SLICES), :] for k in range(BATCH)]
    total = [acc[pl.ds(four(index[k]), SLICES), :] + grads[k] for k in range(BATCH)]
    for k in range(1, BATCH):
        for earlier in range(k):
            total[k] = total[k] + jnp.where(index[earlier] == index[k], grads[earlier], 0.0)
    return index, total


def add_rows(chains, count):
    for first in range(0, count, BATCH):
        done = [batch_sums(acc, ids, base + first, rows, row_base + SLICES * first) for acc, ids, base, rows, row_base in chains]
        for (acc, *_), (index, total) in zip(chains, done):
            for k in range(BATCH):
                acc[pl.ds(four(index[k]), SLICES), :] = total[k]


def put_halves(core, keep, sent, cols, block_of, dim):
    half = dim // 2
    for side in range(2):
        @pl.when(core == side)
        def _():
            for j in range(SLICES):
                block = block_of(j)
                for h in range(2):
                    lo, hi = max(j * LANES, h * half), min((j + 1) * LANES, (h + 1) * half)
                    if lo < hi:
                        (keep if h == side else sent)[pl.ds(lo - h * half, hi - lo), cols] = block[lo - j * LANES:hi - j * LANES]


def zero_rows(ref, step=1024):
    rows = ref.shape[0]
    whole = rows // step

    def body(i, _):
        ref[pl.ds(pl.multiple_of(i * step, 8), step), :] = jnp.zeros((step, LANES), ref.dtype)
        return 0

    lax.fori_loop(0, whole, body, 0)
    if rows % step:
        ref[pl.ds(whole * step, rows % step), :] = jnp.zeros((rows % step, LANES), ref.dtype)


def gather_out(dim, table, ids, out, stage, count):
    def body(b, _):
        gather_rows(table, ids, b * LANES, stage, LANES)
        cols = pl.ds(pl.multiple_of(b * LANES, LANES), LANES)
        for j in range(SLICES):
            size = min(LANES, dim - j * LANES)
            out[pl.ds(j * LANES, size), cols] = stage_cols(stage, j)[:size].astype(BF16)
        return 0

    lax.fori_loop(0, count // LANES, body, 0)


def gather_negs(dim, core, table, negs, nk, ns, nbuf, stage):
    half = nbuf.shape[1] // 2
    gather_out(dim, table, negs, nbuf, stage, nbuf.shape[1])
    nk[...] = nbuf[:, pl.ds(pl.multiple_of(core * half, LANES), half)]
    ns[...] = nbuf[:, pl.ds(pl.multiple_of((1 - core) * half, LANES), half)]


def entry_kernel(dim, rows, core_ref, negs, et, t4, nk, ns, inbuf, stage, nbuf, in_sem):
    cols = inbuf.shape[2]
    steps = rows // cols
    per = cols // LANES

    def fetch(step, slot):
        return pltpu.make_async_copy(et.at[:, pl.ds(pl.multiple_of(step * cols, LANES), cols)],
                                     inbuf.at[slot, pl.ds(0, dim)], in_sem.at[slot])

    slots = inbuf.shape[0]
    for slot in range(slots - 1):
        fetch(slot, slot).start()
    for slot in range(slots):
        inbuf[slot, pl.ds(dim, SLICES * LANES - dim), :] = jnp.zeros((SLICES * LANES - dim, cols), F32)
    t4[pl.ds(rows * SLICES, 32), :] = jnp.zeros((32, LANES), F32)

    def body(step, _):
        slot = lax.rem(step, slots)

        @pl.when(step + slots - 1 < steps)
        def _():
            fetch(step + slots - 1, lax.rem(step + slots - 1, slots)).start()

        fetch(step, slot).wait()
        for b in range(per):
            row0 = (step * per + b) * LANES
            for j in range(SLICES):
                t4[pl.ds(SLICES * row0 + j, LANES, stride=SLICES), :] = inbuf[slot, pl.ds(j * LANES, LANES), pl.ds(b * LANES, LANES)].T
        return 0

    lax.fori_loop(0, steps, body, 0)
    gather_negs(dim, core_ref[0], t4, negs, nk, ns, nbuf, stage)


def gather_kernel(dim, lists, *refs):
    ids, t4, outs, stage = refs[:lists], refs[lists], refs[lists + 1:2 * lists + 1], refs[2 * lists + 1]
    for i in range(lists):
        gather_out(dim, t4, ids[i], outs[i], stage, outs[i].shape[1])


def query_kernel(dim, edges, first, *refs):
    if first:
        core_ref, rel, hb, rfm, q_out, r_out, r4, stage, fm = refs
    else:
        core_ref, rel, hb, rfm_in, vr_in, rmine, rother, q_out, r_out, r4, rfm, vr, stage, fm = refs
        core = core_ref[0]
    half = dim // 2
    relp = rfm.shape[1]
    tops = SLICES * LANES
    if not first:
        fm[pl.ds(pl.multiple_of(core * half, 8), half), :] = rmine[...]
        fm[pl.ds(pl.multiple_of((1 - core) * half, 8), half), :] = rother[...]
        grad = fm[pl.ds(0, dim), :]
        vr[...] = vr_in[...] + jnp.sum(grad * grad, axis=0, keepdims=True) / dim
        rate = LEARN_RATE / jnp.sqrt(vr[...] + ADA_EPS)
        rfm[...] = rfm_in[...] - fm[pl.ds(0, dim), :] * rate
    fm[pl.ds(dim, tops - dim), pl.ds(0, LANES)] = jnp.zeros((tops - dim, LANES), F32)
    for b in range(relp // LANES):
        for j in range(SLICES):
            if (j + 1) * LANES <= dim:
                block = rfm[pl.ds(j * LANES, LANES), pl.ds(b * LANES, LANES)]
            else:
                fm[pl.ds(j * LANES, dim - j * LANES), pl.ds(0, LANES)] = rfm[pl.ds(j * LANES, dim - j * LANES), pl.ds(b * LANES, LANES)]
                block = fm[pl.ds(j * LANES, LANES), pl.ds(0, LANES)]
            r4[pl.ds(SLICES * b * LANES + j, LANES, stride=SLICES), :] = block.T

    def step(b, _):
        cols = pl.ds(pl.multiple_of(b * LANES, LANES), LANES)
        gather_rows(r4, rel, b * LANES, stage, LANES)
        for j in range(SLICES):
            size = min(LANES, dim - j * LANES)
            r_out[pl.ds(j * LANES, size), cols] = stage_cols(stage, j)[:size]
        h = hb[:, cols].astype(F32)
        r_re, r_im = r_out[pl.ds(0, half), cols], r_out[pl.ds(half, half), cols]
        q_out[pl.ds(0, half), cols] = h[:half] * r_re - h[half:] * r_im
        q_out[pl.ds(half, half), cols] = h[:half] * r_im + h[half:] * r_re
        return 0

    lax.fori_loop(0, edges // LANES, step, 0)


def place_negs(core, nb, nfull, nother):
    nhalf = nfull.shape[1]
    nb[:, pl.ds(pl.multiple_of(core * nhalf, LANES), nhalf)] = nfull[...]
    nb[:, pl.ds(pl.multiple_of((1 - core) * nhalf, LANES), nhalf)] = nother[...]


def exp_kernel(neg_count, edges, core_ref, q, nfull, nother, e_out, top_out, sum_out, nb, nbt, sc):
    negp = nb.shape[1]
    place_negs(core_ref[0], nb, nfull, nother)
    for b in range(negp // LANES):
        nbt[pl.ds(b * LANES, LANES), :] = nb[:, pl.ds(b * LANES, LANES)].astype(F32).T.astype(BF16)

    def step(c, _):
        cols = pl.ds(pl.multiple_of(c * CHUNK, LANES), CHUNK)
        sc[...] = lax.dot_general(nbt[pl.ds(0, neg_count), :], q[:, cols].astype(BF16), (((1,), (0,)), ((), ())), preferred_element_type=F32)
        top = jnp.max(sc[...], axis=0, keepdims=True)
        top_out[:, cols] = top
        total = jnp.zeros((1, CHUNK), F32)
        part = 200
        for i in range(0, neg_count, part):
            size = min(part, neg_count - i)
            e = jnp.exp(sc[pl.ds(i, size), :] - top)
            e_out[pl.ds(i, size), cols] = e
            total = total + jnp.sum(e, axis=0, keepdims=True)
        sum_out[:, cols] = total
        return 0

    lax.fori_loop(0, edges // CHUNK, step, 0)


def score_kernel(dim, neg_count, edges, core_ref, w, q, tb, e, neg_top, neg_sum,
                 loss, dp_out, ds, nk, ns, ng):
    core = core_ref[0]
    negp = ds.shape[0]
    ng[...] = jnp.zeros(ng.shape, F32)
    ds[pl.ds(neg_count, negp - neg_count), :] = jnp.zeros((negp - neg_count, edges), BF16)

    def step(c, loss_row):
        cols = pl.ds(pl.multiple_of(c * CHUNK, LANES), CHUNK)
        pos = jnp.sum(q[:, cols] * tb[:, cols].astype(F32), axis=0, keepdims=True)
        top = jnp.maximum(pos, neg_top[:, cols])
        pos_exp = jnp.exp(pos - top)
        shrink = jnp.exp(neg_top[:, cols] - top)
        norm = pos_exp + shrink * neg_sum[:, cols]
        wt = w[:, cols]
        loss_row = loss_row + wt * (top + jnp.log(norm) - pos)
        dp_out[:, cols] = wt * (pos_exp / norm - 1.0)
        ds[pl.ds(0, neg_count), cols] = (e[:, cols] * (wt * shrink / norm)).astype(BF16)
        ng[...] += lax.dot_general(ds[:, cols], q[:, cols].astype(BF16), (((1,), (1,)), ((), ())), preferred_element_type=F32)
        return loss_row

    loss_row = lax.fori_loop(0, edges // CHUNK, step, jnp.zeros((1, CHUNK), F32))
    loss[...] = jnp.broadcast_to(jnp.sum(loss_row, axis=1, keepdims=True) / edges, loss.shape)

    def save(b, _):
        rows = pl.ds(pl.multiple_of(b * LANES, LANES), LANES)
        put_halves(core, nk, ns, rows, lambda j: ng[rows, pl.ds(j * LANES, min(LANES, dim - j * LANES))].T, dim)
        return 0

    lax.fori_loop(0, negp // LANES, save, 0)


def grad_kernel(dim, edges, core_ref, rel, ds, dp, tb, hb, r, nfull, nother, hg, rk, rs, nb, racc, stage, qs):
    half = dim // 2
    tops = SLICES * LANES
    place_negs(core_ref[0], nb, nfull, nother)
    zero_rows(racc)
    qs[:, pl.ds(dim, tops - dim), :] = jnp.zeros((2, tops - dim, CHUNK), F32)

    def compute(c, slot):
        cols = pl.ds(pl.multiple_of(c * CHUNK, LANES), CHUNK)
        gq = lax.dot_general(nb[...], ds[:, cols], (((1,), (0,)), ((), ())), preferred_element_type=F32) + dp[:, cols] * tb[:, cols].astype(F32)
        g_re, g_im = gq[:half], gq[half:]
        h = hb[:, cols].astype(F32)
        h_re, h_im = h[:half], h[half:]
        r_re, r_im = r[pl.ds(0, half), cols], r[pl.ds(half, half), cols]
        for part, (f_re, f_im) in enumerate(((h_re, h_im), (r_re, r_im))):
            qs[part, pl.ds(0, half), :] = g_re * f_re + g_im * f_im
            qs[part, pl.ds(half, half), :] = g_im * f_re - g_re * f_im
        for b in range(CHUNK // LANES):
            for j in range(SLICES):
                place = pl.ds(j * LANES, LANES), pl.ds(b * LANES, LANES)
                stage[slot, pl.ds(SLICES * b * LANES + j, LANES, stride=SLICES), :] = qs[(0,) + place].T
                hg[pl.ds(SLICES * (c * CHUNK + b * LANES) + j, LANES, stride=SLICES), :] = qs[(1,) + place].T

    def scatter(c, slot):
        add_rows([(racc, rel, c * CHUNK, stage.at[slot], 0)], CHUNK)

    compute(0, 0)

    def step(i, _):
        for slot in range(2):
            c = 2 * i + slot
            scatter(c, slot)
            compute(jnp.minimum(c + 1, edges // CHUNK - 1), 1 - slot)
        return 0

    lax.fori_loop(0, edges // CHUNK // 2, step, 0)

    def save(b, _):
        cols = pl.ds(pl.multiple_of(b * LANES, LANES), LANES)
        put_halves(core_ref[0], rk, rs, cols, lambda j: racc[pl.ds(SLICES * LANES * b + j, LANES, stride=SLICES), :].T, dim)
        return 0

    lax.fori_loop(0, rk.shape[1] // LANES, save, 0)


def unstage(rt, stage):
    for j in range(SLICES):
        stage[pl.ds(j, LANES, stride=SLICES), :] = rt[pl.ds(j * LANES, LANES), :].T


def scatter_kernel(dim, edges, own, *refs):
    if own:
        heads, tails, hg, dp, q, acc, stage, rows, rt = refs
    else:
        heads, tails, rel, hg, dp, hb_in, r4, acc, stage, rows, rt = refs
    half = dim // 2
    blocks = edges // LANES
    zero_rows(acc)
    rt[:, pl.ds(dim, SLICES * LANES - dim), :] = jnp.zeros((2, SLICES * LANES - dim, LANES), F32)

    def compute(b, slot):
        cols = pl.ds(pl.multiple_of(b * LANES, LANES), LANES)
        scale = dp[:, cols]
        if own:
            rt[1, pl.ds(0, dim), :] = q[:, cols] * scale
        else:
            gather_rows(r4, rel, b * LANES, stage, LANES)
            for j in range(SLICES):
                rt[0, pl.ds(j * LANES, LANES), :] = stage_cols(stage, j)
            h = hb_in[:, cols].astype(F32)
            r_re, r_im = rt[0, pl.ds(0, half), :], rt[0, pl.ds(half, half), :]
            rt[1, pl.ds(0, half), :] = scale * (h[:half] * r_re - h[half:] * r_im)
            rt[1, pl.ds(half, half), :] = scale * (h[:half] * r_im + h[half:] * r_re)
        unstage(rt.at[1], rows.at[slot])

    compute(0, 0)

    def step(i, _):
        for slot in range(2):
            b = 2 * i + slot
            add_rows([(acc, tails, b * LANES, rows.at[slot], 0)], LANES)
            add_rows([(acc, heads, b * LANES, hg, b * LANES * SLICES)], LANES)
            compute(jnp.minimum(b + 1, blocks - 1), 1 - slot)
        return 0

    lax.fori_loop(0, blocks // 2, step, 0)


def update_kernel(dim, rows, last, *refs):
    if last:
        core_ref, negs, t4, v, _, nmine, nother, acc, et_out, g_out, stage, rt, rate, outbuf, out_sem = refs
    else:
        core_ref, negs, negs_n, old_t4, v, _, nmine, nother, acc, t4, new_v, nk, ns, stage, rt, rate, nbuf = refs
    core = core_ref[0]
    half = dim // 2
    rt[pl.ds(dim, SLICES * LANES - dim), :] = jnp.zeros((SLICES * LANES - dim, LANES), F32)

    def neg_step(b, _):
        cols = pl.ds(pl.multiple_of(b * LANES, LANES), LANES)
        rt[pl.ds(pl.multiple_of(core * half, 8), half), :] = nmine[:, cols]
        rt[pl.ds(pl.multiple_of((1 - core) * half, 8), half), :] = nother[:, cols]
        unstage(rt, stage)
        add_rows([(acc, negs, b * LANES, stage, 0)], LANES)
        return 0

    lax.fori_loop(0, nmine.shape[1] // LANES, neg_step, 0)

    blocks = rows // LANES

    def slices(b):
        return [pl.ds(SLICES * LANES * b + j, LANES, stride=SLICES) for j in range(SLICES)]

    def advance(b, out):
        where = slices(b)
        square = acc[where[0], :] * acc[where[0], :]
        for j in range(1, SLICES):
            square = square + acc[where[j], :] * acc[where[j], :]
        state = v[pl.ds(b, 1), :] + jnp.sum(square.T, axis=0, keepdims=True) / dim
        out[pl.ds(b, 1), :] = state
        return jnp.broadcast_to(LEARN_RATE / jnp.sqrt(state + ADA_EPS), (LANES, LANES)).T

    if not last:
        def open_pair(p):
            steps = [advance(2 * p + i, new_v) for i in range(2)]
            for i in range(2):
                rate[i] = steps[i]

        def close_pair(p, steps):
            for i in range(2):
                for w in slices(2 * p + i):
                    t4[w, :] = old_t4[w, :] - acc[w, :] * steps[i]

        def ada_step(p, _):
            steps = [rate[0], rate[1]]
            close_pair(p - 1, steps)
            open_pair(p)
            return 0

        open_pair(0)
        lax.fori_loop(1, blocks // 2, ada_step, 0)
        close_pair(blocks // 2 - 1, [rate[0], rate[1]])
        t4[pl.ds(rows * SLICES, 32), :] = jnp.zeros((32, LANES), F32)
        gather_negs(dim, core, t4, negs_n, nk, ns, nbuf, stage)
        return

    width = outbuf.shape[2]
    per = width // LANES
    steps = rows // width

    def save(step, slot):
        return pltpu.make_async_copy(outbuf.at[slot], et_out.at[:, pl.ds(pl.multiple_of(step * width, LANES), width)], out_sem.at[slot])

    def open_group(step, slot):
        for i in range(per):
            rate[slot, i] = advance(step * per + i, g_out)

    open_group(0, 0)

    def exit_step(step, _):
        slot = lax.rem(step, 2)

        @pl.when(step >= 2)
        def _():
            save(step - 2, slot).wait()

        for i in range(per):
            step_size = rate[slot, i]
            for j, w in enumerate(slices(step * per + i)):
                size = min(LANES, dim - j * LANES)
                outbuf[slot, pl.ds(j * LANES, size), pl.ds(i * LANES, LANES)] = (t4[w, :] - acc[w, :] * step_size).T[:size]
        open_group(jnp.minimum(step + 1, steps - 1), 1 - slot)
        save(step, slot).start()
        return 0

    lax.fori_loop(0, steps, exit_step, 0)
    save(steps - 2, (steps - 2) % 2).wait()
    save(steps - 1, (steps - 1) % 2).wait()


def padded_bytes(dims, dtype):
    size = jnp.dtype(dtype).itemsize
    dims = (1,) * (2 - len(dims)) + tuple(dims)
    total = ceil_to(dims[-2], 32 // size) * ceil_to(dims[-1], LANES) * size
    for d in dims[:-2]:
        total *= d
    return total


def cost(micros):
    return pl.CostEstimate(flops=int(micros * 5e6), bytes_accessed=0, transcendentals=0)


def shape(dims, dtype=F32):
    return jax.ShapeDtypeStruct(dims, dtype)


def solution(mesh):
    ent_size = mesh.shape['ent']
    row_spec = P(('sweep', 'ent'), None)
    flat_spec = P(('sweep', 'ent'))
    rel_spec = P('sweep', None)
    state_spec = P('sweep')
    edge_spec = P(('sweep', 'ent'), None, None)
    swap = [(i, i ^ 1) for i in range(ent_size)]
    cross = [(i, i ^ 2) for i in range(ent_size)]

    def shift(amount):
        return [(i, (i + amount) % ent_size) for i in range(ent_size)]

    tie = lax.optimization_barrier

    def chip_sum(keep, send):
        return keep + lax.ppermute(send, 'ent', swap)

    def send(value, pairs):
        return lax.ppermute(value, 'ent', pairs)

    def link(part):
        return send(part, cross)

    def finish(part, got):
        mine = part + got
        return mine, lax.ppermute(mine, 'ent', swap)

    def device_fn(ent_emb, ent_ada, rel_emb, rel_ada, head_idx, tail_idx, rel_idx, edge_mask, neg_idx):
        rows, dim = ent_emb.shape
        num_rel = rel_emb.shape[0]
        _, rounds, edges = head_idx.shape
        neg_count = neg_idx.shape[1]
        negp = ceil_to(neg_count, 2 * LANES)
        relp = ceil_to(num_rel, LANES)
        half = dim // 2
        my_dev = lax.axis_index('ent')
        core = (my_dev % 2).reshape(1)

        heads = [head_idx[0, s] * SLICES for s in range(rounds)]
        own_tails = [tail_idx[0, s] * SLICES for s in range(rounds)]
        own_rels = [rel_idx[0, s] * SLICES for s in range(rounds)]
        tails, rels = [own_tails[0]], [own_rels[0]]
        for s in range(1, rounds):
            got = send(jnp.stack([own_tails[s], own_rels[s]]), shift(s))
            tails.append(got[0])
            rels.append(got[1])
        owned = (neg_idx // rows) == my_dev
        neg_local = jnp.where(owned, neg_idx % rows, rows) * SLICES
        neg_local = jnp.pad(neg_local, ((0, 0), (0, negp - neg_count)), constant_values=rows * SLICES)
        negs = [neg_local[s] for s in range(rounds)]
        weights = edge_mask[0].astype(F32)

        wide_rows = (rows + 8) * SLICES
        stage_shape = pltpu.VMEM((SLICES * LANES, LANES), F32)
        square_shape = pltpu.VMEM((SLICES * LANES, LANES), F32)
        table_out, state_out = shape((wide_rows, LANES)), shape((rows // LANES, LANES))
        cols_bf = shape((dim, edges), BF16)
        neg_half = shape((dim, negp // 2), BF16)

        def call(kernel, args, kinds, outs, out_kinds, scratch, micros, name, aliases=None):
            places = {'s': smem, 'h': hbm, 'v': vmem, 'V': vmem}
            windows = [a for a, k in zip(list(args) + outs, kinds + out_kinds) if k == 'v']
            limit = (4 if name == 'grad' else 3) * 2 ** 20 + sum(padded_bytes(a.shape, a.dtype) for a in windows)
            limit += sum(padded_bytes(a.shape, a.dtype) for a in scratch if a.memory_space == pltpu.VMEM)
            args = [pltpu.with_memory_space_constraint(a, pltpu.VMEM) if k == 'V' else a for a, k in zip(args, kinds)]
            outs = [pltpu.VMEM(o.shape, o.dtype) if k == 'V' else o for o, k in zip(outs, out_kinds)]
            return pl.pallas_call(
                kernel, out_shape=outs, in_specs=[places[k]() for k in kinds], out_specs=[places[k]() for k in out_kinds],
                scratch_shapes=scratch, compiler_params=pltpu.CompilerParams(vmem_limit_bytes=limit),
                input_output_aliases=aliases or {}, cost_estimate=cost(micros))(*args)

        def gather(lists, t4):
            return call(functools.partial(gather_kernel, dim, len(lists)), lists + [t4], 's' * len(lists) + 'V',
                        [cols_bf] * len(lists), 'V' * len(lists), [stage_shape], 1 + 5 * len(lists), 'gather')

        t4, nk, ns = call(
            functools.partial(entry_kernel, dim, rows), [core, negs[0], pltpu.with_memory_space_constraint(ent_emb.T, pltpu.HBM)], 'ssh',
            [table_out, neg_half, neg_half], 'VVV',
            [pltpu.VMEM((4, SLICES * LANES, 4 * LANES), F32), stage_shape, pltpu.VMEM((dim, negp), BF16), pltpu.SemaphoreType.DMA((4,))], 20, 'entry')
        v = ent_ada.reshape(rows // LANES, LANES)

        rfm = jnp.pad(rel_emb.T, ((0, 0), (0, relp - num_rel)))
        vr = jnp.pad(rel_ada, (0, relp - num_rel), constant_values=1.0).reshape(1, relp)
        losses = []
        rel_grads = None
        for s in range(rounds):
            first, last = s == 0, s == rounds - 1
            neg_part = chip_sum(nk, ns)
            if first:
                neg_part, t4, tails, rels = tie((neg_part, t4, tails, rels))
                neg_got = link(neg_part)
                tail_cols, hb = gather([tails[0], heads[0]], t4)
                head_cols = hb
                neg_got, hb = tie((neg_got, hb))
            else:
                neg_part, t4 = tie((neg_part, t4))
                neg_got = link(neg_part)
                tb, = gather([tails[s]], t4)
                tail_cols = send(tb, shift(-s))
                t4, tb = tie((t4, tb))
                hb, = gather([heads[s]], t4)
                rel_got, hb = tie((rel_got, hb))
                rel_grads = finish(rel_part, rel_got)
            wide = shape((dim, edges))
            outs, out_kinds = [wide, wide, shape((relp * SLICES, LANES))], 'VVV'
            args, kinds = [core, own_rels[s], hb, rfm], 'ssV' + ('v' if first else 'V')
            if not first:
                outs += [shape((dim, relp)), shape((1, relp))]
                out_kinds += 'Vv'
                args += [vr] + list(rel_grads)
                kinds += 'vVV'
            res = call(functools.partial(query_kernel, dim, edges, first), args, kinds, outs, out_kinds,
                       [stage_shape, pltpu.VMEM((SLICES * LANES, relp), F32)], 10, 'query')
            q, r, r4 = res[:3]
            neg_got, q = tie((neg_got, q))
            nmine, nother = finish(neg_part, neg_got)
            if not first:
                rfm, vr = res[3:]
            e, neg_top, neg_total = call(
                functools.partial(exp_kernel, neg_count, edges), [core, q, nmine, nother], 'sVVV',
                [shape((neg_count, edges)), shape((1, edges)), shape((1, edges))], 'Vvv',
                [pltpu.VMEM((dim, negp), BF16), pltpu.VMEM((negp, dim), BF16), pltpu.VMEM((neg_count, CHUNK), F32)], 8, 'exp')
            if not first:
                e, tail_cols = tie((e, tail_cols))
                tail_cols, hb = tie((tail_cols, hb))
                head_cols = send(hb, shift(s))
            loss, dp, ds, gk, gs = call(
                functools.partial(score_kernel, dim, neg_count, edges), [core, weights[s].reshape(1, edges), q, tail_cols, e, neg_top, neg_total], 'svVVVvv',
                [shape((1, LANES)), shape((1, edges)), shape((negp, edges), BF16), shape((half, negp)), shape((half, negp))], 'vvVVV',
                [pltpu.VMEM((negp, dim), F32)], 8, 'score')
            losses.append(loss[0, 0])
            if not first:
                dp_away = send(dp, shift(s))
            neg_part = chip_sum(gk, gs)
            neg_part, ds = tie((neg_part, ds))
            neg_got = link(neg_part)
            hg, rk, rs = call(
                functools.partial(grad_kernel, dim, edges), [core, own_rels[s], ds, dp, tail_cols, hb, r, nmine, nother], 'ssVvVVVVV',
                [shape((edges * SLICES, LANES)), shape((half, relp)), shape((half, relp))], 'VVV',
                [pltpu.VMEM((dim, negp), BF16), pltpu.VMEM((relp * SLICES, LANES), F32), pltpu.VMEM((2, SLICES * CHUNK, LANES), F32),
                 pltpu.VMEM((2, SLICES * LANES, CHUNK), F32)], 12, 'grad')
            rel_part = chip_sum(rk, rs)
            rel_part, hg = tie((rel_part, hg))
            rel_got = link(rel_part)
            if first:
                args, kinds = [heads[s], tails[s], hg, dp, q], 'ssVvV'
            else:
                args, kinds = [heads[s], tails[s], rels[s], hg, dp_away, head_cols, r4], 'sssVvVV'
            acc, = call(functools.partial(scatter_kernel, dim, edges, first), args, kinds, [table_out], 'V',
                        [stage_shape] + [pltpu.VMEM((2, SLICES * LANES, LANES), F32)] * 2, 15, 'scatter')
            neg_got, acc = tie((neg_got, acc))
            gmine, gother = finish(neg_part, neg_got)
            scratch = [stage_shape, square_shape, pltpu.VMEM((2, 4, LANES, LANES) if last else (2, LANES, LANES), F32)]
            if last:
                args, kinds = [core, negs[s], t4, v, acc], 'ssVVV'
                outs, out_kinds = [table_out, shape((dim, rows)), shape((rows // LANES, LANES))], 'Vhv'
                scratch += [pltpu.VMEM((2, dim, 4 * LANES), F32), pltpu.SemaphoreType.DMA((2,))]
                aliases = {4: 0}
            else:
                args, kinds = [core, negs[s], negs[s + 1], t4, v, acc], 'sssVVV'
                outs, out_kinds = [table_out, table_out, state_out, neg_half, neg_half], 'VVVVV'
                scratch += [pltpu.VMEM((dim, negp), BF16)]
                aliases = {5: 0, 3: 1, 4: 2}
            res = call(functools.partial(update_kernel, dim, rows, last), args + [gmine, gother], kinds + 'VV',
                       outs, out_kinds, scratch, 30, 'update', aliases)
            if last:
                _, et, g = res
            else:
                _, t4, v, nk, ns = res

        even = core[0] == 0
        rel_grads = finish(rel_part, rel_got)
        rg = jnp.where(even, jnp.concatenate(rel_grads, axis=0), jnp.concatenate(rel_grads[::-1], axis=0))
        new_vr = vr + jnp.mean(rg * rg, axis=0, keepdims=True)
        new_r = rfm - LEARN_RATE * rg / jnp.sqrt(new_vr + ADA_EPS)
        return et.T, g.reshape(rows), new_r[:, :num_rel].T, new_vr[0, :num_rel], jnp.stack(losses)[None, :]

    return jax.shard_map(device_fn, mesh=mesh,
                         in_specs=(row_spec, flat_spec, rel_spec, state_spec, edge_spec, edge_spec, edge_spec, edge_spec, rel_spec),
                         out_specs=(row_spec, flat_spec, rel_spec, state_spec, row_spec), check_vma=False)
```

```python
import functools

import jax
import jax.numpy as jnp
from jax import lax
from jax.experimental import pallas as pl
from jax.experimental.pallas import tpu as pltpu
from jax.sharding import PartitionSpec as P


LEARN_RATE = 0.05
ADA_EPS = 1e-10
LANES = 128
SLICES = 4
CHUNK = 256
BATCH = 4
F32 = jnp.float32
BF16 = jnp.bfloat16


def ceil_to(value, unit):
    return -(-value // unit) * unit


def vmem():
    return pl.BlockSpec(memory_space=pltpu.VMEM)


def smem():
    return pl.BlockSpec(memory_space=pltpu.SMEM)


def hbm():
    return pl.BlockSpec(memory_space=pltpu.MemorySpace.HBM)


def four(index):
    return pl.multiple_of(index, SLICES)


def gather_rows(src, ids, base, stage, count):
    for k in range(count):
        stage[pl.ds(SLICES * k, SLICES), :] = src[pl.ds(four(ids[base + k]), SLICES), :]


def stage_cols(stage, slice_no):
    return stage[pl.ds(slice_no, LANES, stride=SLICES), :].T


def batch_sums(acc, ids, base, rows, row_base):
    index = [ids[base + k] for k in range(BATCH)]
    grads = [rows[pl.ds(four(row_base + SLICES * k), SLICES), :] for k in range(BATCH)]
    total = []
    for k in range(BATCH):
        repeats = [jnp.where(index[earlier] == index[k], grads[earlier], 0.0) for earlier in range(k)]
        total.append(functools.reduce(jnp.add, repeats, grads[k]))
    total = [acc[pl.ds(four(index[k]), SLICES), :] + total[k] for k in range(BATCH)]
    return index, total


def add_rows(chains, count):
    for first in range(0, count, BATCH):
        done = [batch_sums(acc, ids, base + first, rows, row_base + SLICES * first) for acc, ids, base, rows, row_base in chains]
        for (acc, *_), (index, total) in zip(chains, done):
            for k in range(BATCH):
                acc[pl.ds(four(index[k]), SLICES), :] = total[k]


def put_halves(core, keep, sent, cols, block_of, dim):
    half = dim // 2
    for side in range(2):
        @pl.when(core == side)
        def _():
            for j in range(SLICES):
                block = block_of(j)
                for h in range(2):
                    lo, hi = max(j * LANES, h * half), min((j + 1) * LANES, (h + 1) * half)
                    if lo < hi:
                        (keep if h == side else sent)[pl.ds(lo - h * half, hi - lo), cols] = block[lo - j * LANES:hi - j * LANES]


def zero_rows(ref, step=1024):
    rows = ref.shape[0]
    whole = rows // step

    def body(i, _):
        ref[pl.ds(pl.multiple_of(i * step, 8), step), :] = jnp.zeros((step, LANES), ref.dtype)
        return 0

    lax.fori_loop(0, whole, body, 0)
    if rows % step:
        ref[pl.ds(whole * step, rows % step), :] = jnp.zeros((rows % step, LANES), ref.dtype)


def gather_out(dim, table, ids, out, stage, count):
    def body(b, _):
        gather_rows(table, ids, b * LANES, stage, LANES)
        cols = pl.ds(pl.multiple_of(b * LANES, LANES), LANES)
        for j in range(SLICES):
            size = min(LANES, dim - j * LANES)
            out[pl.ds(j * LANES, size), cols] = stage_cols(stage, j)[:size].astype(BF16)
        return 0

    lax.fori_loop(0, count // LANES, body, 0)


def gather_negs(dim, core, table, negs, nk, ns, nbuf, stage):
    half = nbuf.shape[1] // 2
    gather_out(dim, table, negs, nbuf, stage, nbuf.shape[1])
    nk[...] = nbuf[:, pl.ds(pl.multiple_of(core * half, LANES), half)]
    ns[...] = nbuf[:, pl.ds(pl.multiple_of((1 - core) * half, LANES), half)]


def entry_kernel(dim, rows, core_ref, negs, et, t4, nk, ns, inbuf, stage, nbuf, in_sem):
    cols = inbuf.shape[2]
    steps = rows // cols
    per = cols // LANES

    def fetch(step, slot):
        return pltpu.make_async_copy(et.at[:, pl.ds(pl.multiple_of(step * cols, LANES), cols)],
                                     inbuf.at[slot, pl.ds(0, dim)], in_sem.at[slot])

    slots = inbuf.shape[0]
    for slot in range(slots - 1):
        fetch(slot, slot).start()
    for slot in range(slots):
        inbuf[slot, pl.ds(dim, SLICES * LANES - dim), :] = jnp.zeros((SLICES * LANES - dim, cols), F32)
    t4[pl.ds(rows * SLICES, 32), :] = jnp.zeros((32, LANES), F32)

    def body(step, _):
        slot = lax.rem(step, slots)

        @pl.when(step + slots - 1 < steps)
        def _():
            fetch(step + slots - 1, lax.rem(step + slots - 1, slots)).start()

        fetch(step, slot).wait()
        for b in range(per):
            row0 = (step * per + b) * LANES
            for j in range(SLICES):
                t4[pl.ds(SLICES * row0 + j, LANES, stride=SLICES), :] = inbuf[slot, pl.ds(j * LANES, LANES), pl.ds(b * LANES, LANES)].T
        return 0

    lax.fori_loop(0, steps, body, 0)
    gather_negs(dim, core_ref[0], t4, negs, nk, ns, nbuf, stage)


def gather_kernel(dim, lists, *refs):
    ids, t4, outs, stage = refs[:lists], refs[lists], refs[lists + 1:2 * lists + 1], refs[2 * lists + 1]
    for i in range(lists):
        gather_out(dim, t4, ids[i], outs[i], stage, outs[i].shape[1])


def query_kernel(dim, edges, first, *refs):
    if first:
        core_ref, rel, hb, rfm, q_out, r_out, stage, fm, r4 = refs
    else:
        core_ref, rel, hb, rfm_in, vr_in, rmine, rother, q_out, r_out, r4_out, rfm, vr, stage, fm, r4, out_sem = refs
        core = core_ref[0]
    half = dim // 2
    relp = rfm.shape[1]
    tops = SLICES * LANES
    if not first:
        fm[pl.ds(pl.multiple_of(core * half, 8), half), :] = rmine[...]
        fm[pl.ds(pl.multiple_of((1 - core) * half, 8), half), :] = rother[...]
        grad = fm[pl.ds(0, dim), :]
        vr[...] = vr_in[...] + jnp.sum(grad * grad, axis=0, keepdims=True) / dim
        rate = LEARN_RATE / jnp.sqrt(vr[...] + ADA_EPS)
        rfm[...] = rfm_in[...] - fm[pl.ds(0, dim), :] * rate
    fm[pl.ds(dim, tops - dim), pl.ds(0, LANES)] = jnp.zeros((tops - dim, LANES), F32)
    for b in range(relp // LANES):
        for j in range(SLICES):
            if (j + 1) * LANES <= dim:
                block = rfm[pl.ds(j * LANES, LANES), pl.ds(b * LANES, LANES)]
            else:
                fm[pl.ds(j * LANES, dim - j * LANES), pl.ds(0, LANES)] = rfm[pl.ds(j * LANES, dim - j * LANES), pl.ds(b * LANES, LANES)]
                block = fm[pl.ds(j * LANES, LANES), pl.ds(0, LANES)]
            r4[pl.ds(SLICES * b * LANES + j, LANES, stride=SLICES), :] = block.T

    def step(b, _):
        cols = pl.ds(pl.multiple_of(b * LANES, LANES), LANES)
        gather_rows(r4, rel, b * LANES, stage, LANES)
        for j in range(SLICES):
            size = min(LANES, dim - j * LANES)
            r_out[pl.ds(j * LANES, size), cols] = stage_cols(stage, j)[:size]
        h = hb[:, cols].astype(F32)
        r_re, r_im = r_out[pl.ds(0, half), cols], r_out[pl.ds(half, half), cols]
        q_out[pl.ds(0, half), cols] = h[:half] * r_re - h[half:] * r_im
        q_out[pl.ds(half, half), cols] = h[:half] * r_im + h[half:] * r_re
        return 0

    step(0, 0)
    if not first:
        save = pltpu.make_async_copy(r4, r4_out, out_sem)
        save.start()
    lax.fori_loop(1, edges // LANES, step, 0)
    if not first:
        save.wait()


def place_negs(core, nb, nfull, nother):
    nhalf = nfull.shape[1]
    nb[:, pl.ds(pl.multiple_of(core * nhalf, LANES), nhalf)] = nfull[...]
    nb[:, pl.ds(pl.multiple_of((1 - core) * nhalf, LANES), nhalf)] = nother[...]


def exp_kernel(neg_count, edges, core_ref, q, nfull, nother, e_out, top_out, sum_out, nb, nbt, sc):
    negp = nb.shape[1]
    place_negs(core_ref[0], nb, nfull, nother)
    for b in range(negp // LANES):
        nbt[pl.ds(b * LANES, LANES), :] = nb[:, pl.ds(b * LANES, LANES)].astype(F32).T.astype(BF16)

    def step(c, _):
        cols = pl.ds(pl.multiple_of(c * CHUNK, LANES), CHUNK)
        sc[...] = lax.dot_general(nbt[pl.ds(0, neg_count), :], q[:, cols].astype(BF16), (((1,), (0,)), ((), ())), preferred_element_type=F32)
        top = jnp.max(sc[...], axis=0, keepdims=True)
        top_out[:, cols] = top
        total = jnp.zeros((1, CHUNK), F32)
        part = 200
        for i in range(0, neg_count, part):
            size = min(part, neg_count - i)
            e = jnp.exp(sc[pl.ds(i, size), :] - top)
            e_out[pl.ds(i, size), cols] = e
            total = total + jnp.sum(e, axis=0, keepdims=True)
        sum_out[:, cols] = total
        return 0

    lax.fori_loop(0, edges // CHUNK, step, 0)


def score_kernel(dim, neg_count, edges, core_ref, w, q, tb, e, neg_top, neg_sum,
                 loss, dp_out, ds, nk, ns, ng):
    core = core_ref[0]
    negp = ds.shape[0]
    ng[...] = jnp.zeros(ng.shape, F32)
    ds[pl.ds(neg_count, negp - neg_count), :] = jnp.zeros((negp - neg_count, edges), BF16)

    def step(c, loss_row):
        cols = pl.ds(pl.multiple_of(c * CHUNK, LANES), CHUNK)
        pos = jnp.sum(q[:, cols] * tb[:, cols].astype(F32), axis=0, keepdims=True)
        top = jnp.maximum(pos, neg_top[:, cols])
        pos_exp = jnp.exp(pos - top)
        shrink = jnp.exp(neg_top[:, cols] - top)
        norm = pos_exp + shrink * neg_sum[:, cols]
        wt = w[:, cols]
        loss_row = loss_row + wt * (top + jnp.log(norm) - pos)
        dp_out[:, cols] = wt * (pos_exp / norm - 1.0)
        ds[pl.ds(0, neg_count), cols] = (e[:, cols] * (wt * shrink / norm)).astype(BF16)
        ng[...] += lax.dot_general(ds[:, cols], q[:, cols].astype(BF16), (((1,), (1,)), ((), ())), preferred_element_type=F32)
        return loss_row

    loss_row = lax.fori_loop(0, edges // CHUNK, step, jnp.zeros((1, CHUNK), F32))
    loss[...] = jnp.broadcast_to(jnp.sum(loss_row, axis=1, keepdims=True) / edges, loss.shape)

    def save(b, _):
        rows = pl.ds(pl.multiple_of(b * LANES, LANES), LANES)
        put_halves(core, nk, ns, rows, lambda j: ng[rows, pl.ds(j * LANES, min(LANES, dim - j * LANES))].T, dim)
        return 0

    lax.fori_loop(0, negp // LANES, save, 0)


def grad_kernel(dim, edges, core_ref, rel, ds, dp, tb, hb, r, nfull, nother, hg, rk, rs, nb, racc, stage, qs):
    half = dim // 2
    tops = SLICES * LANES
    place_negs(core_ref[0], nb, nfull, nother)
    zero_rows(racc)
    qs[:, pl.ds(dim, tops - dim), :] = jnp.zeros((2, tops - dim, CHUNK), F32)

    def compute(c, slot):
        cols = pl.ds(pl.multiple_of(c * CHUNK, LANES), CHUNK)
        gq = lax.dot_general(nb[...], ds[:, cols], (((1,), (0,)), ((), ())), preferred_element_type=F32) + dp[:, cols] * tb[:, cols].astype(F32)
        g_re, g_im = gq[:half], gq[half:]
        h = hb[:, cols].astype(F32)
        h_re, h_im = h[:half], h[half:]
        r_re, r_im = r[pl.ds(0, half), cols], r[pl.ds(half, half), cols]
        for part, (f_re, f_im) in enumerate(((h_re, h_im), (r_re, r_im))):
            qs[part, pl.ds(0, half), :] = g_re * f_re + g_im * f_im
            qs[part, pl.ds(half, half), :] = g_im * f_re - g_re * f_im
        for b in range(CHUNK // LANES):
            for j in range(SLICES):
                place = pl.ds(j * LANES, LANES), pl.ds(b * LANES, LANES)
                stage[slot, pl.ds(SLICES * b * LANES + j, LANES, stride=SLICES), :] = qs[(0,) + place].T
                hg[pl.ds(SLICES * (c * CHUNK + b * LANES) + j, LANES, stride=SLICES), :] = qs[(1,) + place].T

    def scatter(c, slot):
        add_rows([(racc, rel, c * CHUNK, stage.at[slot], 0)], CHUNK)

    compute(0, 0)

    def step(i, _):
        for slot in range(2):
            c = 2 * i + slot
            scatter(c, slot)
            compute(jnp.minimum(c + 1, edges // CHUNK - 1), 1 - slot)
        return 0

    lax.fori_loop(0, edges // CHUNK // 2, step, 0)

    def save(b, _):
        cols = pl.ds(pl.multiple_of(b * LANES, LANES), LANES)
        put_halves(core_ref[0], rk, rs, cols, lambda j: racc[pl.ds(SLICES * LANES * b + j, LANES, stride=SLICES), :].T, dim)
        return 0

    lax.fori_loop(0, rk.shape[1] // LANES, save, 0)


def unstage(rt, stage):
    for j in range(SLICES):
        stage[pl.ds(j, LANES, stride=SLICES), :] = rt[pl.ds(j * LANES, LANES), :].T


def scatter_kernel(dim, edges, own, *refs):
    if own:
        heads, tails, hg, dp, q, acc, stage, rows, rt = refs
    else:
        heads, tails, rel, hg, dp, hb_hbm, r4_hbm, acc, stage, rows, rt, hb_in, r4, in_sem = refs
        loads = [pltpu.make_async_copy(hb_hbm, hb_in, in_sem.at[0]), pltpu.make_async_copy(r4_hbm, r4, in_sem.at[1])]
        for load in loads:
            load.start()
    half = dim // 2
    blocks = edges // LANES
    zero_rows(acc)
    rt[:, pl.ds(dim, SLICES * LANES - dim), :] = jnp.zeros((2, SLICES * LANES - dim, LANES), F32)

    def compute(b, slot):
        cols = pl.ds(pl.multiple_of(b * LANES, LANES), LANES)
        scale = dp[:, cols]
        if own:
            rt[1, pl.ds(0, dim), :] = q[:, cols] * scale
        else:
            gather_rows(r4, rel, b * LANES, stage, LANES)
            for j in range(SLICES):
                rt[0, pl.ds(j * LANES, LANES), :] = stage_cols(stage, j)
            h = hb_in[:, cols].astype(F32)
            r_re, r_im = rt[0, pl.ds(0, half), :], rt[0, pl.ds(half, half), :]
            rt[1, pl.ds(0, half), :] = scale * (h[:half] * r_re - h[half:] * r_im)
            rt[1, pl.ds(half, half), :] = scale * (h[:half] * r_im + h[half:] * r_re)
        unstage(rt.at[1], rows.at[slot])

    if not own:
        for load in loads:
            load.wait()
    compute(0, 0)

    def step(i, _):
        for slot in range(2):
            b = 2 * i + slot
            add_rows([(acc, tails, b * LANES, rows.at[slot], 0)], LANES)
            add_rows([(acc, heads, b * LANES, hg, b * LANES * SLICES)], LANES)
            compute(jnp.minimum(b + 1, blocks - 1), 1 - slot)
        return 0

    lax.fori_loop(0, blocks // 2, step, 0)


def update_kernel(dim, rows, last, *refs):
    if last:
        core_ref, negs, t4, v, _, nmine, nother, acc, et_out, g_out, stage, rt, rate, outbuf, out_sem = refs
    else:
        core_ref, negs, negs_n, old_t4, v, _, nmine, nother, acc, t4, new_v, nk, ns, stage, rt, rate, nbuf = refs
    core = core_ref[0]
    half = dim // 2
    rt[pl.ds(dim, SLICES * LANES - dim), :] = jnp.zeros((SLICES * LANES - dim, LANES), F32)

    def neg_step(b, _):
        cols = pl.ds(pl.multiple_of(b * LANES, LANES), LANES)
        rt[pl.ds(pl.multiple_of(core * half, 8), half), :] = nmine[:, cols]
        rt[pl.ds(pl.multiple_of((1 - core) * half, 8), half), :] = nother[:, cols]
        unstage(rt, stage)
        add_rows([(acc, negs, b * LANES, stage, 0)], LANES)
        return 0

    lax.fori_loop(0, nmine.shape[1] // LANES, neg_step, 0)

    blocks = rows // LANES

    def slices(b):
        return [pl.ds(SLICES * LANES * b + j, LANES, stride=SLICES) for j in range(SLICES)]

    def advance(b, out):
        where = slices(b)
        square = acc[where[0], :] * acc[where[0], :]
        for j in range(1, SLICES):
            square = square + acc[where[j], :] * acc[where[j], :]
        state = v[pl.ds(b, 1), :] + jnp.sum(square.T, axis=0, keepdims=True) / dim
        out[pl.ds(b, 1), :] = state
        return jnp.broadcast_to(LEARN_RATE / jnp.sqrt(state + ADA_EPS), (LANES, LANES)).T

    if not last:
        def open_pair(p):
            steps = [advance(2 * p + i, new_v) for i in range(2)]
            for i in range(2):
                rate[i] = steps[i]

        def close_pair(p, steps):
            for i in range(2):
                for w in slices(2 * p + i):
                    t4[w, :] = old_t4[w, :] - acc[w, :] * steps[i]

        def ada_step(p, _):
            steps = [rate[0], rate[1]]
            close_pair(p - 1, steps)
            open_pair(p)
            return 0

        open_pair(0)
        lax.fori_loop(1, blocks // 2, ada_step, 0)
        close_pair(blocks // 2 - 1, [rate[0], rate[1]])
        t4[pl.ds(rows * SLICES, 32), :] = jnp.zeros((32, LANES), F32)
        gather_negs(dim, core, t4, negs_n, nk, ns, nbuf, stage)
        return

    width = outbuf.shape[2]
    per = width // LANES
    steps = rows // width

    def save(step, slot):
        return pltpu.make_async_copy(outbuf.at[slot], et_out.at[:, pl.ds(pl.multiple_of(step * width, LANES), width)], out_sem.at[slot])

    def open_group(step, slot):
        for i in range(per):
            rate[slot, i] = advance(step * per + i, g_out)

    open_group(0, 0)

    def exit_step(step, _):
        slot = lax.rem(step, 2)

        @pl.when(step >= 2)
        def _():
            save(step - 2, slot).wait()

        for i in range(per):
            step_size = rate[slot, i]
            for j, w in enumerate(slices(step * per + i)):
                size = min(LANES, dim - j * LANES)
                outbuf[slot, pl.ds(j * LANES, size), pl.ds(i * LANES, LANES)] = (t4[w, :] - acc[w, :] * step_size).T[:size]
        open_group(jnp.minimum(step + 1, steps - 1), 1 - slot)
        save(step, slot).start()
        return 0

    lax.fori_loop(0, steps, exit_step, 0)
    save(steps - 2, (steps - 2) % 2).wait()
    save(steps - 1, (steps - 1) % 2).wait()


def padded_bytes(dims, dtype):
    size = jnp.dtype(dtype).itemsize
    dims = (1,) * (2 - len(dims)) + tuple(dims)
    total = ceil_to(dims[-2], 32 // size) * ceil_to(dims[-1], LANES) * size
    for d in dims[:-2]:
        total *= d
    return total


def cost(micros):
    return pl.CostEstimate(flops=int(micros * 5e6), bytes_accessed=0, transcendentals=0)


def shape(dims, dtype=F32):
    return jax.ShapeDtypeStruct(dims, dtype)


def solution(mesh):
    ent_size = mesh.shape['ent']
    row_spec = P(('sweep', 'ent'), None)
    flat_spec = P(('sweep', 'ent'))
    rel_spec = P('sweep', None)
    state_spec = P('sweep')
    edge_spec = P(('sweep', 'ent'), None, None)
    swap = [(i, i ^ 1) for i in range(ent_size)]
    cross = [(i, i ^ 2) for i in range(ent_size)]

    def shift(amount):
        return [(i, (i + amount) % ent_size) for i in range(ent_size)]

    tie = lax.optimization_barrier

    def chip_sum(keep, send):
        return keep + lax.ppermute(send, 'ent', swap)

    def send(value, pairs):
        return lax.ppermute(value, 'ent', pairs)

    def link(part):
        return send(part, cross)

    def finish(part, got):
        mine = part + got
        return mine, lax.ppermute(mine, 'ent', swap)

    def device_fn(ent_emb, ent_ada, rel_emb, rel_ada, head_idx, tail_idx, rel_idx, edge_mask, neg_idx):
        rows, dim = ent_emb.shape
        num_rel = rel_emb.shape[0]
        _, rounds, edges = head_idx.shape
        neg_count = neg_idx.shape[1]
        negp = ceil_to(neg_count, 2 * LANES)
        relp = ceil_to(num_rel, LANES)
        half = dim // 2
        my_dev = lax.axis_index('ent')
        core = (my_dev % 2).reshape(1)

        heads = [head_idx[0, s] * SLICES for s in range(rounds)]
        own_tails = [tail_idx[0, s] * SLICES for s in range(rounds)]
        own_rels = [rel_idx[0, s] * SLICES for s in range(rounds)]
        tails, rels = [own_tails[0]], [own_rels[0]]
        owned = (neg_idx // rows) == my_dev
        neg_local = jnp.where(owned, neg_idx % rows, rows) * SLICES
        neg_local = jnp.pad(neg_local, ((0, 0), (0, negp - neg_count)), constant_values=rows * SLICES)
        negs = [neg_local[s] for s in range(rounds)]
        weights = edge_mask[0].astype(F32)

        wide_rows = (rows + 8) * SLICES
        stage_shape = pltpu.VMEM((SLICES * LANES, LANES), F32)
        square_shape = pltpu.VMEM((SLICES * LANES, LANES), F32)
        table_out, state_out = shape((wide_rows, LANES)), shape((rows // LANES, LANES))
        cols_bf = shape((dim, edges), BF16)
        neg_half = shape((dim, negp // 2), BF16)

        def call(kernel, args, kinds, outs, out_kinds, scratch, micros, name, aliases=None):
            places = {'s': smem, 'h': hbm, 'v': vmem, 'V': vmem}
            windows = [a for a, k in zip(list(args) + outs, kinds + out_kinds) if k == 'v']
            limit = (4 if name == 'grad' else 3) * 2 ** 20 + sum(padded_bytes(a.shape, a.dtype) for a in windows)
            limit += sum(padded_bytes(a.shape, a.dtype) for a in scratch if getattr(a, 'memory_space', None) == pltpu.VMEM)
            args = [pltpu.with_memory_space_constraint(a, pltpu.VMEM if k == 'V' else pltpu.HBM) if k in 'Vh' else a for a, k in zip(args, kinds)]
            outs = [{'V': pltpu.VMEM, 'h': pltpu.HBM}[k](o.shape, o.dtype) if k in 'Vh' else o for o, k in zip(outs, out_kinds)]
            return pl.pallas_call(
                kernel, out_shape=outs, in_specs=[places[k]() for k in kinds], out_specs=[places[k]() for k in out_kinds],
                scratch_shapes=scratch, compiler_params=pltpu.CompilerParams(vmem_limit_bytes=limit),
                input_output_aliases=aliases or {}, cost_estimate=cost(micros))(*args)

        def gather(lists, t4):
            return call(functools.partial(gather_kernel, dim, len(lists)), lists + [t4], 's' * len(lists) + 'V',
                        [cols_bf] * len(lists), 'V' * len(lists), [stage_shape], 1 + 5 * len(lists), 'gather')

        t4, nk, ns = call(
            functools.partial(entry_kernel, dim, rows), [core, negs[0], ent_emb.T], 'ssh',
            [table_out, neg_half, neg_half], 'VVV',
            [pltpu.VMEM((4, SLICES * LANES, 4 * LANES), F32), stage_shape, pltpu.VMEM((dim, negp), BF16), pltpu.SemaphoreType.DMA((4,))], 20, 'entry')
        v = ent_ada.reshape(rows // LANES, LANES)

        rfm = jnp.pad(rel_emb.T, ((0, 0), (0, relp - num_rel)))
        vr = jnp.pad(rel_ada, (0, relp - num_rel), constant_values=1.0).reshape(1, relp)
        losses = []
        rel_grads = None
        for s in range(rounds):
            first, last = s == 0, s == rounds - 1
            neg_part = chip_sum(nk, ns)
            if first:
                neg_part, t4 = tie((neg_part, t4))
                neg_got = link(neg_part)
                tail_cols, hb = gather([tails[0], heads[0]], t4)
                hb, own_tails, own_rels = tie((hb, own_tails, own_rels))
                for later in range(1, rounds):
                    got = send(jnp.stack([own_tails[later], own_rels[later]]), shift(later))
                    tails.append(got[0])
                    rels.append(got[1])
                neg_got, hb = tie((neg_got, hb))
            else:
                neg_part, t4 = tie((neg_part, t4))
                neg_got = link(neg_part)
                tb, = gather([tails[s]], t4)
                tail_cols = send(tb, shift(-s))
                t4, tb = tie((t4, tb))
                hb, = gather([heads[s]], t4)
                rel_got, hb = tie((rel_got, hb))
                rel_grads = finish(rel_part, rel_got)
            wide = shape((dim, edges))
            outs, out_kinds = [wide, wide], 'VV'
            rel_rows = pltpu.VMEM((relp * SLICES, LANES), F32)
            scratch = [stage_shape, pltpu.VMEM((SLICES * LANES, relp), F32), rel_rows]
            args, kinds = [core, own_rels[s], hb, rfm], 'ssV' + ('v' if first else 'V')
            if not first:
                outs += [shape((relp * SLICES, LANES)), shape((dim, relp)), shape((1, relp))]
                out_kinds += 'hVv'
                scratch += [pltpu.SemaphoreType.DMA]
                args += [vr] + list(rel_grads)
                kinds += 'vVV'
            res = call(functools.partial(query_kernel, dim, edges, first), args, kinds, outs, out_kinds,
                       scratch, 10, 'query')
            q, r = res[:2]
            neg_got, q = tie((neg_got, q))
            nmine, nother = finish(neg_part, neg_got)
            if not first:
                r4, rfm, vr = res[2:]
            e, neg_top, neg_total = call(
                functools.partial(exp_kernel, neg_count, edges), [core, q, nmine, nother], 'sVVV',
                [shape((neg_count, edges)), shape((1, edges)), shape((1, edges))], 'Vvv',
                [pltpu.VMEM((dim, negp), BF16), pltpu.VMEM((negp, dim), BF16), pltpu.VMEM((neg_count, CHUNK), F32)], 8, 'exp')
            if not first:
                e, tail_cols = tie((e, tail_cols))
                tail_cols, hb = tie((tail_cols, hb))
                head_cols = send(hb, shift(s))
            loss, dp, ds, gk, gs = call(
                functools.partial(score_kernel, dim, neg_count, edges), [core, weights[s].reshape(1, edges), q, tail_cols, e, neg_top, neg_total], 'svVVVvv',
                [shape((1, LANES)), shape((1, edges)), shape((negp, edges), BF16), shape((half, negp)), shape((half, negp))], 'vvVVV',
                [pltpu.VMEM((negp, dim), F32)], 8, 'score')
            losses.append(loss[0, 0])
            if not first:
                dp_away = send(dp, shift(s))
            neg_part = chip_sum(gk, gs)
            neg_part, ds = tie((neg_part, ds))
            neg_got = link(neg_part)
            hg, rk, rs = call(
                functools.partial(grad_kernel, dim, edges), [core, own_rels[s], ds, dp, tail_cols, hb, r, nmine, nother], 'ssVvVVVVV',
                [shape((edges * SLICES, LANES)), shape((half, relp)), shape((half, relp))], 'VVV',
                [pltpu.VMEM((dim, negp), BF16), pltpu.VMEM((relp * SLICES, LANES), F32), pltpu.VMEM((2, SLICES * CHUNK, LANES), F32),
                 pltpu.VMEM((2, SLICES * LANES, CHUNK), F32)], 12, 'grad')
            rel_part = chip_sum(rk, rs)
            rel_part, hg = tie((rel_part, hg))
            rel_got = link(rel_part)
            scratch = [stage_shape] + [pltpu.VMEM((2, SLICES * LANES, LANES), F32)] * 2
            if first:
                args, kinds = [heads[s], tails[s], hg, dp, q], 'ssVvV'
            else:
                args, kinds = [heads[s], tails[s], rels[s], hg, dp_away, head_cols, r4], 'sssVvhh'
                scratch += [pltpu.VMEM((dim, edges), BF16), rel_rows, pltpu.SemaphoreType.DMA((2,))]
            acc, = call(functools.partial(scatter_kernel, dim, edges, first), args, kinds, [table_out], 'V', scratch, 15, 'scatter')
            neg_got, acc = tie((neg_got, acc))
            gmine, gother = finish(neg_part, neg_got)
            scratch = [stage_shape, square_shape, pltpu.VMEM((2, 4, LANES, LANES) if last else (2, LANES, LANES), F32)]
            if last:
                args, kinds = [core, negs[s], t4, v, acc], 'ssVVV'
                outs, out_kinds = [table_out, shape((dim, rows)), shape((rows // LANES, LANES))], 'Vhv'
                scratch += [pltpu.VMEM((2, dim, 4 * LANES), F32), pltpu.SemaphoreType.DMA((2,))]
                aliases = {4: 0}
            else:
                args, kinds = [core, negs[s], negs[s + 1], t4, v, acc], 'sssVVV'
                outs, out_kinds = [table_out, table_out, state_out, neg_half, neg_half], 'VVVVV'
                scratch += [pltpu.VMEM((dim, negp), BF16)]
                aliases = {5: 0, 3: 1, 4: 2}
            res = call(functools.partial(update_kernel, dim, rows, last), args + [gmine, gother], kinds + 'VV',
                       outs, out_kinds, scratch, 30, 'update', aliases)
            if last:
                _, et, g = res
            else:
                _, t4, v, nk, ns = res

        even = core[0] == 0
        rel_grads = finish(rel_part, rel_got)
        rg = jnp.where(even, jnp.concatenate(rel_grads, axis=0), jnp.concatenate(rel_grads[::-1], axis=0))
        new_vr = vr + jnp.mean(rg * rg, axis=0, keepdims=True)
        new_r = rfm - LEARN_RATE * rg / jnp.sqrt(new_vr + ADA_EPS)
        return et.T, g.reshape(rows), new_r[:, :num_rel].T, new_vr[0, :num_rel], jnp.stack(losses)[None, :]

    return jax.shard_map(device_fn, mesh=mesh,
                         in_specs=(row_spec, flat_spec, rel_spec, state_spec, edge_spec, edge_spec, edge_spec, edge_spec, rel_spec),
                         out_specs=(row_spec, flat_spec, rel_spec, state_spec, row_spec), check_vma=False)
```

```python
import functools

import jax
import jax.numpy as jnp
from jax import lax
from jax.experimental import pallas as pl
from jax.experimental.pallas import tpu as pltpu
from jax.sharding import PartitionSpec as P


LEARN_RATE = 0.05
ADA_EPS = 1e-10
LANES = 128
SLICES = 4
CHUNK = 256
BATCH = 4
F32 = jnp.float32
BF16 = jnp.bfloat16


def ceil_to(value, unit):
    return -(-value // unit) * unit


def vmem():
    return pl.BlockSpec(memory_space=pltpu.VMEM)


def smem():
    return pl.BlockSpec(memory_space=pltpu.SMEM)


def hbm():
    return pl.BlockSpec(memory_space=pltpu.MemorySpace.HBM)


def four(index):
    return pl.multiple_of(index, SLICES)


def gather_rows(src, ids, base, stage, count):
    for k in range(count):
        stage[pl.ds(SLICES * k, SLICES), :] = src[pl.ds(four(ids[base + k]), SLICES), :]


def stage_cols(stage, slice_no):
    return stage[pl.ds(slice_no, LANES, stride=SLICES), :].T


def batch_sums(acc, ids, base, rows, row_base):
    index = [ids[base + k] for k in range(BATCH)]
    grads = [rows[pl.ds(four(row_base + SLICES * k), SLICES), :] for k in range(BATCH)]
    total = []
    lanes = [jnp.full((SLICES, LANES), i, jnp.int32) for i in index]
    for k in range(BATCH):
        repeats = [jnp.where(lanes[earlier] == lanes[k], grads[earlier], 0.0) for earlier in range(k)]
        total.append(functools.reduce(jnp.add, repeats, grads[k]))
    total = [acc[pl.ds(four(index[k]), SLICES), :] + total[k] for k in range(BATCH)]
    return index, total


def add_rows(chains, count):
    for first in range(0, count, BATCH):
        done = [batch_sums(acc, ids, base + first, rows, row_base + SLICES * first) for acc, ids, base, rows, row_base in chains]
        for (acc, *_), (index, total) in zip(chains, done):
            for k in range(BATCH):
                acc[pl.ds(four(index[k]), SLICES), :] = total[k]


def put_halves(core, keep, sent, cols, block_of, dim):
    half = dim // 2
    for side in range(2):
        @pl.when(core == side)
        def _():
            for j in range(SLICES):
                block = block_of(j)
                for h in range(2):
                    lo, hi = max(j * LANES, h * half), min((j + 1) * LANES, (h + 1) * half)
                    if lo < hi:
                        (keep if h == side else sent)[pl.ds(lo - h * half, hi - lo), cols] = block[lo - j * LANES:hi - j * LANES]


def zero_rows(ref, step=1024):
    rows = ref.shape[0]
    whole = rows // step

    def body(i, _):
        ref[pl.ds(pl.multiple_of(i * step, 8), step), :] = jnp.zeros((step, LANES), ref.dtype)
        return 0

    lax.fori_loop(0, whole, body, 0)
    if rows % step:
        ref[pl.ds(whole * step, rows % step), :] = jnp.zeros((rows % step, LANES), ref.dtype)


def gather_out(dim, table, ids, out, stage, count):
    def body(b, _):
        gather_rows(table, ids, b * LANES, stage, LANES)
        cols = pl.ds(pl.multiple_of(b * LANES, LANES), LANES)
        for j in range(SLICES):
            size = min(LANES, dim - j * LANES)
            out[pl.ds(j * LANES, size), cols] = stage_cols(stage, j)[:size].astype(BF16)
        return 0

    lax.fori_loop(0, count // LANES, body, 0)


def gather_negs(dim, core, table, negs, nk, ns, nbuf, stage):
    half = nbuf.shape[1] // 2
    gather_out(dim, table, negs, nbuf, stage, nbuf.shape[1])
    nk[...] = nbuf[:, pl.ds(pl.multiple_of(core * half, LANES), half)]
    ns[...] = nbuf[:, pl.ds(pl.multiple_of((1 - core) * half, LANES), half)]


def entry_kernel(dim, rows, core_ref, negs, et, t4, nk, ns, inbuf, stage, nbuf, in_sem):
    cols = inbuf.shape[2]
    steps = rows // cols
    per = cols // LANES

    def fetch(step, slot):
        return pltpu.make_async_copy(et.at[:, pl.ds(pl.multiple_of(step * cols, LANES), cols)],
                                     inbuf.at[slot, pl.ds(0, dim)], in_sem.at[slot])

    slots = inbuf.shape[0]
    for slot in range(slots - 1):
        fetch(slot, slot).start()
    for slot in range(slots):
        inbuf[slot, pl.ds(dim, SLICES * LANES - dim), :] = jnp.zeros((SLICES * LANES - dim, cols), F32)
    t4[pl.ds(rows * SLICES, 32), :] = jnp.zeros((32, LANES), F32)

    def body(step, _):
        slot = lax.rem(step, slots)

        @pl.when(step + slots - 1 < steps)
        def _():
            fetch(step + slots - 1, lax.rem(step + slots - 1, slots)).start()

        fetch(step, slot).wait()
        for b in range(per):
            row0 = (step * per + b) * LANES
            for j in range(SLICES):
                t4[pl.ds(SLICES * row0 + j, LANES, stride=SLICES), :] = inbuf[slot, pl.ds(j * LANES, LANES), pl.ds(b * LANES, LANES)].T
        return 0

    lax.fori_loop(0, steps, body, 0)
    gather_negs(dim, core_ref[0], t4, negs, nk, ns, nbuf, stage)


def gather_kernel(dim, lists, *refs):
    ids, t4, outs, stage = refs[:lists], refs[lists], refs[lists + 1:2 * lists + 1], refs[2 * lists + 1]
    for i in range(lists):
        gather_out(dim, t4, ids[i], outs[i], stage, outs[i].shape[1])


def query_kernel(dim, edges, first, *refs):
    if first:
        core_ref, rel, hb, rfm, q_out, r_out, stage, fm, r4 = refs
    else:
        core_ref, rel, hb, rfm_in, vr_in, rmine, rother, q_out, r_out, r4_out, rfm, vr, stage, fm, r4, out_sem = refs
        core = core_ref[0]
    half = dim // 2
    relp = rfm.shape[1]
    tops = SLICES * LANES
    if not first:
        fm[pl.ds(pl.multiple_of(core * half, 8), half), :] = rmine[...]
        fm[pl.ds(pl.multiple_of((1 - core) * half, 8), half), :] = rother[...]
        grad = fm[pl.ds(0, dim), :]
        vr[...] = vr_in[...] + jnp.sum(grad * grad, axis=0, keepdims=True) / dim
        rate = LEARN_RATE / jnp.sqrt(vr[...] + ADA_EPS)
        rfm[...] = rfm_in[...] - fm[pl.ds(0, dim), :] * rate
    fm[pl.ds(dim, tops - dim), pl.ds(0, LANES)] = jnp.zeros((tops - dim, LANES), F32)
    for b in range(relp // LANES):
        for j in range(SLICES):
            if (j + 1) * LANES <= dim:
                block = rfm[pl.ds(j * LANES, LANES), pl.ds(b * LANES, LANES)]
            else:
                fm[pl.ds(j * LANES, dim - j * LANES), pl.ds(0, LANES)] = rfm[pl.ds(j * LANES, dim - j * LANES), pl.ds(b * LANES, LANES)]
                block = fm[pl.ds(j * LANES, LANES), pl.ds(0, LANES)]
            r4[pl.ds(SLICES * b * LANES + j, LANES, stride=SLICES), :] = block.T

    def step(b, _):
        cols = pl.ds(pl.multiple_of(b * LANES, LANES), LANES)
        gather_rows(r4, rel, b * LANES, stage, LANES)
        for j in range(SLICES):
            size = min(LANES, dim - j * LANES)
            r_out[pl.ds(j * LANES, size), cols] = stage_cols(stage, j)[:size]
        h = hb[:, cols].astype(F32)
        r_re, r_im = r_out[pl.ds(0, half), cols], r_out[pl.ds(half, half), cols]
        q_out[pl.ds(0, half), cols] = h[:half] * r_re - h[half:] * r_im
        q_out[pl.ds(half, half), cols] = h[:half] * r_im + h[half:] * r_re
        return 0

    step(0, 0)
    if not first:
        save = pltpu.make_async_copy(r4, r4_out, out_sem)
        save.start()
    lax.fori_loop(1, edges // LANES, step, 0)
    if not first:
        save.wait()


def place_negs(core, nb, nfull, nother):
    nhalf = nfull.shape[1]
    nb[:, pl.ds(pl.multiple_of(core * nhalf, LANES), nhalf)] = nfull[...]
    nb[:, pl.ds(pl.multiple_of((1 - core) * nhalf, LANES), nhalf)] = nother[...]


def exp_kernel(neg_count, edges, core_ref, q, nfull, nother, e_out, top_out, sum_out, nb, nbt, sc):
    negp = nb.shape[1]
    place_negs(core_ref[0], nb, nfull, nother)
    for b in range(negp // LANES):
        nbt[pl.ds(b * LANES, LANES), :] = nb[:, pl.ds(b * LANES, LANES)].astype(F32).T.astype(BF16)

    def step(c, _):
        cols = pl.ds(pl.multiple_of(c * CHUNK, LANES), CHUNK)
        sc[...] = lax.dot_general(nbt[pl.ds(0, neg_count), :], q[:, cols].astype(BF16), (((1,), (0,)), ((), ())), preferred_element_type=F32)
        top = jnp.max(sc[...], axis=0, keepdims=True)
        top_out[:, cols] = top
        total = jnp.zeros((1, CHUNK), F32)
        part = 200
        for i in range(0, neg_count, part):
            size = min(part, neg_count - i)
            e = jnp.exp(sc[pl.ds(i, size), :] - top)
            e_out[pl.ds(i, size), cols] = e
            total = total + jnp.sum(e, axis=0, keepdims=True)
        sum_out[:, cols] = total
        return 0

    lax.fori_loop(0, edges // CHUNK, step, 0)


def score_kernel(dim, neg_count, edges, core_ref, w, q, tb, e, neg_top, neg_sum,
                 loss, dp_out, ds, nk, ns, ng):
    core = core_ref[0]
    negp = ds.shape[0]
    ng[...] = jnp.zeros(ng.shape, F32)
    ds[pl.ds(neg_count, negp - neg_count), :] = jnp.zeros((negp - neg_count, edges), BF16)

    def step(c, loss_row):
        cols = pl.ds(pl.multiple_of(c * CHUNK, LANES), CHUNK)
        pos = jnp.sum(q[:, cols] * tb[:, cols].astype(F32), axis=0, keepdims=True)
        top = jnp.maximum(pos, neg_top[:, cols])
        pos_exp = jnp.exp(pos - top)
        shrink = jnp.exp(neg_top[:, cols] - top)
        norm = pos_exp + shrink * neg_sum[:, cols]
        wt = w[:, cols]
        loss_row = loss_row + wt * (top + jnp.log(norm) - pos)
        dp_out[:, cols] = wt * (pos_exp / norm - 1.0)
        ds[pl.ds(0, neg_count), cols] = (e[:, cols] * (wt * shrink / norm)).astype(BF16)
        ng[...] += lax.dot_general(ds[:, cols], q[:, cols].astype(BF16), (((1,), (1,)), ((), ())), preferred_element_type=F32)
        return loss_row

    loss_row = lax.fori_loop(0, edges // CHUNK, step, jnp.zeros((1, CHUNK), F32))
    loss[...] = jnp.broadcast_to(jnp.sum(loss_row, axis=1, keepdims=True) / edges, loss.shape)

    def save(b, _):
        rows = pl.ds(pl.multiple_of(b * LANES, LANES), LANES)
        put_halves(core, nk, ns, rows, lambda j: ng[rows, pl.ds(j * LANES, min(LANES, dim - j * LANES))].T, dim)
        return 0

    lax.fori_loop(0, negp // LANES, save, 0)


def grad_kernel(dim, edges, core_ref, rel, ds, dp, tb, hb, r, nfull, nother, hg, rk, rs, nb, racc, stage, qs):
    half = dim // 2
    tops = SLICES * LANES
    place_negs(core_ref[0], nb, nfull, nother)
    zero_rows(racc)
    qs[:, pl.ds(dim, tops - dim), :] = jnp.zeros((2, tops - dim, CHUNK), F32)

    def compute(c):
        cols = pl.ds(pl.multiple_of(c * CHUNK, LANES), CHUNK)
        gq = lax.dot_general(nb[...], ds[:, cols], (((1,), (0,)), ((), ())), preferred_element_type=F32) + dp[:, cols] * tb[:, cols].astype(F32)
        g_re, g_im = gq[:half], gq[half:]
        h = hb[:, cols].astype(F32)
        h_re, h_im = h[:half], h[half:]
        r_re, r_im = r[pl.ds(0, half), cols], r[pl.ds(half, half), cols]
        for part, (f_re, f_im) in enumerate(((h_re, h_im), (r_re, r_im))):
            qs[part, pl.ds(0, half), :] = g_re * f_re + g_im * f_im
            qs[part, pl.ds(half, half), :] = g_im * f_re - g_re * f_im

    def turn(c, slot, b, j):
        place = pl.ds(j * LANES, LANES), pl.ds(b * LANES, LANES)
        stage[slot, pl.ds(SLICES * b * LANES + j, LANES, stride=SLICES), :] = qs[(0,) + place].T
        hg[pl.ds(SLICES * (c * CHUNK + b * LANES) + j, LANES, stride=SLICES), :] = qs[(1,) + place].T

    blocks = [(b, j) for b in range(CHUNK // LANES) for j in range(SLICES)]
    share = CHUNK // len(blocks)
    compute(0)
    for b, j in blocks:
        turn(0, 0, b, j)

    def step(i, _):
        for slot in range(2):
            c = 2 * i + slot
            after = jnp.minimum(c + 1, edges // CHUNK - 1)
            compute(after)
            for k, (b, j) in enumerate(blocks):
                add_rows([(racc, rel, c * CHUNK + k * share, stage.at[slot], k * share * SLICES)], share)
                turn(after, 1 - slot, b, j)
        return 0

    lax.fori_loop(0, edges // CHUNK // 2, step, 0)

    def save(b, _):
        cols = pl.ds(pl.multiple_of(b * LANES, LANES), LANES)
        put_halves(core_ref[0], rk, rs, cols, lambda j: racc[pl.ds(SLICES * LANES * b + j, LANES, stride=SLICES), :].T, dim)
        return 0

    lax.fori_loop(0, rk.shape[1] // LANES, save, 0)


def unstage(rt, stage):
    for j in range(SLICES):
        stage[pl.ds(j, LANES, stride=SLICES), :] = rt[pl.ds(j * LANES, LANES), :].T


def scatter_kernel(dim, edges, own, *refs):
    if own:
        heads, tails, hg, dp, q, acc, stage, rows, rt = refs
    else:
        heads, tails, rel, hg, dp, hb_hbm, r4_hbm, acc, stage, rows, rt, hb_in, r4, in_sem = refs
        loads = [pltpu.make_async_copy(hb_hbm, hb_in, in_sem.at[0]), pltpu.make_async_copy(r4_hbm, r4, in_sem.at[1])]
        for load in loads:
            load.start()
    half = dim // 2
    blocks = edges // LANES
    zero_rows(acc)
    rt[:, pl.ds(dim, SLICES * LANES - dim), :] = jnp.zeros((2, SLICES * LANES - dim, LANES), F32)

    def compute(b, slot):
        cols = pl.ds(pl.multiple_of(b * LANES, LANES), LANES)
        scale = dp[:, cols]
        if own:
            rt[1, pl.ds(0, dim), :] = q[:, cols] * scale
        else:
            gather_rows(r4, rel, b * LANES, stage, LANES)
            for j in range(SLICES):
                rt[0, pl.ds(j * LANES, LANES), :] = stage_cols(stage, j)
            h = hb_in[:, cols].astype(F32)
            r_re, r_im = rt[0, pl.ds(0, half), :], rt[0, pl.ds(half, half), :]
            rt[1, pl.ds(0, half), :] = scale * (h[:half] * r_re - h[half:] * r_im)
            rt[1, pl.ds(half, half), :] = scale * (h[:half] * r_im + h[half:] * r_re)
        unstage(rt.at[1], rows.at[slot])

    if not own:
        for load in loads:
            load.wait()
    compute(0, 0)

    def step(i, _):
        for slot in range(2):
            b = 2 * i + slot
            add_rows([(acc, tails, b * LANES, rows.at[slot], 0)], LANES)
            add_rows([(acc, heads, b * LANES, hg, b * LANES * SLICES)], LANES)
            compute(jnp.minimum(b + 1, blocks - 1), 1 - slot)
        return 0

    lax.fori_loop(0, blocks // 2, step, 0)


def update_kernel(dim, rows, last, *refs):
    if last:
        core_ref, negs, t4, v, _, nmine, nother, acc, et_out, g_out, stage, rt, rate, outbuf, out_sem = refs
    else:
        core_ref, negs, negs_n, old_t4, v, _, nmine, nother, acc, t4, new_v, nk, ns, stage, rt, rate, nbuf = refs
    core = core_ref[0]
    half = dim // 2
    rt[pl.ds(dim, SLICES * LANES - dim), :] = jnp.zeros((SLICES * LANES - dim, LANES), F32)

    def neg_step(b, _):
        cols = pl.ds(pl.multiple_of(b * LANES, LANES), LANES)
        rt[pl.ds(pl.multiple_of(core * half, 8), half), :] = nmine[:, cols]
        rt[pl.ds(pl.multiple_of((1 - core) * half, 8), half), :] = nother[:, cols]
        unstage(rt, stage)
        add_rows([(acc, negs, b * LANES, stage, 0)], LANES)
        return 0

    lax.fori_loop(0, nmine.shape[1] // LANES, neg_step, 0)

    blocks = rows // LANES

    def slices(b):
        return [pl.ds(SLICES * LANES * b + j, LANES, stride=SLICES) for j in range(SLICES)]

    def advance(b, out):
        where = slices(b)
        square = acc[where[0], :] * acc[where[0], :]
        for j in range(1, SLICES):
            square = square + acc[where[j], :] * acc[where[j], :]
        state = v[pl.ds(b, 1), :] + jnp.sum(square.T, axis=0, keepdims=True) / dim
        out[pl.ds(b, 1), :] = state
        return jnp.broadcast_to(LEARN_RATE / jnp.sqrt(state + ADA_EPS), (LANES, LANES)).T

    if not last:
        def open_pair(p):
            steps = [advance(2 * p + i, new_v) for i in range(2)]
            for i in range(2):
                rate[i] = steps[i]

        def close_pair(p, steps):
            for i in range(2):
                for w in slices(2 * p + i):
                    t4[w, :] = old_t4[w, :] - acc[w, :] * steps[i]

        def ada_step(p, _):
            steps = [rate[0], rate[1]]
            close_pair(p - 1, steps)
            open_pair(p)
            return 0

        open_pair(0)
        lax.fori_loop(1, blocks // 2, ada_step, 0)
        close_pair(blocks // 2 - 1, [rate[0], rate[1]])
        t4[pl.ds(rows * SLICES, 32), :] = jnp.zeros((32, LANES), F32)
        gather_negs(dim, core, t4, negs_n, nk, ns, nbuf, stage)
        return

    width = outbuf.shape[2]
    per = width // LANES
    steps = rows // width

    def save(step, slot):
        return pltpu.make_async_copy(outbuf.at[slot], et_out.at[:, pl.ds(pl.multiple_of(step * width, LANES), width)], out_sem.at[slot])

    def open_group(step, slot):
        for i in range(per):
            rate[slot, i] = advance(step * per + i, g_out)

    open_group(0, 0)

    def exit_step(step, _):
        slot = lax.rem(step, 2)

        @pl.when(step >= 2)
        def _():
            save(step - 2, slot).wait()

        for i in range(per):
            step_size = rate[slot, i]
            for j, w in enumerate(slices(step * per + i)):
                size = min(LANES, dim - j * LANES)
                outbuf[slot, pl.ds(j * LANES, size), pl.ds(i * LANES, LANES)] = (t4[w, :] - acc[w, :] * step_size).T[:size]
        open_group(jnp.minimum(step + 1, steps - 1), 1 - slot)
        save(step, slot).start()
        return 0

    lax.fori_loop(0, steps, exit_step, 0)
    save(steps - 2, (steps - 2) % 2).wait()
    save(steps - 1, (steps - 1) % 2).wait()


def padded_bytes(dims, dtype):
    size = jnp.dtype(dtype).itemsize
    dims = (1,) * (2 - len(dims)) + tuple(dims)
    total = ceil_to(dims[-2], 32 // size) * ceil_to(dims[-1], LANES) * size
    for d in dims[:-2]:
        total *= d
    return total


def cost(micros):
    return pl.CostEstimate(flops=int(micros * 5e6), bytes_accessed=0, transcendentals=0)


def shape(dims, dtype=F32):
    return jax.ShapeDtypeStruct(dims, dtype)


def solution(mesh):
    ent_size = mesh.shape['ent']
    row_spec = P(('sweep', 'ent'), None)
    flat_spec = P(('sweep', 'ent'))
    rel_spec = P('sweep', None)
    state_spec = P('sweep')
    edge_spec = P(('sweep', 'ent'), None, None)
    swap = [(i, i ^ 1) for i in range(ent_size)]
    cross = [(i, i ^ 2) for i in range(ent_size)]

    def shift(amount):
        return [(i, (i + amount) % ent_size) for i in range(ent_size)]

    tie = lax.optimization_barrier

    def chip_sum(keep, send):
        return keep + lax.ppermute(send, 'ent', swap)

    def send(value, pairs):
        return lax.ppermute(value, 'ent', pairs)

    def link(part):
        return send(part, cross)

    def finish(part, got):
        mine = part + got
        return mine, lax.ppermute(mine, 'ent', swap)

    def device_fn(ent_emb, ent_ada, rel_emb, rel_ada, head_idx, tail_idx, rel_idx, edge_mask, neg_idx):
        rows, dim = ent_emb.shape
        num_rel = rel_emb.shape[0]
        _, rounds, edges = head_idx.shape
        neg_count = neg_idx.shape[1]
        negp = ceil_to(neg_count, 2 * LANES)
        relp = ceil_to(num_rel, LANES)
        half = dim // 2
        my_dev = lax.axis_index('ent')
        core = (my_dev % 2).reshape(1)

        heads = [head_idx[0, s] * SLICES for s in range(rounds)]
        own_tails = [tail_idx[0, s] * SLICES for s in range(rounds)]
        own_rels = [rel_idx[0, s] * SLICES for s in range(rounds)]
        tails, rels = [own_tails[0]], [own_rels[0]]
        owned = (neg_idx // rows) == my_dev
        neg_local = jnp.where(owned, neg_idx % rows, rows) * SLICES
        neg_local = jnp.pad(neg_local, ((0, 0), (0, negp - neg_count)), constant_values=rows * SLICES)
        negs = [neg_local[s] for s in range(rounds)]
        weights = edge_mask[0].astype(F32)

        wide_rows = (rows + 8) * SLICES
        stage_shape = pltpu.VMEM((SLICES * LANES, LANES), F32)
        square_shape = pltpu.VMEM((SLICES * LANES, LANES), F32)
        table_out, state_out = shape((wide_rows, LANES)), shape((rows // LANES, LANES))
        cols_bf = shape((dim, edges), BF16)
        neg_half = shape((dim, negp // 2), BF16)

        def call(kernel, args, kinds, outs, out_kinds, scratch, micros, name, aliases=None):
            places = {'s': smem, 'h': hbm, 'v': vmem, 'V': vmem}
            windows = [a for a, k in zip(list(args) + outs, kinds + out_kinds) if k == 'v']
            limit = (4 if name == 'grad' else 2) * 2 ** 20 + sum(padded_bytes(a.shape, a.dtype) for a in windows)
            limit += sum(padded_bytes(a.shape, a.dtype) for a in scratch if getattr(a, 'memory_space', None) == pltpu.VMEM)
            args = [pltpu.with_memory_space_constraint(a, pltpu.VMEM if k == 'V' else pltpu.HBM) if k in 'Vh' else a for a, k in zip(args, kinds)]
            outs = [{'V': pltpu.VMEM, 'h': pltpu.HBM}[k](o.shape, o.dtype) if k in 'Vh' else o for o, k in zip(outs, out_kinds)]
            return pl.pallas_call(
                kernel, out_shape=outs, in_specs=[places[k]() for k in kinds], out_specs=[places[k]() for k in out_kinds],
                scratch_shapes=scratch, compiler_params=pltpu.CompilerParams(vmem_limit_bytes=limit),
                input_output_aliases=aliases or {}, cost_estimate=cost(micros))(*args)

        def gather(lists, t4):
            return call(functools.partial(gather_kernel, dim, len(lists)), lists + [t4], 's' * len(lists) + 'V',
                        [cols_bf] * len(lists), 'V' * len(lists), [stage_shape], 1 + 5 * len(lists), 'gather')

        t4, nk, ns = call(
            functools.partial(entry_kernel, dim, rows), [core, negs[0], ent_emb.T], 'ssh',
            [table_out, neg_half, neg_half], 'VVV',
            [pltpu.VMEM((4, SLICES * LANES, 4 * LANES), F32), stage_shape, pltpu.VMEM((dim, negp), BF16), pltpu.SemaphoreType.DMA((4,))], 20, 'entry')
        v = ent_ada.reshape(rows // LANES, LANES)

        rfm = jnp.pad(rel_emb.T, ((0, 0), (0, relp - num_rel)))
        vr = jnp.pad(rel_ada, (0, relp - num_rel), constant_values=1.0).reshape(1, relp)
        losses = []
        rel_grads = None
        for s in range(rounds):
            first, last = s == 0, s == rounds - 1
            neg_part = chip_sum(nk, ns)
            if first:
                neg_part, t4 = tie((neg_part, t4))
                neg_got = link(neg_part)
                tail_cols, hb = gather([tails[0], heads[0]], t4)
                hb, own_tails, own_rels = tie((hb, own_tails, own_rels))
                for later in range(1, rounds):
                    got = send(jnp.stack([own_tails[later], own_rels[later]]), shift(later))
                    tails.append(got[0])
                    rels.append(got[1])
                neg_got, hb = tie((neg_got, hb))
            else:
                neg_part, t4 = tie((neg_part, t4))
                neg_got = link(neg_part)
                tb, = gather([tails[s]], t4)
                tail_cols = send(tb, shift(-s))
                t4, tb = tie((t4, tb))
                hb, = gather([heads[s]], t4)
                rel_got, hb = tie((rel_got, hb))
                rel_grads = finish(rel_part, rel_got)
            wide = shape((dim, edges))
            outs, out_kinds = [wide, wide], 'VV'
            rel_rows = pltpu.VMEM((relp * SLICES, LANES), F32)
            scratch = [stage_shape, pltpu.VMEM((SLICES * LANES, relp), F32), rel_rows]
            args, kinds = [core, own_rels[s], hb, rfm], 'ssV' + ('v' if first else 'V')
            if not first:
                outs += [shape((relp * SLICES, LANES)), shape((dim, relp)), shape((1, relp))]
                out_kinds += 'hVv'
                scratch += [pltpu.SemaphoreType.DMA]
                args += [vr] + list(rel_grads)
                kinds += 'vVV'
            res = call(functools.partial(query_kernel, dim, edges, first), args, kinds, outs, out_kinds,
                       scratch, 10, 'query')
            q, r = res[:2]
            neg_got, q = tie((neg_got, q))
            nmine, nother = finish(neg_part, neg_got)
            if not first:
                r4, rfm, vr = res[2:]
            e, neg_top, neg_total = call(
                functools.partial(exp_kernel, neg_count, edges), [core, q, nmine, nother], 'sVVV',
                [shape((neg_count, edges)), shape((1, edges)), shape((1, edges))], 'Vvv',
                [pltpu.VMEM((dim, negp), BF16), pltpu.VMEM((negp, dim), BF16), pltpu.VMEM((neg_count, CHUNK), F32)], 8, 'exp')
            if not first:
                e, tail_cols = tie((e, tail_cols))
                tail_cols, hb = tie((tail_cols, hb))
                head_cols = send(hb, shift(s))
            loss, dp, ds, gk, gs = call(
                functools.partial(score_kernel, dim, neg_count, edges), [core, weights[s].reshape(1, edges), q, tail_cols, e, neg_top, neg_total], 'svVVVvv',
                [shape((1, LANES)), shape((1, edges)), shape((negp, edges), BF16), shape((half, negp)), shape((half, negp))], 'vvVVV',
                [pltpu.VMEM((negp, dim), F32)], 8, 'score')
            losses.append(loss[0, 0])
            if not first:
                dp_away = send(dp, shift(s))
            neg_part = chip_sum(gk, gs)
            neg_part, ds = tie((neg_part, ds))
            neg_got = link(neg_part)
            hg, rk, rs = call(
                functools.partial(grad_kernel, dim, edges), [core, own_rels[s], ds, dp, tail_cols, hb, r, nmine, nother], 'ssVvVVVVV',
                [shape((edges * SLICES, LANES)), shape((half, relp)), shape((half, relp))], 'VVV',
                [pltpu.VMEM((dim, negp), BF16), pltpu.VMEM((relp * SLICES, LANES), F32), pltpu.VMEM((2, SLICES * CHUNK, LANES), F32),
                 pltpu.VMEM((2, SLICES * LANES, CHUNK), F32)], 12, 'grad')
            rel_part = chip_sum(rk, rs)
            rel_part, hg = tie((rel_part, hg))
            rel_got = link(rel_part)
            scratch = [stage_shape] + [pltpu.VMEM((2, SLICES * LANES, LANES), F32)] * 2
            if first:
                args, kinds = [heads[s], tails[s], hg, dp, q], 'ssVvV'
            else:
                args, kinds = [heads[s], tails[s], rels[s], hg, dp_away, head_cols, r4], 'sssVvhh'
                scratch += [pltpu.VMEM((dim, edges), BF16), rel_rows, pltpu.SemaphoreType.DMA((2,))]
            acc, = call(functools.partial(scatter_kernel, dim, edges, first), args, kinds, [table_out], 'V', scratch, 15, 'scatter')
            neg_got, acc = tie((neg_got, acc))
            gmine, gother = finish(neg_part, neg_got)
            scratch = [stage_shape, square_shape, pltpu.VMEM((2, 4, LANES, LANES) if last else (2, LANES, LANES), F32)]
            if last:
                args, kinds = [core, negs[s], t4, v, acc], 'ssVVV'
                outs, out_kinds = [table_out, shape((dim, rows)), shape((rows // LANES, LANES))], 'Vhv'
                scratch += [pltpu.VMEM((2, dim, 4 * LANES), F32), pltpu.SemaphoreType.DMA((2,))]
                aliases = {4: 0}
            else:
                args, kinds = [core, negs[s], negs[s + 1], t4, v, acc], 'sssVVV'
                outs, out_kinds = [table_out, table_out, state_out, neg_half, neg_half], 'VVVVV'
                scratch += [pltpu.VMEM((dim, negp), BF16)]
                aliases = {5: 0, 3: 1, 4: 2}
            res = call(functools.partial(update_kernel, dim, rows, last), args + [gmine, gother], kinds + 'VV',
                       outs, out_kinds, scratch, 30, 'update', aliases)
            if last:
                _, et, g = res
            else:
                _, t4, v, nk, ns = res

        even = core[0] == 0
        rel_grads = finish(rel_part, rel_got)
        rg = jnp.where(even, jnp.concatenate(rel_grads, axis=0), jnp.concatenate(rel_grads[::-1], axis=0))
        new_vr = vr + jnp.mean(rg * rg, axis=0, keepdims=True)
        new_r = rfm - LEARN_RATE * rg / jnp.sqrt(new_vr + ADA_EPS)
        return et.T, g.reshape(rows), new_r[:, :num_rel].T, new_vr[0, :num_rel], jnp.stack(losses)[None, :]

    return jax.shard_map(device_fn, mesh=mesh,
                         in_specs=(row_spec, flat_spec, rel_spec, state_spec, edge_spec, edge_spec, edge_spec, edge_spec, rel_spec),
                         out_specs=(row_spec, flat_spec, rel_spec, state_spec, row_spec), check_vma=False)
```

```python
import functools

import jax
import jax.numpy as jnp
from jax import lax
from jax.experimental import pallas as pl
from jax.experimental.pallas import tpu as pltpu
from jax.sharding import PartitionSpec as P


LEARN_RATE = 0.05
ADA_EPS = 1e-10
LANES = 128
SLICES = 4
CHUNK = 256
BATCH = 4
F32 = jnp.float32
BF16 = jnp.bfloat16


def ceil_to(value, unit):
    return -(-value // unit) * unit


def vmem():
    return pl.BlockSpec(memory_space=pltpu.VMEM)


def smem():
    return pl.BlockSpec(memory_space=pltpu.SMEM)


def hbm():
    return pl.BlockSpec(memory_space=pltpu.MemorySpace.HBM)


def four(index):
    return pl.multiple_of(index, SLICES)


def gather_rows(src, ids, base, stage, count):
    for k in range(count):
        stage[pl.ds(SLICES * k, SLICES), :] = src[pl.ds(four(ids[base + k]), SLICES), :]


def stage_cols(stage, slice_no):
    return stage[pl.ds(slice_no, LANES, stride=SLICES), :].T


def batch_sums(acc, ids, base, rows, row_base):
    index = [ids[base + k] for k in range(BATCH)]
    grads = [rows[pl.ds(four(row_base + SLICES * k), SLICES), :] for k in range(BATCH)]
    total = []
    lanes = [jnp.full((SLICES, LANES), i, jnp.int32) for i in index]
    for k in range(BATCH):
        repeats = [jnp.where(lanes[earlier] == lanes[k], grads[earlier], 0.0) for earlier in range(k)]
        total.append(functools.reduce(jnp.add, repeats, grads[k]))
    total = [acc[pl.ds(four(index[k]), SLICES), :] + total[k] for k in range(BATCH)]
    return index, total


def add_rows(chains, count):
    for first in range(0, count, BATCH):
        done = [batch_sums(acc, ids, base + first, rows, row_base + SLICES * first) for acc, ids, base, rows, row_base in chains]
        for (acc, *_), (index, total) in zip(chains, done):
            for k in range(BATCH):
                acc[pl.ds(four(index[k]), SLICES), :] = total[k]


def put_halves(core, keep, sent, cols, block_of, dim):
    half = dim // 2
    for side in range(2):
        @pl.when(core == side)
        def _():
            for j in range(SLICES):
                block = block_of(j)
                for h in range(2):
                    lo, hi = max(j * LANES, h * half), min((j + 1) * LANES, (h + 1) * half)
                    if lo < hi:
                        (keep if h == side else sent)[pl.ds(lo - h * half, hi - lo), cols] = block[lo - j * LANES:hi - j * LANES]


def zero_rows(ref, step=1024):
    rows = ref.shape[0]
    whole = rows // step

    def body(i, _):
        ref[pl.ds(pl.multiple_of(i * step, 8), step), :] = jnp.zeros((step, LANES), ref.dtype)
        return 0

    lax.fori_loop(0, whole, body, 0)
    if rows % step:
        ref[pl.ds(whole * step, rows % step), :] = jnp.zeros((rows % step, LANES), ref.dtype)


def gather_out(dim, table, ids, out, stage, count):
    def body(b, _):
        gather_rows(table, ids, b * LANES, stage, LANES)
        cols = pl.ds(pl.multiple_of(b * LANES, LANES), LANES)
        for j in range(SLICES):
            size = min(LANES, dim - j * LANES)
            out[pl.ds(j * LANES, size), cols] = stage_cols(stage, j)[:size].astype(BF16)
        return 0

    lax.fori_loop(0, count // LANES, body, 0)


def gather_negs(dim, core, table, negs, nk, ns, nbuf, stage):
    half = nbuf.shape[1] // 2
    gather_out(dim, table, negs, nbuf, stage, nbuf.shape[1])
    nk[...] = nbuf[:, pl.ds(pl.multiple_of(core * half, LANES), half)]
    ns[...] = nbuf[:, pl.ds(pl.multiple_of((1 - core) * half, LANES), half)]


def entry_kernel(dim, rows, core_ref, negs, et, t4, nk, ns, inbuf, stage, nbuf, in_sem):
    cols = inbuf.shape[2]
    steps = rows // cols
    per = cols // LANES

    def fetch(step, slot):
        return pltpu.make_async_copy(et.at[:, pl.ds(pl.multiple_of(step * cols, LANES), cols)],
                                     inbuf.at[slot, pl.ds(0, dim)], in_sem.at[slot])

    slots = inbuf.shape[0]
    for slot in range(slots - 1):
        fetch(slot, slot).start()
    for slot in range(slots):
        inbuf[slot, pl.ds(dim, SLICES * LANES - dim), :] = jnp.zeros((SLICES * LANES - dim, cols), F32)
    t4[pl.ds(rows * SLICES, 32), :] = jnp.zeros((32, LANES), F32)

    def body(step, _):
        slot = lax.rem(step, slots)

        @pl.when(step + slots - 1 < steps)
        def _():
            fetch(step + slots - 1, lax.rem(step + slots - 1, slots)).start()

        fetch(step, slot).wait()
        for b in range(per):
            row0 = (step * per + b) * LANES
            for j in range(SLICES):
                t4[pl.ds(SLICES * row0 + j, LANES, stride=SLICES), :] = inbuf[slot, pl.ds(j * LANES, LANES), pl.ds(b * LANES, LANES)].T
        return 0

    lax.fori_loop(0, steps, body, 0)
    gather_negs(dim, core_ref[0], t4, negs, nk, ns, nbuf, stage)


def gather_kernel(dim, lists, *refs):
    ids, t4, outs, stage = refs[:lists], refs[lists], refs[lists + 1:2 * lists + 1], refs[2 * lists + 1]
    for i in range(lists):
        gather_out(dim, t4, ids[i], outs[i], stage, outs[i].shape[1])


def query_kernel(dim, edges, first, *refs):
    if first:
        core_ref, rel, hb, rfm, q_out, r_out, stage, fm, r4 = refs
    else:
        core_ref, rel, hb, rfm_in, vr_in, rmine, rother, q_out, r_out, r4_out, rfm, vr, stage, fm, r4, out_sem = refs
        core = core_ref[0]
    half = dim // 2
    relp = rfm.shape[1]
    tops = SLICES * LANES
    if not first:
        fm[pl.ds(pl.multiple_of(core * half, 8), half), :] = rmine[...]
        fm[pl.ds(pl.multiple_of((1 - core) * half, 8), half), :] = rother[...]
        grad = fm[pl.ds(0, dim), :]
        vr[...] = vr_in[...] + jnp.sum(grad * grad, axis=0, keepdims=True) / dim
        rate = LEARN_RATE / jnp.sqrt(vr[...] + ADA_EPS)
        rfm[...] = rfm_in[...] - fm[pl.ds(0, dim), :] * rate
    fm[pl.ds(dim, tops - dim), pl.ds(0, LANES)] = jnp.zeros((tops - dim, LANES), F32)
    for b in range(relp // LANES):
        for j in range(SLICES):
            if (j + 1) * LANES <= dim:
                block = rfm[pl.ds(j * LANES, LANES), pl.ds(b * LANES, LANES)]
            else:
                fm[pl.ds(j * LANES, dim - j * LANES), pl.ds(0, LANES)] = rfm[pl.ds(j * LANES, dim - j * LANES), pl.ds(b * LANES, LANES)]
                block = fm[pl.ds(j * LANES, LANES), pl.ds(0, LANES)]
            r4[pl.ds(SLICES * b * LANES + j, LANES, stride=SLICES), :] = block.T

    def step(b, _):
        cols = pl.ds(pl.multiple_of(b * LANES, LANES), LANES)
        gather_rows(r4, rel, b * LANES, stage, LANES)
        for j in range(SLICES):
            size = min(LANES, dim - j * LANES)
            r_out[pl.ds(j * LANES, size), cols] = stage_cols(stage, j)[:size]
        h = hb[:, cols].astype(F32)
        r_re, r_im = r_out[pl.ds(0, half), cols], r_out[pl.ds(half, half), cols]
        q_out[pl.ds(0, half), cols] = h[:half] * r_re - h[half:] * r_im
        q_out[pl.ds(half, half), cols] = h[:half] * r_im + h[half:] * r_re
        return 0

    step(0, 0)
    if not first:
        save = pltpu.make_async_copy(r4, r4_out, out_sem)
        save.start()
    lax.fori_loop(1, edges // LANES, step, 0)
    if not first:
        save.wait()


def place_negs(core, nb, nfull, nother):
    nhalf = nfull.shape[1]
    nb[:, pl.ds(pl.multiple_of(core * nhalf, LANES), nhalf)] = nfull[...]
    nb[:, pl.ds(pl.multiple_of((1 - core) * nhalf, LANES), nhalf)] = nother[...]


def exp_kernel(neg_count, edges, core_ref, q, nfull, nother, e_out, top_out, sum_out, nb, nbt, sc):
    negp = nb.shape[1]
    place_negs(core_ref[0], nb, nfull, nother)
    for b in range(negp // LANES):
        nbt[pl.ds(b * LANES, LANES), :] = nb[:, pl.ds(b * LANES, LANES)].astype(F32).T.astype(BF16)

    def step(c, _):
        cols = pl.ds(pl.multiple_of(c * CHUNK, LANES), CHUNK)
        sc[...] = lax.dot_general(nbt[pl.ds(0, neg_count), :], q[:, cols].astype(BF16), (((1,), (0,)), ((), ())), preferred_element_type=F32)
        top = jnp.max(sc[...], axis=0, keepdims=True)
        top_out[:, cols] = top
        total = jnp.zeros((1, CHUNK), F32)
        part = 200
        for i in range(0, neg_count, part):
            size = min(part, neg_count - i)
            e = jnp.exp(sc[pl.ds(i, size), :] - top)
            e_out[pl.ds(i, size), cols] = e
            total = total + jnp.sum(e, axis=0, keepdims=True)
        sum_out[:, cols] = total
        return 0

    lax.fori_loop(0, edges // CHUNK, step, 0)


def score_kernel(dim, neg_count, edges, core_ref, w, q, tb, e, neg_top, neg_sum,
                 loss, dp_out, ds, nk, ns, ng):
    core = core_ref[0]
    negp = ds.shape[0]
    ng[...] = jnp.zeros(ng.shape, F32)
    ds[pl.ds(neg_count, negp - neg_count), :] = jnp.zeros((negp - neg_count, edges), BF16)

    def step(c, loss_row):
        cols = pl.ds(pl.multiple_of(c * CHUNK, LANES), CHUNK)
        pos = jnp.sum(q[:, cols] * tb[:, cols].astype(F32), axis=0, keepdims=True)
        top = jnp.maximum(pos, neg_top[:, cols])
        pos_exp = jnp.exp(pos - top)
        shrink = jnp.exp(neg_top[:, cols] - top)
        norm = pos_exp + shrink * neg_sum[:, cols]
        wt = w[:, cols]
        loss_row = loss_row + wt * (top + jnp.log(norm) - pos)
        dp_out[:, cols] = wt * (pos_exp / norm - 1.0)
        ds[pl.ds(0, neg_count), cols] = (e[:, cols] * (wt * shrink / norm)).astype(BF16)
        ng[...] += lax.dot_general(ds[:, cols], q[:, cols].astype(BF16), (((1,), (1,)), ((), ())), preferred_element_type=F32)
        return loss_row

    loss_row = lax.fori_loop(0, edges // CHUNK, step, jnp.zeros((1, CHUNK), F32))
    loss[...] = jnp.broadcast_to(jnp.sum(loss_row, axis=1, keepdims=True) / edges, loss.shape)

    def save(b, _):
        rows = pl.ds(pl.multiple_of(b * LANES, LANES), LANES)
        put_halves(core, nk, ns, rows, lambda j: ng[rows, pl.ds(j * LANES, min(LANES, dim - j * LANES))].T, dim)
        return 0

    lax.fori_loop(0, negp // LANES, save, 0)


def grad_kernel(dim, edges, core_ref, rel, ds, dp, tb, hb, r, nfull, nother, hg, rk, rs, nb, racc, stage, qs):
    half = dim // 2
    tops = SLICES * LANES
    place_negs(core_ref[0], nb, nfull, nother)
    zero_rows(racc)
    qs[:, pl.ds(dim, tops - dim), :] = jnp.zeros((2, tops - dim, CHUNK), F32)

    def compute(c):
        cols = pl.ds(pl.multiple_of(c * CHUNK, LANES), CHUNK)
        gq = lax.dot_general(nb[...], ds[:, cols], (((1,), (0,)), ((), ())), preferred_element_type=F32) + dp[:, cols] * tb[:, cols].astype(F32)
        g_re, g_im = gq[:half], gq[half:]
        h = hb[:, cols].astype(F32)
        h_re, h_im = h[:half], h[half:]
        r_re, r_im = r[pl.ds(0, half), cols], r[pl.ds(half, half), cols]
        for part, (f_re, f_im) in enumerate(((h_re, h_im), (r_re, r_im))):
            qs[part, pl.ds(0, half), :] = g_re * f_re + g_im * f_im
            qs[part, pl.ds(half, half), :] = g_im * f_re - g_re * f_im

    def turn(c, slot, b, j):
        place = pl.ds(j * LANES, LANES), pl.ds(b * LANES, LANES)
        stage[slot, pl.ds(SLICES * b * LANES + j, LANES, stride=SLICES), :] = qs[(0,) + place].T
        hg[pl.ds(SLICES * (c * CHUNK + b * LANES) + j, LANES, stride=SLICES), :] = qs[(1,) + place].T

    blocks = [(b, j) for b in range(CHUNK // LANES) for j in range(SLICES)]
    share = CHUNK // len(blocks)
    compute(0)
    for b, j in blocks:
        turn(0, 0, b, j)

    def step(i, _):
        for slot in range(2):
            c = 2 * i + slot
            after = jnp.minimum(c + 1, edges // CHUNK - 1)
            compute(after)
            for k, (b, j) in enumerate(blocks):
                add_rows([(racc, rel, c * CHUNK + k * share, stage.at[slot], k * share * SLICES)], share)
                turn(after, 1 - slot, b, j)
        return 0

    lax.fori_loop(0, edges // CHUNK // 2, step, 0)

    def save(b, _):
        cols = pl.ds(pl.multiple_of(b * LANES, LANES), LANES)
        put_halves(core_ref[0], rk, rs, cols, lambda j: racc[pl.ds(SLICES * LANES * b + j, LANES, stride=SLICES), :].T, dim)
        return 0

    lax.fori_loop(0, rk.shape[1] // LANES, save, 0)


def unstage(rt, stage):
    for j in range(SLICES):
        stage[pl.ds(j, LANES, stride=SLICES), :] = rt[pl.ds(j * LANES, LANES), :].T


def scatter_kernel(dim, edges, own, *refs):
    if own:
        heads, tails, hg, dp, q, acc, stage, rows, rt = refs
    else:
        heads, tails, rel, hg, dp, hb_hbm, r4_hbm, acc, stage, rows, rt, hb_in, r4, in_sem = refs
        loads = [pltpu.make_async_copy(hb_hbm, hb_in, in_sem.at[0]), pltpu.make_async_copy(r4_hbm, r4, in_sem.at[1])]
        for load in loads:
            load.start()
    half = dim // 2
    blocks = edges // LANES
    zero_rows(acc)
    rt[:, pl.ds(dim, SLICES * LANES - dim), :] = jnp.zeros((2, SLICES * LANES - dim, LANES), F32)

    def compute(b, slot):
        cols = pl.ds(pl.multiple_of(b * LANES, LANES), LANES)
        scale = dp[:, cols]
        if own:
            rt[1, pl.ds(0, dim), :] = q[:, cols] * scale
        else:
            gather_rows(r4, rel, b * LANES, stage, LANES)
            for j in range(SLICES):
                rt[0, pl.ds(j * LANES, LANES), :] = stage_cols(stage, j)
            h = hb_in[:, cols].astype(F32)
            r_re, r_im = rt[0, pl.ds(0, half), :], rt[0, pl.ds(half, half), :]
            rt[1, pl.ds(0, half), :] = scale * (h[:half] * r_re - h[half:] * r_im)
            rt[1, pl.ds(half, half), :] = scale * (h[:half] * r_im + h[half:] * r_re)
        unstage(rt.at[1], rows.at[slot])

    if not own:
        for load in loads:
            load.wait()
    compute(0, 0)

    def step(i, _):
        for slot in range(2):
            b = 2 * i + slot
            add_rows([(acc, tails, b * LANES, rows.at[slot], 0)], LANES)
            add_rows([(acc, heads, b * LANES, hg, b * LANES * SLICES)], LANES)
            compute(jnp.minimum(b + 1, blocks - 1), 1 - slot)
        return 0

    lax.fori_loop(0, blocks // 2, step, 0)


def update_kernel(dim, rows, last, *refs):
    if last:
        core_ref, negs, t4, v, _, nmine, nother, acc, et_out, g_out, stage, rt, rate, outbuf, out_sem = refs
    else:
        core_ref, negs, negs_n, old_t4, v, _, nmine, nother, acc, t4, new_v, nk, ns, stage, rt, rate, nbuf = refs
    core = core_ref[0]
    half = dim // 2
    rt[pl.ds(dim, SLICES * LANES - dim), :] = jnp.zeros((SLICES * LANES - dim, LANES), F32)

    def neg_step(b, _):
        cols = pl.ds(pl.multiple_of(b * LANES, LANES), LANES)
        rt[pl.ds(pl.multiple_of(core * half, 8), half), :] = nmine[:, cols]
        rt[pl.ds(pl.multiple_of((1 - core) * half, 8), half), :] = nother[:, cols]
        unstage(rt, stage)
        add_rows([(acc, negs, b * LANES, stage, 0)], LANES)
        return 0

    lax.fori_loop(0, nmine.shape[1] // LANES, neg_step, 0)

    blocks = rows // LANES

    def slices(b):
        return [pl.ds(SLICES * LANES * b + j, LANES, stride=SLICES) for j in range(SLICES)]

    def advance(b, out):
        where = slices(b)
        square = acc[where[0], :] * acc[where[0], :]
        for j in range(1, SLICES):
            square = square + acc[where[j], :] * acc[where[j], :]
        state = v[pl.ds(b, 1), :] + jnp.sum(square.T, axis=0, keepdims=True) / dim
        out[pl.ds(b, 1), :] = state
        return jnp.broadcast_to(LEARN_RATE / jnp.sqrt(state + ADA_EPS), (LANES, LANES)).T

    if not last:
        def open_pair(p):
            steps = [advance(2 * p + i, new_v) for i in range(2)]
            for i in range(2):
                rate[i] = steps[i]

        def close_pair(p, steps):
            for i in range(2):
                for w in slices(2 * p + i):
                    t4[w, :] = old_t4[w, :] - acc[w, :] * steps[i]

        def ada_step(p, _):
            steps = [rate[0], rate[1]]
            close_pair(p - 1, steps)
            open_pair(p)
            return 0

        open_pair(0)
        lax.fori_loop(1, blocks // 2, ada_step, 0)
        close_pair(blocks // 2 - 1, [rate[0], rate[1]])
        t4[pl.ds(rows * SLICES, 32), :] = jnp.zeros((32, LANES), F32)
        gather_negs(dim, core, t4, negs_n, nk, ns, nbuf, stage)
        return

    width = outbuf.shape[2]
    per = width // LANES
    steps = rows // width

    def save(step, slot):
        return pltpu.make_async_copy(outbuf.at[slot], et_out.at[:, pl.ds(pl.multiple_of(step * width, LANES), width)], out_sem.at[slot])

    def open_group(step, slot):
        for i in range(per):
            rate[slot, i] = advance(step * per + i, g_out)

    open_group(0, 0)

    def exit_step(step, _):
        slot = lax.rem(step, 2)

        @pl.when(step >= 2)
        def _():
            save(step - 2, slot).wait()

        for i in range(per):
            step_size = rate[slot, i]
            for j, w in enumerate(slices(step * per + i)):
                size = min(LANES, dim - j * LANES)
                outbuf[slot, pl.ds(j * LANES, size), pl.ds(i * LANES, LANES)] = (t4[w, :] - acc[w, :] * step_size).T[:size]
        open_group(jnp.minimum(step + 1, steps - 1), 1 - slot)
        save(step, slot).start()
        return 0

    lax.fori_loop(0, steps, exit_step, 0)
    save(steps - 2, (steps - 2) % 2).wait()
    save(steps - 1, (steps - 1) % 2).wait()


def padded_bytes(dims, dtype):
    size = jnp.dtype(dtype).itemsize
    dims = (1,) * (2 - len(dims)) + tuple(dims)
    total = ceil_to(dims[-2], 32 // size) * ceil_to(dims[-1], LANES) * size
    for d in dims[:-2]:
        total *= d
    return total


def cost(micros):
    return pl.CostEstimate(flops=int(micros * 5e6), bytes_accessed=0, transcendentals=0)


def shape(dims, dtype=F32):
    return jax.ShapeDtypeStruct(dims, dtype)


def solution(mesh):
    ent_size = mesh.shape['ent']
    row_spec = P(('sweep', 'ent'), None)
    flat_spec = P(('sweep', 'ent'))
    rel_spec = P('sweep', None)
    state_spec = P('sweep')
    edge_spec = P(('sweep', 'ent'), None, None)
    swap = [(i, i ^ 1) for i in range(ent_size)]
    cross = [(i, i ^ 2) for i in range(ent_size)]

    def shift(amount):
        return [(i, (i + amount) % ent_size) for i in range(ent_size)]

    tie = lax.optimization_barrier

    def chip_sum(keep, send):
        return keep + lax.ppermute(send, 'ent', swap)

    def send(value, pairs):
        return lax.ppermute(value, 'ent', pairs)

    def link(part):
        return send(part, cross)

    def finish(part, got):
        mine = part + got
        return mine, lax.ppermute(mine, 'ent', swap)

    def device_fn(ent_emb, ent_ada, rel_emb, rel_ada, head_idx, tail_idx, rel_idx, edge_mask, neg_idx):
        rows, dim = ent_emb.shape
        num_rel = rel_emb.shape[0]
        _, rounds, edges = head_idx.shape
        neg_count = neg_idx.shape[1]
        negp = ceil_to(neg_count, 2 * LANES)
        relp = ceil_to(num_rel, LANES)
        half = dim // 2
        my_dev = lax.axis_index('ent')
        core = (my_dev % 2).reshape(1)

        heads = [head_idx[0, s] * SLICES for s in range(rounds)]
        own_tails = [tail_idx[0, s] * SLICES for s in range(rounds)]
        own_rels = [rel_idx[0, s] * SLICES for s in range(rounds)]
        tails, rels = [own_tails[0]], [own_rels[0]]
        owned = (neg_idx // rows) == my_dev
        neg_local = jnp.where(owned, neg_idx % rows, rows) * SLICES
        neg_local = jnp.pad(neg_local, ((0, 0), (0, negp - neg_count)), constant_values=rows * SLICES)
        negs = [neg_local[s] for s in range(rounds)]
        weights = edge_mask[0].astype(F32)

        wide_rows = (rows + 8) * SLICES
        stage_shape = pltpu.VMEM((SLICES * LANES, LANES), F32)
        square_shape = pltpu.VMEM((SLICES * LANES, LANES), F32)
        table_out, state_out = shape((wide_rows, LANES)), shape((rows // LANES, LANES))
        cols_bf = shape((dim, edges), BF16)
        neg_half = shape((dim, negp // 2), BF16)

        def call(kernel, args, kinds, outs, out_kinds, scratch, micros, name, aliases=None):
            places = {'s': smem, 'h': hbm, 'v': vmem, 'V': vmem}
            windows = [a for a, k in zip(list(args) + outs, kinds + out_kinds) if k == 'v']
            limit = (4 if name == 'grad' else 2) * 2 ** 20 + sum(padded_bytes(a.shape, a.dtype) for a in windows)
            limit += sum(padded_bytes(a.shape, a.dtype) for a in scratch if getattr(a, 'memory_space', None) == pltpu.VMEM)
            args = [pltpu.with_memory_space_constraint(a, pltpu.VMEM if k == 'V' else pltpu.HBM) if k in 'Vh' else a for a, k in zip(args, kinds)]
            outs = [{'V': pltpu.VMEM, 'h': pltpu.HBM}[k](o.shape, o.dtype) if k in 'Vh' else o for o, k in zip(outs, out_kinds)]
            return pl.pallas_call(
                kernel, out_shape=outs, in_specs=[places[k]() for k in kinds], out_specs=[places[k]() for k in out_kinds],
                scratch_shapes=scratch, compiler_params=pltpu.CompilerParams(vmem_limit_bytes=limit),
                input_output_aliases=aliases or {}, cost_estimate=cost(micros))(*args)

        def gather(lists, t4):
            return call(functools.partial(gather_kernel, dim, len(lists)), lists + [t4], 's' * len(lists) + 'V',
                        [cols_bf] * len(lists), 'V' * len(lists), [stage_shape], 1 + 5 * len(lists), 'gather')

        t4, nk, ns = call(
            functools.partial(entry_kernel, dim, rows), [core, negs[0], ent_emb.T], 'ssh',
            [table_out, neg_half, neg_half], 'VVV',
            [pltpu.VMEM((4, SLICES * LANES, 4 * LANES), F32), stage_shape, pltpu.VMEM((dim, negp), BF16), pltpu.SemaphoreType.DMA((4,))], 20, 'entry')
        v = ent_ada.reshape(rows // LANES, LANES)

        rfm = jnp.pad(rel_emb.T, ((0, 0), (0, relp - num_rel)))
        vr = jnp.pad(rel_ada, (0, relp - num_rel), constant_values=1.0).reshape(1, relp)
        losses = []
        rel_grads = None
        for s in range(rounds):
            first, last = s == 0, s == rounds - 1
            even_load = 2 * s == ent_size
            neg_part = chip_sum(nk, ns)
            if first:
                neg_part, t4 = tie((neg_part, t4))
                neg_got = link(neg_part)
                tail_cols, hb = gather([tails[0], heads[0]], t4)
                hb, own_tails, own_rels = tie((hb, own_tails, own_rels))
                for later in range(1, rounds):
                    got = send(jnp.stack([own_tails[later], own_rels[later]]), shift(later))
                    tails.append(got[0])
                    rels.append(got[1])
            else:
                neg_part, t4 = tie((neg_part, t4))
                neg_got = link(neg_part)
                tb, = gather([tails[s]], t4)
                tail_cols = send(tb, shift(-s))
                t4, tb = tie((t4, tb))
                hb, = gather([heads[s]], t4)
                if even_load:
                    head_cols = send(hb, shift(s))
                rel_got, hb = tie((rel_got, hb))
                rel_grads = finish(rel_part, rel_got)
            wide = shape((dim, edges))
            outs, out_kinds = [wide, wide], 'VV'
            rel_rows = pltpu.VMEM((relp * SLICES, LANES), F32)
            scratch = [stage_shape, pltpu.VMEM((SLICES * LANES, relp), F32), rel_rows]
            args, kinds = [core, own_rels[s], hb, rfm], 'ssV' + ('v' if first else 'V')
            if not first:
                outs += [shape((relp * SLICES, LANES)), shape((dim, relp)), shape((1, relp))]
                out_kinds += 'hVv'
                scratch += [pltpu.SemaphoreType.DMA]
                args += [vr] + list(rel_grads)
                kinds += 'vVV'
            res = call(functools.partial(query_kernel, dim, edges, first), args, kinds, outs, out_kinds,
                       scratch, 10, 'query')
            q, r = res[:2]
            neg_got, q = tie((neg_got, q))
            nmine, nother = finish(neg_part, neg_got)
            if not first:
                r4, rfm, vr = res[2:]
            e, neg_top, neg_total = call(
                functools.partial(exp_kernel, neg_count, edges), [core, q, nmine, nother], 'sVVV',
                [shape((neg_count, edges)), shape((1, edges)), shape((1, edges))], 'Vvv',
                [pltpu.VMEM((dim, negp), BF16), pltpu.VMEM((negp, dim), BF16), pltpu.VMEM((neg_count, CHUNK), F32)], 8, 'exp')
            if not first:
                e, tail_cols = tie((e, tail_cols))
                if not even_load:
                    tail_cols, hb = tie((tail_cols, hb))
                    head_cols = send(hb, shift(s))
            loss, dp, ds, gk, gs = call(
                functools.partial(score_kernel, dim, neg_count, edges), [core, weights[s].reshape(1, edges), q, tail_cols, e, neg_top, neg_total], 'svVVVvv',
                [shape((1, LANES)), shape((1, edges)), shape((negp, edges), BF16), shape((half, negp)), shape((half, negp))], 'vvVVV',
                [pltpu.VMEM((negp, dim), F32)], 8, 'score')
            losses.append(loss[0, 0])
            if not first:
                dp_away = send(dp, shift(s))
            neg_part = chip_sum(gk, gs)
            neg_part, ds = tie((neg_part, ds))
            neg_got = link(neg_part)
            hg, rk, rs = call(
                functools.partial(grad_kernel, dim, edges), [core, own_rels[s], ds, dp, tail_cols, hb, r, nmine, nother], 'ssVvVVVVV',
                [shape((edges * SLICES, LANES)), shape((half, relp)), shape((half, relp))], 'VVV',
                [pltpu.VMEM((dim, negp), BF16), pltpu.VMEM((relp * SLICES, LANES), F32), pltpu.VMEM((2, SLICES * CHUNK, LANES), F32),
                 pltpu.VMEM((2, SLICES * LANES, CHUNK), F32)], 12, 'grad')
            rel_part = chip_sum(rk, rs)
            rel_part, hg = tie((rel_part, hg))
            rel_got = link(rel_part)
            scratch = [stage_shape] + [pltpu.VMEM((2, SLICES * LANES, LANES), F32)] * 2
            if first:
                args, kinds = [heads[s], tails[s], hg, dp, q], 'ssVvV'
            else:
                args, kinds = [heads[s], tails[s], rels[s], hg, dp_away, head_cols, r4], 'sssVvhh'
                scratch += [pltpu.VMEM((dim, edges), BF16), rel_rows, pltpu.SemaphoreType.DMA((2,))]
            acc, = call(functools.partial(scatter_kernel, dim, edges, first), args, kinds, [table_out], 'V', scratch, 15, 'scatter')
            neg_got, acc = tie((neg_got, acc))
            gmine, gother = finish(neg_part, neg_got)
            scratch = [stage_shape, square_shape, pltpu.VMEM((2, 4, LANES, LANES) if last else (2, LANES, LANES), F32)]
            if last:
                args, kinds = [core, negs[s], t4, v, acc], 'ssVVV'
                outs, out_kinds = [table_out, shape((dim, rows)), shape((rows // LANES, LANES))], 'Vhv'
                scratch += [pltpu.VMEM((2, dim, 4 * LANES), F32), pltpu.SemaphoreType.DMA((2,))]
                aliases = {4: 0}
            else:
                args, kinds = [core, negs[s], negs[s + 1], t4, v, acc], 'sssVVV'
                outs, out_kinds = [table_out, table_out, state_out, neg_half, neg_half], 'VVVVV'
                scratch += [pltpu.VMEM((dim, negp), BF16)]
                aliases = {5: 0, 3: 1, 4: 2}
            res = call(functools.partial(update_kernel, dim, rows, last), args + [gmine, gother], kinds + 'VV',
                       outs, out_kinds, scratch, 30, 'update', aliases)
            if last:
                _, et, g = res
            else:
                _, t4, v, nk, ns = res

        even = core[0] == 0
        rel_grads = finish(rel_part, rel_got)
        rg = jnp.where(even, jnp.concatenate(rel_grads, axis=0), jnp.concatenate(rel_grads[::-1], axis=0))
        new_vr = vr + jnp.mean(rg * rg, axis=0, keepdims=True)
        new_r = rfm - LEARN_RATE * rg / jnp.sqrt(new_vr + ADA_EPS)
        return et.T, g.reshape(rows), new_r[:, :num_rel].T, new_vr[0, :num_rel], jnp.stack(losses)[None, :]


    return jax.shard_map(device_fn, mesh=mesh,
                         in_specs=(row_spec, flat_spec, rel_spec, state_spec, edge_spec, edge_spec, edge_spec, edge_spec, rel_spec),
                         out_specs=(row_spec, flat_spec, rel_spec, state_spec, row_spec), check_vma=False)
```

```python
import functools

import jax
import jax.numpy as jnp
from jax import lax
from jax.experimental import pallas as pl
from jax.experimental.pallas import tpu as pltpu
from jax.sharding import PartitionSpec as P


LEARN_RATE = 0.05
ADA_EPS = 1e-10
LANES = 128
SLICES = 4
CHUNK = 256
WIDE = 512
BATCH = 4
F32 = jnp.float32
BF16 = jnp.bfloat16


def ceil_to(value, unit):
    return -(-value // unit) * unit


def vmem():
    return pl.BlockSpec(memory_space=pltpu.VMEM)


def smem():
    return pl.BlockSpec(memory_space=pltpu.SMEM)


def hbm():
    return pl.BlockSpec(memory_space=pltpu.MemorySpace.HBM)


def four(index):
    return pl.multiple_of(index, SLICES)


def gather_rows(src, ids, base, stage, count):
    for k in range(count):
        stage[pl.ds(SLICES * k, SLICES), :] = src[pl.ds(four(ids[base + k]), SLICES), :]


def stage_cols(stage, slice_no):
    return stage[pl.ds(slice_no, LANES, stride=SLICES), :].T


def batch_sums(acc, ids, base, rows, row_base):
    index = [ids[base + k] for k in range(BATCH)]
    grads = [rows[pl.ds(four(row_base + SLICES * k), SLICES), :] for k in range(BATCH)]
    total = []
    lanes = [jnp.full((SLICES, LANES), i, jnp.int32) for i in index]
    for k in range(BATCH):
        repeats = [jnp.where(lanes[earlier] == lanes[k], grads[earlier], 0.0) for earlier in range(k)]
        total.append(functools.reduce(jnp.add, repeats, grads[k]))
    total = [acc[pl.ds(four(index[k]), SLICES), :] + total[k] for k in range(BATCH)]
    return index, total


def add_rows(chains, count):
    for first in range(0, count, BATCH):
        done = [batch_sums(acc, ids, base + first, rows, row_base + SLICES * first) for acc, ids, base, rows, row_base in chains]
        for (acc, *_), (index, total) in zip(chains, done):
            for k in range(BATCH):
                acc[pl.ds(four(index[k]), SLICES), :] = total[k]


def put_halves(core, keep, sent, cols, block_of, dim):
    half = dim // 2
    for side in range(2):
        @pl.when(core == side)
        def _():
            for j in range(SLICES):
                block = block_of(j)
                for h in range(2):
                    lo, hi = max(j * LANES, h * half), min((j + 1) * LANES, (h + 1) * half)
                    if lo < hi:
                        (keep if h == side else sent)[pl.ds(lo - h * half, hi - lo), cols] = block[lo - j * LANES:hi - j * LANES]


def zero_rows(ref, step=1024):
    rows = ref.shape[0]
    whole = rows // step

    def body(i, _):
        ref[pl.ds(pl.multiple_of(i * step, 8), step), :] = jnp.zeros((step, LANES), ref.dtype)
        return 0

    lax.fori_loop(0, whole, body, 0)
    if rows % step:
        ref[pl.ds(whole * step, rows % step), :] = jnp.zeros((rows % step, LANES), ref.dtype)


def gather_out(dim, table, ids, out, stage, count):
    def body(b, _):
        gather_rows(table, ids, b * LANES, stage, LANES)
        cols = pl.ds(pl.multiple_of(b * LANES, LANES), LANES)
        for j in range(SLICES):
            size = min(LANES, dim - j * LANES)
            out[pl.ds(j * LANES, size), cols] = stage_cols(stage, j)[:size].astype(BF16)
        return 0

    lax.fori_loop(0, count // LANES, body, 0)


def gather_negs(dim, core, table, negs, nk, ns, nbuf, stage):
    half = nbuf.shape[1] // 2
    gather_out(dim, table, negs, nbuf, stage, nbuf.shape[1])
    nk[...] = nbuf[:, pl.ds(pl.multiple_of(core * half, LANES), half)]
    ns[...] = nbuf[:, pl.ds(pl.multiple_of((1 - core) * half, LANES), half)]


def entry_kernel(dim, rows, core_ref, negs, et, t4, nk, ns, inbuf, stage, nbuf, in_sem):
    cols = inbuf.shape[2]
    steps = rows // cols
    per = cols // LANES

    def fetch(step, slot):
        return pltpu.make_async_copy(et.at[:, pl.ds(pl.multiple_of(step * cols, LANES), cols)],
                                     inbuf.at[slot, pl.ds(0, dim)], in_sem.at[slot])

    slots = inbuf.shape[0]
    for slot in range(slots - 1):
        fetch(slot, slot).start()
    for slot in range(slots):
        inbuf[slot, pl.ds(dim, SLICES * LANES - dim), :] = jnp.zeros((SLICES * LANES - dim, cols), F32)
    t4[pl.ds(rows * SLICES, 32), :] = jnp.zeros((32, LANES), F32)

    def body(step, _):
        slot = lax.rem(step, slots)

        @pl.when(step + slots - 1 < steps)
        def _():
            fetch(step + slots - 1, lax.rem(step + slots - 1, slots)).start()

        fetch(step, slot).wait()
        for b in range(per):
            row0 = (step * per + b) * LANES
            for j in range(SLICES):
                t4[pl.ds(SLICES * row0 + j, LANES, stride=SLICES), :] = inbuf[slot, pl.ds(j * LANES, LANES), pl.ds(b * LANES, LANES)].T
        return 0

    lax.fori_loop(0, steps, body, 0)
    gather_negs(dim, core_ref[0], t4, negs, nk, ns, nbuf, stage)


def gather_kernel(dim, lists, *refs):
    ids, t4, outs, stage = refs[:lists], refs[lists], refs[lists + 1:2 * lists + 1], refs[2 * lists + 1]
    for i in range(lists):
        gather_out(dim, t4, ids[i], outs[i], stage, outs[i].shape[1])


def query_kernel(dim, edges, first, *refs):
    if first:
        core_ref, rel, hb, rfm, q_out, r_out, stage, fm, r4 = refs
    else:
        core_ref, rel, hb, rfm_in, vr_in, rmine, rother, q_out, r_out, r4_out, rfm, vr, stage, fm, r4, out_sem = refs
        core = core_ref[0]
    half = dim // 2
    relp = rfm.shape[1]
    tops = SLICES * LANES
    if not first:
        fm[pl.ds(pl.multiple_of(core * half, 8), half), :] = rmine[...]
        fm[pl.ds(pl.multiple_of((1 - core) * half, 8), half), :] = rother[...]
        grad = fm[pl.ds(0, dim), :]
        vr[...] = vr_in[...] + jnp.sum(grad * grad, axis=0, keepdims=True) / dim
        rate = LEARN_RATE / jnp.sqrt(vr[...] + ADA_EPS)
        rfm[...] = rfm_in[...] - fm[pl.ds(0, dim), :] * rate
    fm[pl.ds(dim, tops - dim), pl.ds(0, LANES)] = jnp.zeros((tops - dim, LANES), F32)
    for b in range(relp // LANES):
        for j in range(SLICES):
            if (j + 1) * LANES <= dim:
                block = rfm[pl.ds(j * LANES, LANES), pl.ds(b * LANES, LANES)]
            else:
                fm[pl.ds(j * LANES, dim - j * LANES), pl.ds(0, LANES)] = rfm[pl.ds(j * LANES, dim - j * LANES), pl.ds(b * LANES, LANES)]
                block = fm[pl.ds(j * LANES, LANES), pl.ds(0, LANES)]
            r4[pl.ds(SLICES * b * LANES + j, LANES, stride=SLICES), :] = block.T

    def step(b, _):
        cols = pl.ds(pl.multiple_of(b * LANES, LANES), LANES)
        gather_rows(r4, rel, b * LANES, stage, LANES)
        for j in range(SLICES):
            size = min(LANES, dim - j * LANES)
            r_out[pl.ds(j * LANES, size), cols] = stage_cols(stage, j)[:size]
        h = hb[:, cols].astype(F32)
        r_re, r_im = r_out[pl.ds(0, half), cols], r_out[pl.ds(half, half), cols]
        q_out[pl.ds(0, half), cols] = h[:half] * r_re - h[half:] * r_im
        q_out[pl.ds(half, half), cols] = h[:half] * r_im + h[half:] * r_re
        return 0

    step(0, 0)
    if not first:
        save = pltpu.make_async_copy(r4, r4_out, out_sem)
        save.start()
    lax.fori_loop(1, edges // LANES, step, 0)
    if not first:
        save.wait()


def place_negs(core, nb, nfull, nother):
    nhalf = nfull.shape[1]
    nb[:, pl.ds(pl.multiple_of(core * nhalf, LANES), nhalf)] = nfull[...]
    nb[:, pl.ds(pl.multiple_of((1 - core) * nhalf, LANES), nhalf)] = nother[...]


def exp_kernel(neg_count, edges, core_ref, q, nfull, nother, e_out, top_out, sum_out, nb, nbt):
    negp = nb.shape[1]
    place_negs(core_ref[0], nb, nfull, nother)
    for b in range(negp // LANES):
        nbt[pl.ds(b * LANES, LANES), :] = nb[:, pl.ds(b * LANES, LANES)].astype(F32).T.astype(BF16)

    def step(c, _):
        cols = pl.ds(pl.multiple_of(c * WIDE, LANES), WIDE)
        e_out[:, cols] = lax.dot_general(nbt[pl.ds(0, neg_count), :], q[:, cols].astype(BF16), (((1,), (0,)), ((), ())), preferred_element_type=F32)
        top = jnp.max(e_out[:, cols], axis=0, keepdims=True)
        top_out[:, cols] = top
        total = jnp.zeros((1, WIDE), F32)
        part = 200
        for i in range(0, neg_count, part):
            size = min(part, neg_count - i)
            e = jnp.exp(e_out[pl.ds(i, size), cols] - top)
            e_out[pl.ds(i, size), cols] = e
            total = total + jnp.sum(e, axis=0, keepdims=True)
        sum_out[:, cols] = total
        return 0

    lax.fori_loop(0, edges // WIDE, step, 0)


def score_kernel(dim, neg_count, edges, core_ref, w, q, tb, e, neg_top, neg_sum,
                 loss, dp_out, ds, nk, ns, ng):
    core = core_ref[0]
    negp = ds.shape[0]
    ng[...] = jnp.zeros(ng.shape, F32)
    ds[pl.ds(neg_count, negp - neg_count), :] = jnp.zeros((negp - neg_count, edges), BF16)

    def step(c, loss_row):
        cols = pl.ds(pl.multiple_of(c * WIDE, LANES), WIDE)
        pos = jnp.sum(q[:, cols] * tb[:, cols].astype(F32), axis=0, keepdims=True)
        top = jnp.maximum(pos, neg_top[:, cols])
        pos_exp = jnp.exp(pos - top)
        shrink = jnp.exp(neg_top[:, cols] - top)
        norm = pos_exp + shrink * neg_sum[:, cols]
        wt = w[:, cols]
        loss_row = loss_row + wt * (top + jnp.log(norm) - pos)
        dp_out[:, cols] = wt * (pos_exp / norm - 1.0)
        ds[pl.ds(0, neg_count), cols] = (e[:, cols] * (wt * shrink / norm)).astype(BF16)
        ng[...] += lax.dot_general(ds[:, cols], q[:, cols].astype(BF16), (((1,), (1,)), ((), ())), preferred_element_type=F32)
        return loss_row

    loss_row = lax.fori_loop(0, edges // WIDE, step, jnp.zeros((1, WIDE), F32))
    loss[...] = jnp.broadcast_to(jnp.sum(loss_row, axis=1, keepdims=True) / edges, loss.shape)

    def save(b, _):
        rows = pl.ds(pl.multiple_of(b * LANES, LANES), LANES)
        put_halves(core, nk, ns, rows, lambda j: ng[rows, pl.ds(j * LANES, min(LANES, dim - j * LANES))].T, dim)
        return 0

    lax.fori_loop(0, negp // LANES, save, 0)


def grad_kernel(dim, edges, core_ref, rel, ds, dp, tb, hb, r, nfull, nother, hg, rk, rs, nb, racc, stage, qs):
    half = dim // 2
    tops = SLICES * LANES
    place_negs(core_ref[0], nb, nfull, nother)
    zero_rows(racc)
    qs[:, pl.ds(dim, tops - dim), :] = jnp.zeros((2, tops - dim, CHUNK), F32)

    def compute(c):
        cols = pl.ds(pl.multiple_of(c * CHUNK, LANES), CHUNK)
        gq = lax.dot_general(nb[...], ds[:, cols], (((1,), (0,)), ((), ())), preferred_element_type=F32) + dp[:, cols] * tb[:, cols].astype(F32)
        g_re, g_im = gq[:half], gq[half:]
        h = hb[:, cols].astype(F32)
        h_re, h_im = h[:half], h[half:]
        r_re, r_im = r[pl.ds(0, half), cols], r[pl.ds(half, half), cols]
        for part, (f_re, f_im) in enumerate(((h_re, h_im), (r_re, r_im))):
            qs[part, pl.ds(0, half), :] = g_re * f_re + g_im * f_im
            qs[part, pl.ds(half, half), :] = g_im * f_re - g_re * f_im

    def turn(c, slot, b, j):
        place = pl.ds(j * LANES, LANES), pl.ds(b * LANES, LANES)
        stage[slot, pl.ds(SLICES * b * LANES + j, LANES, stride=SLICES), :] = qs[(0,) + place].T
        hg[pl.ds(SLICES * (c * CHUNK + b * LANES) + j, LANES, stride=SLICES), :] = qs[(1,) + place].T

    blocks = [(b, j) for b in range(CHUNK // LANES) for j in range(SLICES)]
    share = CHUNK // len(blocks)
    compute(0)
    for b, j in blocks:
        turn(0, 0, b, j)

    def step(i, _):
        for slot in range(2):
            c = 2 * i + slot
            after = jnp.minimum(c + 1, edges // CHUNK - 1)
            compute(after)
            for k, (b, j) in enumerate(blocks):
                add_rows([(racc, rel, c * CHUNK + k * share, stage.at[slot], k * share * SLICES)], share)
                turn(after, 1 - slot, b, j)
        return 0

    lax.fori_loop(0, edges // CHUNK // 2, step, 0)

    def save(b, _):
        cols = pl.ds(pl.multiple_of(b * LANES, LANES), LANES)
        put_halves(core_ref[0], rk, rs, cols, lambda j: racc[pl.ds(SLICES * LANES * b + j, LANES, stride=SLICES), :].T, dim)
        return 0

    lax.fori_loop(0, rk.shape[1] // LANES, save, 0)


def unstage(rt, stage):
    for j in range(SLICES):
        stage[pl.ds(j, LANES, stride=SLICES), :] = rt[pl.ds(j * LANES, LANES), :].T


def scatter_kernel(dim, edges, own, *refs):
    if own:
        heads, tails, hg, dp, q, acc, stage, rows, rt = refs
    else:
        heads, tails, rel, hg, dp, hb_hbm, r4_hbm, acc, stage, rows, rt, hb_in, r4, in_sem = refs
        loads = [pltpu.make_async_copy(hb_hbm, hb_in, in_sem.at[0]), pltpu.make_async_copy(r4_hbm, r4, in_sem.at[1])]
        for load in loads:
            load.start()
    half = dim // 2
    blocks = edges // LANES
    zero_rows(acc)
    rt[:, pl.ds(dim, SLICES * LANES - dim), :] = jnp.zeros((2, SLICES * LANES - dim, LANES), F32)

    def compute(b, slot):
        cols = pl.ds(pl.multiple_of(b * LANES, LANES), LANES)
        scale = dp[:, cols]
        if own:
            rt[1, pl.ds(0, dim), :] = q[:, cols] * scale
        else:
            gather_rows(r4, rel, b * LANES, stage, LANES)
            for j in range(SLICES):
                rt[0, pl.ds(j * LANES, LANES), :] = stage_cols(stage, j)
            h = hb_in[:, cols].astype(F32)
            r_re, r_im = rt[0, pl.ds(0, half), :], rt[0, pl.ds(half, half), :]
            rt[1, pl.ds(0, half), :] = scale * (h[:half] * r_re - h[half:] * r_im)
            rt[1, pl.ds(half, half), :] = scale * (h[:half] * r_im + h[half:] * r_re)
        unstage(rt.at[1], rows.at[slot])

    if not own:
        for load in loads:
            load.wait()
    compute(0, 0)

    def step(i, _):
        for slot in range(2):
            b = 2 * i + slot
            add_rows([(acc, tails, b * LANES, rows.at[slot], 0)], LANES)
            add_rows([(acc, heads, b * LANES, hg, b * LANES * SLICES)], LANES)
            compute(jnp.minimum(b + 1, blocks - 1), 1 - slot)
        return 0

    lax.fori_loop(0, blocks // 2, step, 0)


def update_kernel(dim, rows, last, *refs):
    if last:
        core_ref, negs, t4, v, _, nmine, nother, acc, et_out, g_out, stage, rt, rate, outbuf, out_sem = refs
    else:
        core_ref, negs, negs_n, old_t4, v, _, nmine, nother, acc, t4, new_v, nk, ns, stage, rt, rate, nbuf = refs
    core = core_ref[0]
    half = dim // 2
    rt[pl.ds(dim, SLICES * LANES - dim), :] = jnp.zeros((SLICES * LANES - dim, LANES), F32)

    def neg_step(b, _):
        cols = pl.ds(pl.multiple_of(b * LANES, LANES), LANES)
        rt[pl.ds(pl.multiple_of(core * half, 8), half), :] = nmine[:, cols]
        rt[pl.ds(pl.multiple_of((1 - core) * half, 8), half), :] = nother[:, cols]
        unstage(rt, stage)
        add_rows([(acc, negs, b * LANES, stage, 0)], LANES)
        return 0

    lax.fori_loop(0, nmine.shape[1] // LANES, neg_step, 0)

    blocks = rows // LANES

    def slices(b):
        return [pl.ds(SLICES * LANES * b + j, LANES, stride=SLICES) for j in range(SLICES)]

    def advance(b, out):
        where = slices(b)
        square = acc[where[0], :] * acc[where[0], :]
        for j in range(1, SLICES):
            square = square + acc[where[j], :] * acc[where[j], :]
        state = v[pl.ds(b, 1), :] + jnp.sum(square.T, axis=0, keepdims=True) / dim
        out[pl.ds(b, 1), :] = state
        return jnp.broadcast_to(LEARN_RATE / jnp.sqrt(state + ADA_EPS), (LANES, LANES)).T

    if not last:
        def open_pair(p):
            steps = [advance(2 * p + i, new_v) for i in range(2)]
            for i in range(2):
                rate[i] = steps[i]

        def close_pair(p, steps):
            for i in range(2):
                for w in slices(2 * p + i):
                    t4[w, :] = old_t4[w, :] - acc[w, :] * steps[i]

        def ada_step(p, _):
            steps = [rate[0], rate[1]]
            close_pair(p - 1, steps)
            open_pair(p)
            return 0

        open_pair(0)
        lax.fori_loop(1, blocks // 2, ada_step, 0)
        close_pair(blocks // 2 - 1, [rate[0], rate[1]])
        t4[pl.ds(rows * SLICES, 32), :] = jnp.zeros((32, LANES), F32)
        gather_negs(dim, core, t4, negs_n, nk, ns, nbuf, stage)
        return

    width = outbuf.shape[2]
    per = width // LANES
    steps = rows // width

    def save(step, slot):
        return pltpu.make_async_copy(outbuf.at[slot], et_out.at[:, pl.ds(pl.multiple_of(step * width, LANES), width)], out_sem.at[slot])

    def open_group(step, slot):
        for i in range(per):
            rate[slot, i] = advance(step * per + i, g_out)

    open_group(0, 0)

    def exit_step(step, _):
        slot = lax.rem(step, 2)

        @pl.when(step >= 2)
        def _():
            save(step - 2, slot).wait()

        for i in range(per):
            step_size = rate[slot, i]
            for j, w in enumerate(slices(step * per + i)):
                size = min(LANES, dim - j * LANES)
                outbuf[slot, pl.ds(j * LANES, size), pl.ds(i * LANES, LANES)] = (t4[w, :] - acc[w, :] * step_size).T[:size]
        open_group(jnp.minimum(step + 1, steps - 1), 1 - slot)
        save(step, slot).start()
        return 0

    lax.fori_loop(0, steps, exit_step, 0)
    save(steps - 2, (steps - 2) % 2).wait()
    save(steps - 1, (steps - 1) % 2).wait()


def padded_bytes(dims, dtype):
    size = jnp.dtype(dtype).itemsize
    dims = (1,) * (2 - len(dims)) + tuple(dims)
    total = ceil_to(dims[-2], 32 // size) * ceil_to(dims[-1], LANES) * size
    for d in dims[:-2]:
        total *= d
    return total


def cost(micros):
    return pl.CostEstimate(flops=int(micros * 5e6), bytes_accessed=0, transcendentals=0)


def shape(dims, dtype=F32):
    return jax.ShapeDtypeStruct(dims, dtype)


def solution(mesh):
    ent_size = mesh.shape['ent']
    row_spec = P(('sweep', 'ent'), None)
    flat_spec = P(('sweep', 'ent'))
    rel_spec = P('sweep', None)
    state_spec = P('sweep')
    edge_spec = P(('sweep', 'ent'), None, None)
    swap = [(i, i ^ 1) for i in range(ent_size)]
    cross = [(i, i ^ 2) for i in range(ent_size)]

    def shift(amount):
        return [(i, (i + amount) % ent_size) for i in range(ent_size)]

    tie = lax.optimization_barrier

    def chip_sum(keep, send):
        return keep + lax.ppermute(send, 'ent', swap)

    def send(value, pairs):
        return lax.ppermute(value, 'ent', pairs)

    def link(part):
        return send(part, cross)

    def finish(part, got):
        mine = part + got
        return mine, lax.ppermute(mine, 'ent', swap)

    def device_fn(ent_emb, ent_ada, rel_emb, rel_ada, head_idx, tail_idx, rel_idx, edge_mask, neg_idx):
        rows, dim = ent_emb.shape
        num_rel = rel_emb.shape[0]
        _, rounds, edges = head_idx.shape
        neg_count = neg_idx.shape[1]
        negp = ceil_to(neg_count, 2 * LANES)
        relp = ceil_to(num_rel, LANES)
        half = dim // 2
        my_dev = lax.axis_index('ent')
        core = (my_dev % 2).reshape(1)

        heads = [head_idx[0, s] * SLICES for s in range(rounds)]
        own_tails = [tail_idx[0, s] * SLICES for s in range(rounds)]
        own_rels = [rel_idx[0, s] * SLICES for s in range(rounds)]
        tails, rels = [own_tails[0]], [own_rels[0]]
        owned = (neg_idx // rows) == my_dev
        neg_local = jnp.where(owned, neg_idx % rows, rows) * SLICES
        neg_local = jnp.pad(neg_local, ((0, 0), (0, negp - neg_count)), constant_values=rows * SLICES)
        negs = [neg_local[s] for s in range(rounds)]
        weights = edge_mask[0].astype(F32)

        wide_rows = (rows + 8) * SLICES
        stage_shape = pltpu.VMEM((SLICES * LANES, LANES), F32)
        square_shape = pltpu.VMEM((SLICES * LANES, LANES), F32)
        table_out, state_out = shape((wide_rows, LANES)), shape((rows // LANES, LANES))
        cols_bf = shape((dim, edges), BF16)
        neg_half = shape((dim, negp // 2), BF16)

        def call(kernel, args, kinds, outs, out_kinds, scratch, micros, name, aliases=None):
            places = {'s': smem, 'h': hbm, 'v': vmem, 'V': vmem}
            windows = [a for a, k in zip(list(args) + outs, kinds + out_kinds) if k == 'v']
            limit = (4 if name == 'grad' else 2) * 2 ** 20 + sum(padded_bytes(a.shape, a.dtype) for a in windows)
            limit += sum(padded_bytes(a.shape, a.dtype) for a in scratch if getattr(a, 'memory_space', None) == pltpu.VMEM)
            args = [pltpu.with_memory_space_constraint(a, pltpu.VMEM if k == 'V' else pltpu.HBM) if k in 'Vh' else a for a, k in zip(args, kinds)]
            outs = [{'V': pltpu.VMEM, 'h': pltpu.HBM}[k](o.shape, o.dtype) if k in 'Vh' else o for o, k in zip(outs, out_kinds)]
            return pl.pallas_call(
                kernel, out_shape=outs, in_specs=[places[k]() for k in kinds], out_specs=[places[k]() for k in out_kinds],
                scratch_shapes=scratch, compiler_params=pltpu.CompilerParams(vmem_limit_bytes=limit),
                input_output_aliases=aliases or {}, cost_estimate=cost(micros))(*args)

        def gather(lists, t4):
            return call(functools.partial(gather_kernel, dim, len(lists)), lists + [t4], 's' * len(lists) + 'V',
                        [cols_bf] * len(lists), 'V' * len(lists), [stage_shape], 1 + 5 * len(lists), 'gather')

        t4, nk, ns = call(
            functools.partial(entry_kernel, dim, rows), [core, negs[0], ent_emb.T], 'ssh',
            [table_out, neg_half, neg_half], 'VVV',
            [pltpu.VMEM((8, SLICES * LANES, 4 * LANES), F32), stage_shape, pltpu.VMEM((dim, negp), BF16), pltpu.SemaphoreType.DMA((8,))], 20, 'entry')
        v = ent_ada.reshape(rows // LANES, LANES)

        rfm = jnp.pad(rel_emb.T, ((0, 0), (0, relp - num_rel)))
        vr = jnp.pad(rel_ada, (0, relp - num_rel), constant_values=1.0).reshape(1, relp)
        losses = []
        rel_grads = None
        for s in range(rounds):
            first, last = s == 0, s == rounds - 1
            even_load = 2 * s == ent_size
            neg_part = chip_sum(nk, ns)
            if first:
                neg_part, t4 = tie((neg_part, t4))
                neg_got = link(neg_part)
                tail_cols, hb = gather([tails[0], heads[0]], t4)
                hb, own_tails, own_rels = tie((hb, own_tails, own_rels))
                for later in range(1, rounds):
                    got = send(jnp.stack([own_tails[later], own_rels[later]]), shift(later))
                    tails.append(got[0])
                    rels.append(got[1])
            else:
                neg_part, t4 = tie((neg_part, t4))
                neg_got = link(neg_part)
                tb, = gather([tails[s]], t4)
                tail_cols = send(tb, shift(-s))
                t4, tb = tie((t4, tb))
                hb, = gather([heads[s]], t4)
                if even_load:
                    head_cols = send(hb, shift(s))
                rel_got, hb = tie((rel_got, hb))
                rel_grads = finish(rel_part, rel_got)
            wide = shape((dim, edges))
            outs, out_kinds = [wide, wide], 'VV'
            rel_rows = pltpu.VMEM((relp * SLICES, LANES), F32)
            scratch = [stage_shape, pltpu.VMEM((SLICES * LANES, relp), F32), rel_rows]
            args, kinds = [core, own_rels[s], hb, rfm], 'ssV' + ('v' if first else 'V')
            if not first:
                outs += [shape((relp * SLICES, LANES)), shape((dim, relp)), shape((1, relp))]
                out_kinds += 'hVv'
                scratch += [pltpu.SemaphoreType.DMA]
                args += [vr] + list(rel_grads)
                kinds += 'vVV'
            res = call(functools.partial(query_kernel, dim, edges, first), args, kinds, outs, out_kinds,
                       scratch, 10, 'query')
            q, r = res[:2]
            neg_got, q = tie((neg_got, q))
            nmine, nother = finish(neg_part, neg_got)
            if not first:
                r4, rfm, vr = res[2:]
            e, neg_top, neg_total = call(
                functools.partial(exp_kernel, neg_count, edges), [core, q, nmine, nother], 'sVVV',
                [shape((neg_count, edges)), shape((1, edges)), shape((1, edges))], 'Vvv',
                [pltpu.VMEM((dim, negp), BF16), pltpu.VMEM((negp, dim), BF16)], 8, 'exp')
            if not first:
                e, tail_cols = tie((e, tail_cols))
                if not even_load:
                    tail_cols, hb = tie((tail_cols, hb))
                    head_cols = send(hb, shift(s))
            loss, dp, ds, gk, gs = call(
                functools.partial(score_kernel, dim, neg_count, edges), [core, weights[s].reshape(1, edges), q, tail_cols, e, neg_top, neg_total], 'svVVVvv',
                [shape((1, LANES)), shape((1, edges)), shape((negp, edges), BF16), shape((half, negp)), shape((half, negp))], 'vvVVV',
                [pltpu.VMEM((negp, dim), F32)], 8, 'score')
            losses.append(loss[0, 0])
            if not first:
                dp_away = send(dp, shift(s))
            neg_part = chip_sum(gk, gs)
            neg_part, ds = tie((neg_part, ds))
            neg_got = link(neg_part)
            hg, rk, rs = call(
                functools.partial(grad_kernel, dim, edges), [core, own_rels[s], ds, dp, tail_cols, hb, r, nmine, nother], 'ssVvVVVVV',
                [shape((edges * SLICES, LANES)), shape((half, relp)), shape((half, relp))], 'VVV',
                [pltpu.VMEM((dim, negp), BF16), pltpu.VMEM((relp * SLICES, LANES), F32), pltpu.VMEM((2, SLICES * CHUNK, LANES), F32),
                 pltpu.VMEM((2, SLICES * LANES, CHUNK), F32)], 12, 'grad')
            rel_part = chip_sum(rk, rs)
            rel_part, hg = tie((rel_part, hg))
            rel_got = link(rel_part)
            scratch = [stage_shape] + [pltpu.VMEM((2, SLICES * LANES, LANES), F32)] * 2
            if first:
                args, kinds = [heads[s], tails[s], hg, dp, q], 'ssVvV'
            else:
                args, kinds = [heads[s], tails[s], rels[s], hg, dp_away, head_cols, r4], 'sssVvhh'
                scratch += [pltpu.VMEM((dim, edges), BF16), rel_rows, pltpu.SemaphoreType.DMA((2,))]
            acc, = call(functools.partial(scatter_kernel, dim, edges, first), args, kinds, [table_out], 'V', scratch, 15, 'scatter')
            neg_got, acc = tie((neg_got, acc))
            gmine, gother = finish(neg_part, neg_got)
            scratch = [stage_shape, square_shape, pltpu.VMEM((2, 4, LANES, LANES) if last else (2, LANES, LANES), F32)]
            if last:
                args, kinds = [core, negs[s], t4, v, acc], 'ssVVV'
                outs, out_kinds = [table_out, shape((dim, rows)), shape((rows // LANES, LANES))], 'Vhv'
                scratch += [pltpu.VMEM((2, dim, 4 * LANES), F32), pltpu.SemaphoreType.DMA((2,))]
                aliases = {4: 0}
            else:
                args, kinds = [core, negs[s], negs[s + 1], t4, v, acc], 'sssVVV'
                outs, out_kinds = [table_out, table_out, state_out, neg_half, neg_half], 'VVVVV'
                scratch += [pltpu.VMEM((dim, negp), BF16)]
                aliases = {5: 0, 3: 1, 4: 2}
            res = call(functools.partial(update_kernel, dim, rows, last), args + [gmine, gother], kinds + 'VV',
                       outs, out_kinds, scratch, 30, 'update', aliases)
            if last:
                _, et, g = res
            else:
                _, t4, v, nk, ns = res

        even = core[0] == 0
        rel_grads = finish(rel_part, rel_got)
        rg = jnp.where(even, jnp.concatenate(rel_grads, axis=0), jnp.concatenate(rel_grads[::-1], axis=0))
        new_vr = vr + jnp.mean(rg * rg, axis=0, keepdims=True)
        new_r = rfm - LEARN_RATE * rg / jnp.sqrt(new_vr + ADA_EPS)
        return et.T, g.reshape(rows), new_r[:, :num_rel].T, new_vr[0, :num_rel], jnp.stack(losses)[None, :]


    return jax.shard_map(device_fn, mesh=mesh,
                         in_specs=(row_spec, flat_spec, rel_spec, state_spec, edge_spec, edge_spec, edge_spec, edge_spec, rel_spec),
                         out_specs=(row_spec, flat_spec, rel_spec, state_spec, row_spec), check_vma=False)
```

```python
import functools

import jax
import jax.numpy as jnp
from jax import lax
from jax.experimental import pallas as pl
from jax.experimental.pallas import tpu as pltpu
from jax.sharding import PartitionSpec as P


LEARN_RATE = 0.05
ADA_EPS = 1e-10
LANES = 128
SLICES = 4
CHUNK = 256
WIDE = 512
BATCH = 4
F32 = jnp.float32
BF16 = jnp.bfloat16


def ceil_to(value, unit):
    return -(-value // unit) * unit


def vmem():
    return pl.BlockSpec(memory_space=pltpu.VMEM)


def smem():
    return pl.BlockSpec(memory_space=pltpu.SMEM)


def hbm():
    return pl.BlockSpec(memory_space=pltpu.MemorySpace.HBM)


def four(index):
    return pl.multiple_of(index, SLICES)


def gather_rows(src, ids, base, stage, count):
    for k in range(count):
        stage[pl.ds(SLICES * k, SLICES), :] = src[pl.ds(four(ids[base + k]), SLICES), :]


def stage_cols(stage, slice_no):
    return stage[pl.ds(slice_no, LANES, stride=SLICES), :].T


def batch_sums(acc, ids, base, rows, row_base):
    index = [ids[base + k] for k in range(BATCH)]
    grads = [rows[pl.ds(four(row_base + SLICES * k), SLICES), :] for k in range(BATCH)]
    total = []
    lanes = [jnp.full((SLICES, LANES), i, jnp.int32) for i in index]
    for k in range(BATCH):
        repeats = [jnp.where(lanes[earlier] == lanes[k], grads[earlier], 0.0) for earlier in range(k)]
        total.append(functools.reduce(jnp.add, repeats, grads[k]))
    total = [acc[pl.ds(four(index[k]), SLICES), :] + total[k] for k in range(BATCH)]
    return index, total


def add_rows(chains, count):
    for first in range(0, count, BATCH):
        done = [batch_sums(acc, ids, base + first, rows, row_base + SLICES * first) for acc, ids, base, rows, row_base in chains]
        for (acc, *_), (index, total) in zip(chains, done):
            for k in range(BATCH):
                acc[pl.ds(four(index[k]), SLICES), :] = total[k]


def put_halves(core, keep, sent, cols, block_of, dim):
    half = dim // 2
    for side in range(2):
        @pl.when(core == side)
        def _():
            for j in range(SLICES):
                block = block_of(j)
                for h in range(2):
                    lo, hi = max(j * LANES, h * half), min((j + 1) * LANES, (h + 1) * half)
                    if lo < hi:
                        (keep if h == side else sent)[pl.ds(lo - h * half, hi - lo), cols] = block[lo - j * LANES:hi - j * LANES]


def zero_rows(ref, step=1024):
    rows = ref.shape[0]
    whole = rows // step

    def body(i, _):
        ref[pl.ds(pl.multiple_of(i * step, 8), step), :] = jnp.zeros((step, LANES), ref.dtype)
        return 0

    lax.fori_loop(0, whole, body, 0)
    if rows % step:
        ref[pl.ds(whole * step, rows % step), :] = jnp.zeros((rows % step, LANES), ref.dtype)


def gather_out(dim, table, ids, out, stage, count):
    blocks = count // LANES
    gather_rows(table, ids, 0, stage.at[0], LANES)

    def body(i, _):
        for slot in range(2):
            b = 2 * i + slot
            gather_rows(table, ids, jnp.minimum(b + 1, blocks - 1) * LANES, stage.at[1 - slot], LANES)
            cols = pl.ds(pl.multiple_of(b * LANES, LANES), LANES)
            for j in range(SLICES):
                size = min(LANES, dim - j * LANES)
                out[pl.ds(j * LANES, size), cols] = stage_cols(stage.at[slot], j)[:size].astype(BF16)
        return 0

    lax.fori_loop(0, blocks // 2, body, 0)


def gather_negs(dim, core, table, negs, nk, ns, nbuf, stage):
    half = nbuf.shape[1] // 2
    gather_out(dim, table, negs, nbuf, stage, nbuf.shape[1])
    nk[...] = nbuf[:, pl.ds(pl.multiple_of(core * half, LANES), half)]
    ns[...] = nbuf[:, pl.ds(pl.multiple_of((1 - core) * half, LANES), half)]


def entry_kernel(dim, rows, core_ref, negs, et, t4, nk, ns, inbuf, stage, nbuf, in_sem):
    cols = inbuf.shape[2]
    steps = rows // cols
    per = cols // LANES

    def fetch(step, slot):
        return pltpu.make_async_copy(et.at[:, pl.ds(pl.multiple_of(step * cols, LANES), cols)],
                                     inbuf.at[slot, pl.ds(0, dim)], in_sem.at[slot])

    slots = inbuf.shape[0]
    for slot in range(slots - 1):
        fetch(slot, slot).start()
    for slot in range(slots):
        inbuf[slot, pl.ds(dim, SLICES * LANES - dim), :] = jnp.zeros((SLICES * LANES - dim, cols), F32)
    t4[pl.ds(rows * SLICES, 32), :] = jnp.zeros((32, LANES), F32)

    def body(step, _):
        slot = lax.rem(step, slots)

        @pl.when(step + slots - 1 < steps)
        def _():
            fetch(step + slots - 1, lax.rem(step + slots - 1, slots)).start()

        fetch(step, slot).wait()
        for b in range(per):
            row0 = (step * per + b) * LANES
            for j in range(SLICES):
                t4[pl.ds(SLICES * row0 + j, LANES, stride=SLICES), :] = inbuf[slot, pl.ds(j * LANES, LANES), pl.ds(b * LANES, LANES)].T
        return 0

    lax.fori_loop(0, steps, body, 0)
    gather_negs(dim, core_ref[0], t4, negs, nk, ns, nbuf, stage)


def gather_kernel(dim, lists, *refs):
    ids, t4, outs, stage = refs[:lists], refs[lists], refs[lists + 1:2 * lists + 1], refs[2 * lists + 1]
    for i in range(lists):
        gather_out(dim, t4, ids[i], outs[i], stage, outs[i].shape[1])


def query_kernel(dim, edges, first, *refs):
    if first:
        core_ref, rel, hb, rfm, q_out, r_out, stage, fm, r4 = refs
    else:
        core_ref, rel, hb, rfm_in, vr_in, rmine, rother, q_out, r_out, r4_out, rfm, vr, stage, fm, r4, out_sem = refs
        core = core_ref[0]
    half = dim // 2
    relp = rfm.shape[1]
    tops = SLICES * LANES
    if not first:
        fm[pl.ds(pl.multiple_of(core * half, 8), half), :] = rmine[...]
        fm[pl.ds(pl.multiple_of((1 - core) * half, 8), half), :] = rother[...]
        grad = fm[pl.ds(0, dim), :]
        vr[...] = vr_in[...] + jnp.sum(grad * grad, axis=0, keepdims=True) / dim
        rate = LEARN_RATE / jnp.sqrt(vr[...] + ADA_EPS)
        rfm[...] = rfm_in[...] - fm[pl.ds(0, dim), :] * rate
    fm[pl.ds(dim, tops - dim), pl.ds(0, LANES)] = jnp.zeros((tops - dim, LANES), F32)
    for b in range(relp // LANES):
        for j in range(SLICES):
            if (j + 1) * LANES <= dim:
                block = rfm[pl.ds(j * LANES, LANES), pl.ds(b * LANES, LANES)]
            else:
                fm[pl.ds(j * LANES, dim - j * LANES), pl.ds(0, LANES)] = rfm[pl.ds(j * LANES, dim - j * LANES), pl.ds(b * LANES, LANES)]
                block = fm[pl.ds(j * LANES, LANES), pl.ds(0, LANES)]
            r4[pl.ds(SLICES * b * LANES + j, LANES, stride=SLICES), :] = block.T

    blocks = edges // LANES
    gather_rows(r4, rel, 0, stage.at[0], LANES)
    if not first:
        save = pltpu.make_async_copy(r4, r4_out, out_sem)
        save.start()

    def step(i, _):
        for slot in range(2):
            b = 2 * i + slot
            gather_rows(r4, rel, jnp.minimum(b + 1, blocks - 1) * LANES, stage.at[1 - slot], LANES)
            cols = pl.ds(pl.multiple_of(b * LANES, LANES), LANES)
            for j in range(SLICES):
                size = min(LANES, dim - j * LANES)
                r_out[pl.ds(j * LANES, size), cols] = stage_cols(stage.at[slot], j)[:size]
            h = hb[:, cols].astype(F32)
            r_re, r_im = r_out[pl.ds(0, half), cols], r_out[pl.ds(half, half), cols]
            q_out[pl.ds(0, half), cols] = h[:half] * r_re - h[half:] * r_im
            q_out[pl.ds(half, half), cols] = h[:half] * r_im + h[half:] * r_re
        return 0

    lax.fori_loop(0, blocks // 2, step, 0)
    if not first:
        save.wait()


def place_negs(core, nb, nfull, nother):
    nhalf = nfull.shape[1]
    nb[:, pl.ds(pl.multiple_of(core * nhalf, LANES), nhalf)] = nfull[...]
    nb[:, pl.ds(pl.multiple_of((1 - core) * nhalf, LANES), nhalf)] = nother[...]


def exp_kernel(neg_count, edges, core_ref, q, nfull, nother, e_out, top_out, sum_out, nb, nbt):
    negp = nb.shape[1]
    place_negs(core_ref[0], nb, nfull, nother)
    for b in range(negp // LANES):
        nbt[pl.ds(b * LANES, LANES), :] = nb[:, pl.ds(b * LANES, LANES)].astype(F32).T.astype(BF16)

    def step(c, _):
        cols = pl.ds(pl.multiple_of(c * WIDE, LANES), WIDE)
        e_out[:, cols] = lax.dot_general(nbt[pl.ds(0, neg_count), :], q[:, cols].astype(BF16), (((1,), (0,)), ((), ())), preferred_element_type=F32)
        top = jnp.max(e_out[:, cols], axis=0, keepdims=True)
        top_out[:, cols] = top
        total = jnp.zeros((1, WIDE), F32)
        part = 200
        for i in range(0, neg_count, part):
            size = min(part, neg_count - i)
            e = jnp.exp(e_out[pl.ds(i, size), cols] - top)
            e_out[pl.ds(i, size), cols] = e
            total = total + jnp.sum(e, axis=0, keepdims=True)
        sum_out[:, cols] = total
        return 0

    lax.fori_loop(0, edges // WIDE, step, 0)


def score_kernel(dim, neg_count, edges, core_ref, w, q, tb, e, neg_top, neg_sum,
                 loss, dp_out, ds, nk, ns, ng):
    core = core_ref[0]
    negp = ds.shape[0]
    ng[...] = jnp.zeros(ng.shape, F32)
    ds[pl.ds(neg_count, negp - neg_count), :] = jnp.zeros((negp - neg_count, edges), BF16)

    def step(c, loss_row):
        cols = pl.ds(pl.multiple_of(c * WIDE, LANES), WIDE)
        pos = jnp.sum(q[:, cols] * tb[:, cols].astype(F32), axis=0, keepdims=True)
        top = jnp.maximum(pos, neg_top[:, cols])
        pos_exp = jnp.exp(pos - top)
        shrink = jnp.exp(neg_top[:, cols] - top)
        norm = pos_exp + shrink * neg_sum[:, cols]
        wt = w[:, cols]
        loss_row = loss_row + wt * (top + jnp.log(norm) - pos)
        dp_out[:, cols] = wt * (pos_exp / norm - 1.0)
        ds[pl.ds(0, neg_count), cols] = (e[:, cols] * (wt * shrink / norm)).astype(BF16)
        ng[...] += lax.dot_general(ds[:, cols], q[:, cols].astype(BF16), (((1,), (1,)), ((), ())), preferred_element_type=F32)
        return loss_row

    loss_row = lax.fori_loop(0, edges // WIDE, step, jnp.zeros((1, WIDE), F32))
    loss[...] = jnp.broadcast_to(jnp.sum(loss_row, axis=1, keepdims=True) / edges, loss.shape)

    def save(b, _):
        rows = pl.ds(pl.multiple_of(b * LANES, LANES), LANES)
        put_halves(core, nk, ns, rows, lambda j: ng[rows, pl.ds(j * LANES, min(LANES, dim - j * LANES))].T, dim)
        return 0

    lax.fori_loop(0, negp // LANES, save, 0)


def grad_kernel(dim, edges, core_ref, rel, ds, dp, tb, hb, r, nfull, nother, hg, rk, rs, nb, racc, stage, qs):
    half = dim // 2
    tops = SLICES * LANES
    place_negs(core_ref[0], nb, nfull, nother)
    zero_rows(racc)
    qs[:, pl.ds(dim, tops - dim), :] = jnp.zeros((2, tops - dim, CHUNK), F32)

    def compute(c):
        cols = pl.ds(pl.multiple_of(c * CHUNK, LANES), CHUNK)
        gq = lax.dot_general(nb[...], ds[:, cols], (((1,), (0,)), ((), ())), preferred_element_type=F32) + dp[:, cols] * tb[:, cols].astype(F32)
        g_re, g_im = gq[:half], gq[half:]
        h = hb[:, cols].astype(F32)
        h_re, h_im = h[:half], h[half:]
        r_re, r_im = r[pl.ds(0, half), cols], r[pl.ds(half, half), cols]
        for part, (f_re, f_im) in enumerate(((h_re, h_im), (r_re, r_im))):
            qs[part, pl.ds(0, half), :] = g_re * f_re + g_im * f_im
            qs[part, pl.ds(half, half), :] = g_im * f_re - g_re * f_im

    def turn(c, slot, b, j):
        place = pl.ds(j * LANES, LANES), pl.ds(b * LANES, LANES)
        stage[slot, pl.ds(SLICES * b * LANES + j, LANES, stride=SLICES), :] = qs[(0,) + place].T
        hg[pl.ds(SLICES * (c * CHUNK + b * LANES) + j, LANES, stride=SLICES), :] = qs[(1,) + place].T

    blocks = [(b, j) for b in range(CHUNK // LANES) for j in range(SLICES)]
    share = CHUNK // len(blocks)
    compute(0)
    for b, j in blocks:
        turn(0, 0, b, j)

    def step(i, _):
        for slot in range(2):
            c = 2 * i + slot
            after = jnp.minimum(c + 1, edges // CHUNK - 1)
            compute(after)
            for k, (b, j) in enumerate(blocks):
                add_rows([(racc, rel, c * CHUNK + k * share, stage.at[slot], k * share * SLICES)], share)
                turn(after, 1 - slot, b, j)
        return 0

    lax.fori_loop(0, edges // CHUNK // 2, step, 0)

    def save(b, _):
        cols = pl.ds(pl.multiple_of(b * LANES, LANES), LANES)
        put_halves(core_ref[0], rk, rs, cols, lambda j: racc[pl.ds(SLICES * LANES * b + j, LANES, stride=SLICES), :].T, dim)
        return 0

    lax.fori_loop(0, rk.shape[1] // LANES, save, 0)


def unstage(rt, stage):
    for j in range(SLICES):
        stage[pl.ds(j, LANES, stride=SLICES), :] = rt[pl.ds(j * LANES, LANES), :].T


def scatter_kernel(dim, edges, own, *refs):
    if own:
        heads, tails, hg, dp, q, acc, stage, rows, rt = refs
    else:
        heads, tails, rel, hg, dp, hb_hbm, r4_hbm, acc, stage, rows, rt, hb_in, r4, in_sem = refs
        loads = [pltpu.make_async_copy(hb_hbm, hb_in, in_sem.at[0]), pltpu.make_async_copy(r4_hbm, r4, in_sem.at[1])]
        for load in loads:
            load.start()
    half = dim // 2
    blocks = edges // LANES
    zero_rows(acc)
    rt[:, pl.ds(dim, SLICES * LANES - dim), :] = jnp.zeros((2, SLICES * LANES - dim, LANES), F32)

    def compute(b, slot):
        cols = pl.ds(pl.multiple_of(b * LANES, LANES), LANES)
        scale = dp[:, cols]
        if own:
            rt[1, pl.ds(0, dim), :] = q[:, cols] * scale
        else:
            gather_rows(r4, rel, b * LANES, stage, LANES)
            for j in range(SLICES):
                rt[0, pl.ds(j * LANES, LANES), :] = stage_cols(stage, j)
            h = hb_in[:, cols].astype(F32)
            r_re, r_im = rt[0, pl.ds(0, half), :], rt[0, pl.ds(half, half), :]
            rt[1, pl.ds(0, half), :] = scale * (h[:half] * r_re - h[half:] * r_im)
            rt[1, pl.ds(half, half), :] = scale * (h[:half] * r_im + h[half:] * r_re)
        unstage(rt.at[1], rows.at[slot])

    if not own:
        for load in loads:
            load.wait()
    compute(0, 0)

    def step(i, _):
        for slot in range(2):
            b = 2 * i + slot
            add_rows([(acc, tails, b * LANES, rows.at[slot], 0)], LANES)
            add_rows([(acc, heads, b * LANES, hg, b * LANES * SLICES)], LANES)
            compute(jnp.minimum(b + 1, blocks - 1), 1 - slot)
        return 0

    lax.fori_loop(0, blocks // 2, step, 0)


def update_kernel(dim, rows, last, *refs):
    if last:
        core_ref, negs, t4, v, _, nmine, nother, acc, et_out, g_out, stage, rt, rate, outbuf, out_sem = refs
    else:
        core_ref, negs, negs_n, old_t4, v, _, nmine, nother, acc, t4, new_v, nk, ns, stage, rt, rate, nbuf = refs
    core = core_ref[0]
    half = dim // 2
    rt[pl.ds(dim, SLICES * LANES - dim), :] = jnp.zeros((SLICES * LANES - dim, LANES), F32)

    def neg_step(b, _):
        cols = pl.ds(pl.multiple_of(b * LANES, LANES), LANES)
        rt[pl.ds(pl.multiple_of(core * half, 8), half), :] = nmine[:, cols]
        rt[pl.ds(pl.multiple_of((1 - core) * half, 8), half), :] = nother[:, cols]
        unstage(rt, stage.at[0])
        add_rows([(acc, negs, b * LANES, stage.at[0], 0)], LANES)
        return 0

    lax.fori_loop(0, nmine.shape[1] // LANES, neg_step, 0)

    blocks = rows // LANES

    def slices(b):
        return [pl.ds(SLICES * LANES * b + j, LANES, stride=SLICES) for j in range(SLICES)]

    def advance(b, out):
        where = slices(b)
        square = acc[where[0], :] * acc[where[0], :]
        for j in range(1, SLICES):
            square = square + acc[where[j], :] * acc[where[j], :]
        state = v[pl.ds(b, 1), :] + jnp.sum(square.T, axis=0, keepdims=True) / dim
        out[pl.ds(b, 1), :] = state
        return jnp.broadcast_to(LEARN_RATE / jnp.sqrt(state + ADA_EPS), (LANES, LANES)).T

    if not last:
        def open_pair(p):
            steps = [advance(2 * p + i, new_v) for i in range(2)]
            for i in range(2):
                rate[i] = steps[i]

        def close_pair(p, steps):
            for i in range(2):
                for w in slices(2 * p + i):
                    t4[w, :] = old_t4[w, :] - acc[w, :] * steps[i]

        def ada_step(p, _):
            steps = [rate[0], rate[1]]
            close_pair(p - 1, steps)
            open_pair(p)
            return 0

        open_pair(0)
        lax.fori_loop(1, blocks // 2, ada_step, 0)
        close_pair(blocks // 2 - 1, [rate[0], rate[1]])
        t4[pl.ds(rows * SLICES, 32), :] = jnp.zeros((32, LANES), F32)
        gather_negs(dim, core, t4, negs_n, nk, ns, nbuf, stage)
        return

    width = outbuf.shape[2]
    per = width // LANES
    steps = rows // width

    def save(step, slot):
        return pltpu.make_async_copy(outbuf.at[slot], et_out.at[:, pl.ds(pl.multiple_of(step * width, LANES), width)], out_sem.at[slot])

    def open_group(step, slot):
        for i in range(per):
            rate[slot, i] = advance(step * per + i, g_out)

    open_group(0, 0)

    def exit_step(step, _):
        slot = lax.rem(step, 2)

        @pl.when(step >= 2)
        def _():
            save(step - 2, slot).wait()

        for i in range(per):
            step_size = rate[slot, i]
            for j, w in enumerate(slices(step * per + i)):
                size = min(LANES, dim - j * LANES)
                outbuf[slot, pl.ds(j * LANES, size), pl.ds(i * LANES, LANES)] = (t4[w, :] - acc[w, :] * step_size).T[:size]
        open_group(jnp.minimum(step + 1, steps - 1), 1 - slot)
        save(step, slot).start()
        return 0

    lax.fori_loop(0, steps, exit_step, 0)
    save(steps - 2, (steps - 2) % 2).wait()
    save(steps - 1, (steps - 1) % 2).wait()


def padded_bytes(dims, dtype):
    size = jnp.dtype(dtype).itemsize
    dims = (1,) * (2 - len(dims)) + tuple(dims)
    total = ceil_to(dims[-2], 32 // size) * ceil_to(dims[-1], LANES) * size
    for d in dims[:-2]:
        total *= d
    return total


def cost(micros):
    return pl.CostEstimate(flops=int(micros * 5e6), bytes_accessed=0, transcendentals=0)


def shape(dims, dtype=F32):
    return jax.ShapeDtypeStruct(dims, dtype)


def solution(mesh):
    ent_size = mesh.shape['ent']
    row_spec = P(('sweep', 'ent'), None)
    flat_spec = P(('sweep', 'ent'))
    rel_spec = P('sweep', None)
    state_spec = P('sweep')
    edge_spec = P(('sweep', 'ent'), None, None)
    swap = [(i, i ^ 1) for i in range(ent_size)]
    cross = [(i, i ^ 2) for i in range(ent_size)]

    def shift(amount):
        return [(i, (i + amount) % ent_size) for i in range(ent_size)]

    tie = lax.optimization_barrier

    def chip_sum(keep, send):
        return keep + lax.ppermute(send, 'ent', swap)

    def send(value, pairs):
        return lax.ppermute(value, 'ent', pairs)

    def link(part):
        return send(part, cross)

    def finish(part, got):
        mine = part + got
        return mine, lax.ppermute(mine, 'ent', swap)

    def device_fn(ent_emb, ent_ada, rel_emb, rel_ada, head_idx, tail_idx, rel_idx, edge_mask, neg_idx):
        rows, dim = ent_emb.shape
        num_rel = rel_emb.shape[0]
        _, rounds, edges = head_idx.shape
        neg_count = neg_idx.shape[1]
        negp = ceil_to(neg_count, 2 * LANES)
        relp = ceil_to(num_rel, LANES)
        half = dim // 2
        my_dev = lax.axis_index('ent')
        core = (my_dev % 2).reshape(1)

        heads = [head_idx[0, s] * SLICES for s in range(rounds)]
        own_tails = [tail_idx[0, s] * SLICES for s in range(rounds)]
        own_rels = [rel_idx[0, s] * SLICES for s in range(rounds)]
        tails, rels = [own_tails[0]], [own_rels[0]]
        owned = (neg_idx // rows) == my_dev
        neg_local = jnp.where(owned, neg_idx % rows, rows) * SLICES
        neg_local = jnp.pad(neg_local, ((0, 0), (0, negp - neg_count)), constant_values=rows * SLICES)
        negs = [neg_local[s] for s in range(rounds)]
        weights = edge_mask[0].astype(F32)

        wide_rows = (rows + 8) * SLICES
        stage_shape = pltpu.VMEM((SLICES * LANES, LANES), F32)
        pair_shape = pltpu.VMEM((2, SLICES * LANES, LANES), F32)
        square_shape = pltpu.VMEM((SLICES * LANES, LANES), F32)
        table_out, state_out = shape((wide_rows, LANES)), shape((rows // LANES, LANES))
        cols_bf = shape((dim, edges), BF16)
        neg_half = shape((dim, negp // 2), BF16)

        def call(kernel, args, kinds, outs, out_kinds, scratch, micros, name, aliases=None):
            places = {'s': smem, 'h': hbm, 'v': vmem, 'V': vmem}
            windows = [a for a, k in zip(list(args) + outs, kinds + out_kinds) if k == 'v']
            limit = int((4 if name == 'grad' else 1.75) * 2 ** 20) + sum(padded_bytes(a.shape, a.dtype) for a in windows)
            limit += sum(padded_bytes(a.shape, a.dtype) for a in scratch if getattr(a, 'memory_space', None) == pltpu.VMEM)
            args = [pltpu.with_memory_space_constraint(a, pltpu.VMEM if k == 'V' else pltpu.HBM) if k in 'Vh' else a for a, k in zip(args, kinds)]
            outs = [{'V': pltpu.VMEM, 'h': pltpu.HBM}[k](o.shape, o.dtype) if k in 'Vh' else o for o, k in zip(outs, out_kinds)]
            return pl.pallas_call(
                kernel, out_shape=outs, in_specs=[places[k]() for k in kinds], out_specs=[places[k]() for k in out_kinds],
                scratch_shapes=scratch, compiler_params=pltpu.CompilerParams(vmem_limit_bytes=limit),
                input_output_aliases=aliases or {}, cost_estimate=cost(micros))(*args)

        def gather(lists, t4):
            return call(functools.partial(gather_kernel, dim, len(lists)), lists + [t4], 's' * len(lists) + 'V',
                        [cols_bf] * len(lists), 'V' * len(lists), [pair_shape], 1 + 5 * len(lists), 'gather')

        t4, nk, ns = call(
            functools.partial(entry_kernel, dim, rows), [core, negs[0], ent_emb.T], 'ssh',
            [table_out, neg_half, neg_half], 'VVV',
            [pltpu.VMEM((8, SLICES * LANES, 4 * LANES), F32), pair_shape, pltpu.VMEM((dim, negp), BF16), pltpu.SemaphoreType.DMA((8,))], 20, 'entry')
        v = ent_ada.reshape(rows // LANES, LANES)

        rfm = jnp.pad(rel_emb.T, ((0, 0), (0, relp - num_rel)))
        vr = jnp.pad(rel_ada, (0, relp - num_rel), constant_values=1.0).reshape(1, relp)
        losses = []
        rel_grads = None
        for s in range(rounds):
            first, last = s == 0, s == rounds - 1
            even_load = 2 * s == ent_size
            neg_part = chip_sum(nk, ns)
            if first:
                neg_part, t4 = tie((neg_part, t4))
                neg_got = link(neg_part)
                tail_cols, hb = gather([tails[0], heads[0]], t4)
                hb, own_tails, own_rels = tie((hb, own_tails, own_rels))
                for later in range(1, rounds):
                    got = send(jnp.stack([own_tails[later], own_rels[later]]), shift(later))
                    tails.append(got[0])
                    rels.append(got[1])
            else:
                neg_part, t4 = tie((neg_part, t4))
                neg_got = link(neg_part)
                tb, = gather([tails[s]], t4)
                tail_cols = send(tb, shift(-s))
                t4, tb = tie((t4, tb))
                hb, = gather([heads[s]], t4)
                if even_load:
                    head_cols = send(hb, shift(s))
                rel_got, hb = tie((rel_got, hb))
                rel_grads = finish(rel_part, rel_got)
            wide = shape((dim, edges))
            outs, out_kinds = [wide, wide], 'VV'
            rel_rows = pltpu.VMEM((relp * SLICES, LANES), F32)
            scratch = [pair_shape, pltpu.VMEM((SLICES * LANES, relp), F32), rel_rows]
            args, kinds = [core, own_rels[s], hb, rfm], 'ssV' + ('v' if first else 'V')
            if not first:
                outs += [shape((relp * SLICES, LANES)), shape((dim, relp)), shape((1, relp))]
                out_kinds += 'hVv'
                scratch += [pltpu.SemaphoreType.DMA]
                args += [vr] + list(rel_grads)
                kinds += 'vVV'
            res = call(functools.partial(query_kernel, dim, edges, first), args, kinds, outs, out_kinds,
                       scratch, 10, 'query')
            q, r = res[:2]
            neg_got, q = tie((neg_got, q))
            nmine, nother = finish(neg_part, neg_got)
            if not first:
                r4, rfm, vr = res[2:]
            e, neg_top, neg_total = call(
                functools.partial(exp_kernel, neg_count, edges), [core, q, nmine, nother], 'sVVV',
                [shape((neg_count, edges)), shape((1, edges)), shape((1, edges))], 'Vvv',
                [pltpu.VMEM((dim, negp), BF16), pltpu.VMEM((negp, dim), BF16)], 8, 'exp')
            if not first:
                e, tail_cols = tie((e, tail_cols))
                if not even_load:
                    tail_cols, hb = tie((tail_cols, hb))
                    head_cols = send(hb, shift(s))
            loss, dp, ds, gk, gs = call(
                functools.partial(score_kernel, dim, neg_count, edges), [core, weights[s].reshape(1, edges), q, tail_cols, e, neg_top, neg_total], 'svVVVvv',
                [shape((1, LANES)), shape((1, edges)), shape((negp, edges), BF16), shape((half, negp)), shape((half, negp))], 'vvVVV',
                [pltpu.VMEM((negp, dim), F32)], 8, 'score')
            losses.append(loss[0, 0])
            if not first:
                dp_away = send(dp, shift(s))
            neg_part = chip_sum(gk, gs)
            neg_part, ds = tie((neg_part, ds))
            neg_got = link(neg_part)
            hg, rk, rs = call(
                functools.partial(grad_kernel, dim, edges), [core, own_rels[s], ds, dp, tail_cols, hb, r, nmine, nother], 'ssVvVVVVV',
                [shape((edges * SLICES, LANES)), shape((half, relp)), shape((half, relp))], 'VVV',
                [pltpu.VMEM((dim, negp), BF16), pltpu.VMEM((relp * SLICES, LANES), F32), pltpu.VMEM((2, SLICES * CHUNK, LANES), F32),
                 pltpu.VMEM((2, SLICES * LANES, CHUNK), F32)], 12, 'grad')
            rel_part = chip_sum(rk, rs)
            rel_part, hg = tie((rel_part, hg))
            rel_got = link(rel_part)
            scratch = [stage_shape] + [pair_shape] * 2
            if first:
                args, kinds = [heads[s], tails[s], hg, dp, q], 'ssVvV'
            else:
                args, kinds = [heads[s], tails[s], rels[s], hg, dp_away, head_cols, r4], 'sssVvhh'
                scratch += [pltpu.VMEM((dim, edges), BF16), rel_rows, pltpu.SemaphoreType.DMA((2,))]
            acc, = call(functools.partial(scatter_kernel, dim, edges, first), args, kinds, [table_out], 'V', scratch, 15, 'scatter')
            neg_got, acc = tie((neg_got, acc))
            gmine, gother = finish(neg_part, neg_got)
            scratch = [pair_shape, square_shape, pltpu.VMEM((2, 4, LANES, LANES) if last else (2, LANES, LANES), F32)]
            if last:
                args, kinds = [core, negs[s], t4, v, acc], 'ssVVV'
                outs, out_kinds = [table_out, shape((dim, rows)), shape((rows // LANES, LANES))], 'Vhv'
                scratch += [pltpu.VMEM((2, dim, 4 * LANES), F32), pltpu.SemaphoreType.DMA((2,))]
                aliases = {4: 0}
            else:
                args, kinds = [core, negs[s], negs[s + 1], t4, v, acc], 'sssVVV'
                outs, out_kinds = [table_out, table_out, state_out, neg_half, neg_half], 'VVVVV'
                scratch += [pltpu.VMEM((dim, negp), BF16)]
                aliases = {5: 0, 3: 1, 4: 2}
            res = call(functools.partial(update_kernel, dim, rows, last), args + [gmine, gother], kinds + 'VV',
                       outs, out_kinds, scratch, 30, 'update', aliases)
            if last:
                _, et, g = res
            else:
                _, t4, v, nk, ns = res

        even = core[0] == 0
        rel_grads = finish(rel_part, rel_got)
        rg = jnp.where(even, jnp.concatenate(rel_grads, axis=0), jnp.concatenate(rel_grads[::-1], axis=0))
        new_vr = vr + jnp.mean(rg * rg, axis=0, keepdims=True)
        new_r = rfm - LEARN_RATE * rg / jnp.sqrt(new_vr + ADA_EPS)
        return et.T, g.reshape(rows), new_r[:, :num_rel].T, new_vr[0, :num_rel], jnp.stack(losses)[None, :]


    return jax.shard_map(device_fn, mesh=mesh,
                         in_specs=(row_spec, flat_spec, rel_spec, state_spec, edge_spec, edge_spec, edge_spec, edge_spec, rel_spec),
                         out_specs=(row_spec, flat_spec, rel_spec, state_spec, row_spec), check_vma=False)
```
